128 devices in a mesh: seq: 32 (over z, y, core), head: 4 (over x).
Axes of the slice: x: 4, y: 4, z: 4, core: 2. Of those that a mesh axis runs over, the one named last changes fastest.
Arguments:
- tokens: bfloat16 [16384, 2560], P('seq'), may hold values from -6 to 6
- proj_inner: bfloat16 [2560, 5120], P(None, 'head'), may hold values from -0.125 to 0.125
- proj_gate: bfloat16 [2560, 5120], P(None, 'head'), may hold values from -0.125 to 0.125
- proj_bc: bfloat16 [2560, 256], replicated, may hold values from -0.03125 to 0.03125
- proj_step: bfloat16 [2560, 80], P(None, 'head'), may hold values from -0.125 to 0.125
- conv_inner: float32 [4, 5120], P(None, 'head'), may hold values from -3 to 3
- conv_bc: float32 [4, 256], replicated, may hold values from -3 to 3
- offset_inner: float32 [5120], P('head'), may hold values from -3 to 3
- offset_bc: float32 [256], replicated, may hold values from -1.2 to 1.2
- step_bias: float32 [80], P('head'), as said below
- decay_log: float32 [80], P('head'), as said below
- skip_gain: float32 [80], P('head'), may hold values from 0.5 to 2
- norm_weight: float32 [5120], P('head'), may hold values from 0.25 to 1.75
- out_weight: bfloat16 [5120, 2560], P('head'), may hold values from -0.078125 to 0.078125
Outputs:
- layer_out: bfloat16 [16384, 2560], P(('seq', 'head'))
The draws below stay inside these ranges and needn't reach their ends.
Inputs may be any that keep to these rules, and one draw needn't show every extreme that they name: step_bias holds one value for each head, the same for every token. decay_log holds one value for each head, the same for every token.
All inputs are finite; a program needn't handle non-finite values.
Results may differ from the reference program's by a relative error of at most 0.013.
Values may be sent and summed in bfloat16 or wider, within the bound.
A program may use at most 128 MiB of HBM per device.

```python
import jax
import jax.numpy as jnp
from jax import lax

D = 2560
HEADS = 80
HEADDIM = 64
STATE = 128
KERNEL = 4
SPAN = 128
INNER = 5120
TOKENS = 16384


def head_tables(key):
    ranking = jax.random.permutation(jax.random.fold_in(key, 7), HEADS)
    jitter = jax.random.uniform(jax.random.fold_in(key, 11), (HEADS,), jnp.float32, -0.3, 0.3)
    slow_count = HEADS // 2
    slow_heads = ranking < slow_count
    step_target = jnp.where(slow_heads, 8.0 / TOKENS, 0.1)
    decay_target = jnp.where(slow_heads, 1.0 / TOKENS, 1.0 / 40.0)
    return (step_target, decay_target, jitter)


def draw_step_bias(key, part):
    step_target, decay_target, jitter = head_tables(key)
    return (jnp.log(jnp.expm1(step_target)) + jitter).astype(jnp.float32)


def draw_decay_log(key, part):
    step_target, decay_target, jitter = head_tables(key)
    actual_step = jnp.log1p(jnp.exp(jnp.log(jnp.expm1(step_target)) + jitter))
    return (jnp.log(decay_target) - jnp.log(actual_step) - 0.5).astype(jnp.float32)


def steps_of(own_key, dims, cuts, smallest, largest):
    def one(axis_at, blocks):
        steps = jax.random.uniform(jax.random.fold_in(jax.random.fold_in(own_key, 6), axis_at), (blocks,), jnp.float32, smallest / len(cuts), largest / len(cuts))
        return jnp.repeat(jnp.exp(steps), dims[axis_at] // blocks).reshape((-1,) + (1,) * (len(dims) - axis_at - 1))

    loudness = one(*cuts[0])
    for cut in cuts[1:]:
        loudness = loudness * one(*cut)
    return loudness


def normal_values(stream_key, shape, scale, limit, cuts=(), held_as=jnp.bfloat16):
    values = jax.random.normal(stream_key, shape, jnp.float32) * scale
    if len(cuts) > 0:
        values = steps_of(stream_key, shape, cuts, -0.22, 0.18) * values
    return jnp.clip(values, min=-limit, max=limit).astype(held_as)


def setup_inputs(seed: int = 0) -> dict:
    keys = jax.random.split(jax.random.key(seed), 15)
    return {
        "tokens": normal_values(keys[0], (TOKENS, D), 1.0, 6.0, ((0, 32),)),
        "proj_inner": normal_values(keys[1], (D, INNER), D ** -0.5, 0.125, ((1, 4),)),
        "proj_gate": normal_values(keys[2], (D, INNER), D ** -0.5, 0.125, ((1, 4),)),
        "proj_bc": normal_values(keys[3], (D, 2 * STATE), (16 * D) ** -0.5, 0.03125),
        "proj_step": normal_values(keys[4], (D, HEADS), D ** -0.5, 0.125, ((1, 4),)),
        "conv_inner": normal_values(keys[5], (KERNEL, INNER), KERNEL ** -0.5, 3.0, ((1, 4),), jnp.float32),
        "conv_bc": normal_values(keys[6], (KERNEL, 2 * STATE), KERNEL ** -0.5, 3.0, (), jnp.float32),
        "offset_inner": normal_values(keys[7], (INNER,), 0.5, 3.0, ((0, 4),), jnp.float32),
        "offset_bc": normal_values(keys[8], (2 * STATE,), 0.2, 1.2, (), jnp.float32),
        "step_bias": draw_step_bias(jax.random.fold_in(keys[14], 71), 0),
        "decay_log": draw_decay_log(jax.random.fold_in(keys[14], 71), 0),
        "skip_gain": jnp.clip(0.5 + 1.5 * jax.random.uniform(keys[11], (HEADS,), jnp.float32) ** steps_of(keys[11], (HEADS,), ((0, 4),), -0.2, 0.2), 0.5, 2.0),
        "norm_weight": jnp.clip(1.0 + 0.15 * jax.random.normal(keys[12], (INNER,), jnp.float32), 0.25, 1.75),
        "out_weight": normal_values(keys[13], (INNER, D), INNER ** -0.5, 0.078125, ((0, 4),)),
    }


def causal(padded, weight, offset, length):
    summed = jnp.zeros((length, weight.shape[1]), jnp.float32) + offset.astype(jnp.float32)[None, :]
    for tap_index in range(weight.shape[0]):
        summed = summed + weight[tap_index].astype(jnp.float32)[None, :] * padded[tap_index:tap_index + length].astype(jnp.float32)
    return jax.nn.silu(summed).astype(jnp.bfloat16)

def within_span(inner_c, write_c, read_c, step_c, cum_c):
    scores = jnp.dot(read_c, write_c.T, preferred_element_type=jnp.float32)
    cum_t = cum_c.T
    step_t = step_c.T
    log_gaps = cum_t[:, :, None] - cum_t[:, None, :]
    causal_mask = jnp.tril(jnp.ones((cum_c.shape[0], cum_c.shape[0]), bool))[None]
    decays = jnp.where(causal_mask, jnp.exp(jnp.where(causal_mask, log_gaps, 0.0)), 0.0)
    weights = (scores[None] * decays * step_t[:, None, :]).astype(jnp.bfloat16)
    return jnp.einsum('hij,jhp->ihp', weights.astype(jnp.float32), inner_c.astype(jnp.float32))

def reference(tokens, proj_inner, proj_gate, proj_bc, proj_step, conv_inner, conv_bc, offset_inner, offset_bc, step_bias, decay_log, skip_gain, norm_weight, out_weight):
    tok_rows = tokens.shape[0]
    inner_raw = jnp.dot(tokens, proj_inner, preferred_element_type=jnp.float32).astype(jnp.bfloat16)
    gate_raw = jnp.dot(tokens, proj_gate, preferred_element_type=jnp.float32).astype(jnp.bfloat16)
    bc_raw = jnp.dot(tokens, proj_bc, preferred_element_type=jnp.float32).astype(jnp.bfloat16)
    step_raw = jnp.dot(tokens, proj_step, preferred_element_type=jnp.float32)
    zeros_inner = jnp.zeros((KERNEL - 1, inner_raw.shape[1]), jnp.bfloat16)
    zeros_bc = jnp.zeros((KERNEL - 1, bc_raw.shape[1]), jnp.bfloat16)
    inner_conv = causal(jnp.concatenate([zeros_inner, inner_raw], 0), conv_inner, offset_inner, tok_rows)
    bc_conv = causal(jnp.concatenate([zeros_bc, bc_raw], 0), conv_bc, offset_bc, tok_rows)
    step_sizes = jax.nn.softplus(step_raw + step_bias[None, :])
    log_decay = -jnp.exp(decay_log)[None, :] * step_sizes
    span_total = tok_rows // SPAN
    inner_blocks = inner_conv.reshape(span_total, SPAN, HEADS, HEADDIM)
    write_blocks = bc_conv[:, :STATE].reshape(span_total, SPAN, STATE)
    read_blocks = bc_conv[:, STATE:].reshape(span_total, SPAN, STATE)
    step_blocks = step_sizes.reshape(span_total, SPAN, HEADS)
    cumulative = jnp.cumsum(log_decay.reshape(span_total, SPAN, HEADS), axis=1)

    def advance(carried, pieces):
        inner_c, write_c, read_c, step_c, cum_c = pieces
        intra_out = within_span(inner_c, write_c, read_c, step_c, cum_c)
        inter_out = jnp.exp(cum_c)[:, :, None] * jnp.einsum('in,hnp->ihp', read_c.astype(jnp.float32), carried, precision=lax.Precision.HIGHEST)
        end_weights = jnp.exp(cum_c[-1][None, :] - cum_c) * step_c
        local_states = jnp.einsum('jn,jh,jhp->hnp', write_c.astype(jnp.float32), end_weights, inner_c.astype(jnp.float32), precision=lax.Precision.HIGHEST)
        carried = jnp.exp(cum_c[-1])[:, None, None] * carried + local_states
        return (carried, intra_out + inter_out)
    start_state = jnp.zeros((HEADS, STATE, HEADDIM), jnp.float32)
    _, outputs = lax.scan(advance, start_state, (inner_blocks, write_blocks, read_blocks, step_blocks, cumulative))
    mixed_out = outputs.reshape(tok_rows, HEADS, HEADDIM) + skip_gain[None, :, None] * inner_conv.reshape(tok_rows, HEADS, HEADDIM).astype(jnp.float32)
    gated_pre = mixed_out.reshape(tok_rows, HEADS * HEADDIM) * jax.nn.silu(gate_raw.astype(jnp.float32))
    squares = lax.optimization_barrier(jnp.sum(gated_pre * gated_pre, axis=1))
    scale = 1.0 / jnp.sqrt(squares / (HEADS * HEADDIM) + 0.25)
    gated_out = (gated_pre * scale[:, None] * norm_weight[None, :]).astype(jnp.bfloat16)
    return jnp.dot(gated_out, out_weight, preferred_element_type=jnp.float32).astype(jnp.bfloat16)
```

```python
import functools

import jax
import jax.numpy as jnp
from jax import lax
from jax.experimental import pallas as pl
from jax.experimental.pallas import tpu as pltpu
from jax.sharding import PartitionSpec as P

HEADDIM = 64
STATE = 128
KERNEL = 4
SPAN = 128
HALO = 16
CHUNK = 256
LOG2E = 1.4426950408889634
EPS = 0.25
MESH = pl.DeviceIdType.MESH
F32 = jnp.float32
BF16 = jnp.bfloat16
LINK = jnp.bfloat16


def silu(v):
    return v / (1.0 + jnp.exp(-v))


def dot(a, b):
    return jnp.dot(a, b, preferred_element_type=F32)


def kernel(
    seqs,
    parts,
    inner_all,
    tokens_hbm,
    wi_hbm,
    wg_hbm,
    wbc_hbm,
    wst_hbm,
    conv_i,
    conv_b,
    off_i,
    off_b,
    bias,
    decay_log,
    skip,
    norm_w,
    wo_hbm,
    out,
    tok,
    wi,
    wg,
    wbc,
    wst,
    wo,
    raw,
    xs_ref,
    bc_ref,
    wt_ref,
    cum_ref,
    dt_ref,
    gate,
    part_a,
    part_b,
    state,
    prior,
    st_send,
    st_recv,
    dec_send,
    dec_recv,
    pf_send,
    pf_recv,
    s_in,
    gw,
    far_send,
    far_recv,
    own_send,
    own_recv,
    comb_send,
    comb_recv,
    mine,
    sq_send,
    sq_recv,
    load_sem,
    halo_sem,
    dec_ss,
    dec_rs,
    st_ss,
    st_rs,
    pf_ss,
    pf_rs,
    far_ss,
    far_rs,
    own_ss,
    own_rs,
    comb_ss,
    comb_rs,
    sq_ss,
    sq_rs,
):
    r = lax.axis_index("seq")
    g = lax.axis_index("head")
    rows = tokens_hbm.shape[0]
    width = wi_hbm.shape[1]
    spans = rows // SPAN
    heads = width // HEADDIM
    pairs = heads // 2
    chunks = width // CHUNK
    half = width // 2
    right = lax.rem(g + 1, parts)
    left = lax.rem(g + parts - 1, parts)
    across = lax.rem(g + 2, parts)

    def loaded(src, dst, number):
        return pltpu.make_async_copy(src, dst, load_sem.at[number])

    tok_load = loaded(tokens_hbm, tok.at[pl.ds(HALO, rows), :], 0)
    wst_load = loaded(wst_hbm, wst, 1)
    wbc_load = loaded(wbc_hbm, wbc, 2)
    wg_load = [
        loaded(wg_hbm.at[:, pl.ds(c * CHUNK, CHUNK)], wg.at[c], 3 + c) for c in range(chunks)
    ]
    wi_load = [
        loaded(wi_hbm.at[:, pl.ds(c * CHUNK, CHUNK)], wi.at[c], 3 + chunks + c)
        for c in range(chunks)
    ]
    wo_load = [
        loaded(wo_hbm.at[:, pl.ds(c * CHUNK, CHUNK)], wo.at[c], 3 + 2 * chunks + c)
        for c in range(2 * chunks)
    ]
    tok_load.start()
    wst_load.start()
    wg_load[0].start()
    wg_load[1].start()
    wg_load[2].start()
    wbc_load.start()
    for c in range(chunks):
        wi_load[c].start()
    for c in range(3, chunks):
        wg_load[c].start()
    for c in range(2 * chunks):
        wo_load[c].start()

    barrier = pltpu.get_barrier_semaphore()

    def greet_seq(i, carry):
        pl.semaphore_signal(
            barrier,
            inc=1,
            device_id={"seq": lax.rem(r + i, seqs), "head": g},
            device_id_type=MESH,
        )
        return carry

    lax.fori_loop(1, seqs, greet_seq, 0)
    for other in (right, left, across):
        pl.semaphore_signal(
            barrier, inc=1, device_id={"seq": r, "head": other}, device_id_type=MESH
        )

    def far_copy(src, dst, ss, rs, seq, head):
        return pltpu.make_async_remote_copy(
            src_ref=src,
            dst_ref=dst,
            send_sem=ss,
            recv_sem=rs,
            device_id={"seq": seq, "head": head},
            device_id_type=MESH,
        )

    tok_load.wait()
    pl.semaphore_wait(barrier, seqs + 2)

    halo = far_copy(
        tok.at[pl.ds(rows, HALO), :],
        tok.at[pl.ds(0, HALO), :],
        halo_sem.at[0],
        halo_sem.at[1],
        lax.rem(r + 1, seqs),
        g,
    )

    @pl.when(r < seqs - 1)
    def _():
        halo.start()

    lane = lax.broadcasted_iota(jnp.int32, (SPAN, SPAN), 1)
    sub = lax.broadcasted_iota(jnp.int32, (SPAN, SPAN), 0)
    low = lane < HEADDIM
    low_row = low[:1]
    tri = jnp.where(lane <= sub, 1.0, 0.0).astype(F32)
    wst_load.wait()
    step = dot(tok[pl.ds(HALO, rows), :], wst[...]) + bias[...]
    tail = jnp.exp(-jnp.abs(step))
    up = 1.0 + tail
    log1p = jnp.where(up == 1.0, tail, jnp.log(up) * (tail / jnp.where(up == 1.0, 1.0, up - 1.0)))
    dt = jnp.maximum(step, 0.0) + log1p
    log_a = dt * (-LOG2E * jnp.exp(decay_log[...]))
    dt_ref[...] = jnp.zeros_like(dt_ref)
    part_a[:, pl.ds(0, SPAN)] = jnp.zeros((rows, SPAN), F32)
    dt_ref[:, pl.ds(0, heads)] = dt
    part_a[:, pl.ds(0, heads)] = log_a
    for k in range(spans):
        cum_ref[pl.ds(k * SPAN, SPAN), :] = jnp.dot(
            tri,
            part_a[pl.ds(k * SPAN, SPAN), pl.ds(0, SPAN)],
            preferred_element_type=F32,
            precision=lax.Precision.HIGHEST,
        )

    def gate_chunk(c):
        wg_load[c].wait()
        v = dot(tok[pl.ds(HALO, rows), :], wg[c]).astype(BF16).astype(F32)
        gate[:, pl.ds(c * CHUNK, CHUNK)] = silu(v)

    for c in range(3):
        gate_chunk(c)

    @pl.when(r == 0)
    def _():
        tok[pl.ds(0, HALO), :] = jnp.zeros((HALO, tok.shape[1]), BF16)

    @pl.when(r > 0)
    def _():
        halo.wait_recv()

    @pl.when(r < seqs - 1)
    def _():
        halo.wait_send()

    def conv(slot, taps, offset, cols):
        acc = offset[:, cols]
        for k in range(KERNEL):
            acc = acc + taps[pl.ds(k, 1), cols] * raw[slot, pl.ds(HALO - KERNEL + 1 + k, rows), :]
        return silu(acc).astype(BF16)

    def raw_chunk(slot, weights):
        raw[slot] = dot(tok[...], weights).astype(BF16).astype(F32)

    wbc_load.wait()
    raw_chunk(0, wbc[...])
    wi_load[0].wait()
    raw_chunk(1, wi[0])
    bc_ref[...] = conv(0, conv_b, off_b, pl.ds(0, 2 * STATE))
    for k in range(spans):
        wt_ref[k] = bc_ref[pl.ds(k * SPAN, SPAN), pl.ds(0, STATE)].astype(F32).T.astype(BF16)
    for c in range(1, chunks + 1):
        if c < chunks:
            wi_load[c].wait()
            raw_chunk((c + 1) % 2, wi[c])
        cols = pl.ds((c - 1) * CHUNK, CHUNK)
        xs_ref[:, cols] = conv(c % 2, conv_i, off_i, cols)

    state[...] = jnp.zeros_like(state)

    def local_state(k, carry):
        at = pl.ds(pl.multiple_of(k * SPAN, SPAN), SPAN)
        cum = cum_ref[at, :]
        last = cum[SPAN - 1 :, :]
        end_w = jnp.exp2(jnp.minimum(last - cum, 0.0)) * dt_ref[at, :]
        decay = jnp.exp2(last)
        wt = wt_ref[k]
        for p in range(pairs):
            cols = pl.ds(p * SPAN, SPAN)
            x = xs_ref[at, cols].astype(F32)
            w = jnp.where(
                low,
                jnp.broadcast_to(end_w[:, 2 * p : 2 * p + 1], (SPAN, SPAN)),
                jnp.broadcast_to(end_w[:, 2 * p + 1 : 2 * p + 2], (SPAN, SPAN)),
            )
            d = jnp.where(
                low_row,
                jnp.broadcast_to(decay[:, 2 * p : 2 * p + 1], (1, SPAN)),
                jnp.broadcast_to(decay[:, 2 * p + 1 : 2 * p + 2], (1, SPAN)),
            )
            held = state[:, cols]
            prior[k, :, cols] = held.astype(BF16)
            state[:, cols] = d * held + dot(wt, (x * w).astype(BF16))
        return carry

    lax.fori_loop(0, spans, local_state, 0)

    total = jnp.zeros((1, SPAN), F32)
    for k in range(spans):
        total = total + cum_ref[pl.ds(k * SPAN + SPAN - 1, 1), :]
    total = jnp.exp2(total)
    tiles = STATE // 8
    for p in range(pairs):
        side, at = divmod(p * SPAN, half)
        cols = pl.ds(at, SPAN)
        dec_send[side, :, cols] = jnp.where(
            low_row,
            jnp.broadcast_to(total[:, 2 * p : 2 * p + 1], (1, SPAN)),
            jnp.broadcast_to(total[:, 2 * p + 1 : 2 * p + 2], (1, SPAN)),
        )
        st_send[side, :, :, cols] = (
            state[:, pl.ds(p * SPAN, SPAN)].reshape(tiles, 8, SPAN).astype(LINK)
        )

    my_tile = r // 2
    my_side = lax.rem(r, 2)

    def dec_copy(i, src):
        peer = lax.rem(r + i, seqs)
        return far_copy(
            dec_send.at[lax.rem(peer, 2)], dec_recv.at[src], dec_ss.at[i], dec_rs.at[src], peer, g
        )

    def st_copy(i, src):
        peer = lax.rem(r + i, seqs)
        return far_copy(
            st_send.at[lax.rem(peer, 2), peer // 2],
            st_recv.at[src],
            st_ss.at[i],
            st_rs.at[src],
            peer,
            g,
        )

    def send_state(i, carry):
        dec_copy(i, r).start()
        st_copy(i, r).start()
        return carry

    lax.fori_loop(1, seqs, send_state, 0)
    dec_recv[r] = dec_send[my_side]
    st_recv[r] = st_send[my_side, my_tile]

    for c in range(3, chunks):
        gate_chunk(c)

    def within(k, carry):
        at = pl.ds(pl.multiple_of(k * SPAN, SPAN), SPAN)
        cum = cum_ref[at, :]
        cum_t = cum.T
        dt_t = dt_ref[at, :].T
        read = bc_ref[at, pl.ds(STATE, STATE)]
        write_t = wt_ref[k]
        scores = jnp.where(lane <= sub, dot(read, write_t), 0.0)
        base = carry
        for p in range(pairs):
            cols = pl.ds(p * SPAN, SPAN)
            x = xs_ref[at, cols]
            shown = []
            weights = []
            for h in (2 * p, 2 * p + 1):
                spread = jnp.broadcast_to(cum[:, h : h + 1], (SPAN, SPAN))
                shown.append(spread)
                gap = jnp.minimum(spread - cum_t[h : h + 1, :], 0.0)
                weights.append((scores * jnp.exp2(gap) * dt_t[h : h + 1, :]).astype(BF16))
            zero = jnp.zeros_like(x)
            both = jnp.concatenate([jnp.where(low, x, zero), jnp.where(low, zero, x)], axis=0)
            intra = dot(jnp.concatenate(weights, axis=1), both)
            scale = jnp.exp2(jnp.where(low, shown[0], shown[1]))
            inter = scale * dot(read, prior[k, :, cols])
            ahead = jnp.exp2(
                jnp.where(
                    low_row,
                    jnp.broadcast_to(base[:, 2 * p : 2 * p + 1], (1, SPAN)),
                    jnp.broadcast_to(base[:, 2 * p + 1 : 2 * p + 2], (1, SPAN)),
                )
            )
            gain = jnp.where(
                low_row,
                jnp.broadcast_to(skip[:, 2 * p : 2 * p + 1], (1, SPAN)),
                jnp.broadcast_to(skip[:, 2 * p + 1 : 2 * p + 2], (1, SPAN)),
            )
            opened = gate[at, cols]
            part_a[at, cols] = (intra + inter + gain * x.astype(F32)) * opened
            part_b[at, cols] = scale * ahead * opened
        return base + cum[SPAN - 1 :, :]

    lax.fori_loop(0, spans, within, jnp.zeros((1, SPAN), F32))

    def await_state(i, carry):
        src = lax.rem(r + i, seqs)
        dec_copy(i, src).wait_recv()
        st_copy(i, src).wait_recv()
        return carry

    lax.fori_loop(1, seqs, await_state, 0)

    def scan(d, carry):
        pf_send[d] = carry.astype(LINK)
        return dec_recv[d] * carry + st_recv[d].astype(F32)

    lax.fori_loop(0, seqs, scan, jnp.zeros((8, half), F32))

    def pf_copy(i, src):
        peer = lax.rem(r + i, seqs)
        return far_copy(
            pf_send.at[peer],
            pf_recv.at[lax.rem(src, 2), src // 2],
            pf_ss.at[i],
            pf_rs.at[src],
            peer,
            g,
        )

    def send_prefix(i, carry):
        pf_copy(i, r).start()
        return carry

    lax.fori_loop(1, seqs, send_prefix, 0)
    pf_recv[my_side, my_tile] = pf_send[r]

    def drain_state(i, carry):
        dec_copy(i, r).wait_send()
        st_copy(i, r).wait_send()
        return carry

    lax.fori_loop(1, seqs, drain_state, 0)
    for c in range(2 * chunks):
        wo_load[c].wait()

    def await_prefix(i, carry):
        pf_copy(i, lax.rem(r + i, seqs)).wait_recv()
        return carry

    lax.fori_loop(1, seqs, await_prefix, 0)
    for side in range(2):
        s_in[:, pl.ds(side * half, half)] = (
            pf_recv[side].astype(F32).reshape(STATE, half).astype(BF16)
        )

    eye = jnp.where(lane == sub, 1.0, 0.0).astype(F32)

    def gated(slot, block):
        at = pl.ds(pl.multiple_of(block * SPAN, SPAN), SPAN)
        read = bc_ref[at, pl.ds(STATE, STATE)]
        squares = jnp.zeros((SPAN, CHUNK), F32)
        for c in range(chunks):
            cols = pl.ds(c * CHUNK, CHUNK)
            pre = part_a[at, cols] + part_b[at, cols] * dot(read, s_in[:, cols])
            squares = squares + pre * pre
            gw[slot, :, cols] = (pre * norm_w[:, cols]).astype(BF16)
        column = jnp.sum(squares, axis=1, keepdims=True)
        row = jnp.sum(eye * column, axis=0, keepdims=True)
        sq_send[slot] = jnp.broadcast_to(row, (8, SPAN))

    def sq_copy(slot, offset):
        return far_copy(
            sq_send.at[slot],
            sq_recv.at[offset - 1],
            sq_ss.at[offset - 1],
            sq_rs.at[offset - 1],
            r,
            lax.rem(g + offset, parts),
        )

    def stream(send, recv, ss, rs, c, way):
        at = way * chunks + c
        return far_copy(
            send.at[at], recv.at[at], ss.at[at], rs.at[at], r, (right, left)[way]
        )

    def far_step(c, carry):
        for way in range(2):
            far_send[way * chunks + c] = dot(gw[0], wo[way * chunks + c]).astype(BF16)
            stream(far_send, far_recv, far_ss, far_rs, c, way).start()
        return carry

    def own_step(c, carry):
        for way in range(2):
            own_send[way * chunks + c] = dot(gw[1 + way], wo[(1 - way) * chunks + c]).astype(BF16)
            stream(own_send, own_recv, own_ss, own_rs, c, way).start()
        return carry

    def mine_step(c, carry):
        mine[c] = dot(gw[3], wo[c])
        return carry

    def comb_step(c, carry):
        for way in range(2):
            at = way * chunks + c
            value = dot(gw[1 + way], wo[at])
            stream(far_send, far_recv, far_ss, far_rs, c, way).wait_recv()
            comb_send[at] = (value + far_recv[at].astype(F32)).astype(BF16)
            stream(comb_send, comb_recv, comb_ss, comb_rs, c, way).start()
        return carry

    gated(0, across)
    sq_copy(0, 2).start()
    lax.fori_loop(0, chunks, far_step, 0)
    gated(1, right)
    sq_copy(1, 1).start()
    gated(2, left)
    sq_copy(2, 3).start()
    lax.fori_loop(0, chunks, own_step, 0)
    gated(3, g)
    lax.fori_loop(0, 2 * chunks, mine_step, 0)
    lax.fori_loop(0, chunks, comb_step, 0)

    squares = sq_send[3]
    for slot, offset in ((1, 1), (0, 2), (2, 3)):
        sq_copy(slot, offset).wait_recv()
        squares = squares + sq_recv[offset - 1]
    scale_row = 1.0 / jnp.sqrt(squares[:1] * (1.0 / inner_all) + EPS)
    scale = jnp.sum(eye * scale_row, axis=1, keepdims=True)

    for c in range(chunks):
        stream(own_send, own_recv, own_ss, own_rs, c, 1).wait_recv()
        stream(comb_send, comb_recv, comb_ss, comb_rs, c, 0).wait_recv()
        value = mine[c] + own_recv[chunks + c].astype(F32) + comb_recv[c].astype(F32)
        out[:, pl.ds(c * CHUNK, CHUNK)] = (value * scale).astype(BF16)
        stream(own_send, own_recv, own_ss, own_rs, c, 0).wait_recv()
        stream(comb_send, comb_recv, comb_ss, comb_rs, c, 1).wait_recv()
        value = mine[chunks + c] + own_recv[c].astype(F32) + comb_recv[chunks + c].astype(F32)
        out[:, pl.ds((chunks + c) * CHUNK, CHUNK)] = (value * scale).astype(BF16)

    def drain(c, carry):
        for way in range(2):
            stream(far_send, far_recv, far_ss, far_rs, c, way).wait_send()
            stream(own_send, own_recv, own_ss, own_rs, c, way).wait_send()
            stream(comb_send, comb_recv, comb_ss, comb_rs, c, way).wait_send()
        return carry

    lax.fori_loop(0, chunks, drain, 0)
    for slot, offset in ((1, 1), (0, 2), (2, 3)):
        sq_copy(slot, offset).wait_send()

    def drain_prefix(i, carry):
        pf_copy(i, r).wait_send()
        return carry

    lax.fori_loop(1, seqs, drain_prefix, 0)


def per_device(
    seqs,
    parts,
    tokens,
    proj_inner,
    proj_gate,
    proj_bc,
    proj_step,
    conv_inner,
    conv_bc,
    offset_inner,
    offset_bc,
    step_bias,
    decay_log,
    skip_gain,
    norm_weight,
    out_weight,
):
    rows, depth = tokens.shape
    width = proj_inner.shape[1]
    heads = step_bias.shape[0]
    chunks = width // CHUNK
    spans = rows // SPAN
    half = width // 2
    tiles = STATE // 8
    model = out_weight.shape[1]
    any_spec = pl.BlockSpec(memory_space=pl.ANY)
    vmem = pl.BlockSpec(memory_space=pltpu.VMEM)
    dma = pltpu.SemaphoreType.DMA
    streams = [pltpu.VMEM((2 * chunks, SPAN, CHUNK), BF16)] * 6
    scratch = [
        pltpu.VMEM((rows + HALO, depth), BF16),
        pltpu.VMEM((chunks, depth, CHUNK), BF16),
        pltpu.VMEM((chunks, depth, CHUNK), BF16),
        pltpu.VMEM((depth, 2 * STATE), BF16),
        pltpu.VMEM((depth, heads), BF16),
        pltpu.VMEM((2 * chunks, width, CHUNK), BF16),
        pltpu.VMEM((2, rows + HALO, CHUNK), F32),
        pltpu.VMEM((rows, width), BF16),
        pltpu.VMEM((rows, 2 * STATE), BF16),
        pltpu.VMEM((spans, STATE, SPAN), BF16),
        pltpu.VMEM((rows, SPAN), F32),
        pltpu.VMEM((rows, SPAN), F32),
        pltpu.VMEM((rows, width), F32),
        pltpu.VMEM((rows, width), F32),
        pltpu.VMEM((rows, width), F32),
        pltpu.VMEM((STATE, width), F32),
        pltpu.VMEM((spans, STATE, width), BF16),
        pltpu.VMEM((2, tiles, 8, half), LINK),
        pltpu.VMEM((seqs, 8, half), LINK),
        pltpu.VMEM((2, 1, half), F32),
        pltpu.VMEM((seqs, 1, half), F32),
        pltpu.VMEM((seqs, 8, half), LINK),
        pltpu.VMEM((2, tiles, 8, half), LINK),
        pltpu.VMEM((STATE, width), BF16),
        pltpu.VMEM((4, SPAN, width), BF16),
        *streams,
        pltpu.VMEM((2 * chunks, SPAN, CHUNK), F32),
        pltpu.VMEM((4, 8, SPAN), F32),
        pltpu.VMEM((3, 8, SPAN), F32),
        dma((3 + 4 * chunks,)),
        dma((2,)),
        *[dma((seqs,))] * 6,
        *[dma((2 * chunks,))] * 6,
        dma((3,)),
        dma((3,)),
    ]
    row = lambda v: v.reshape(1, -1)
    return pl.pallas_call(
        functools.partial(kernel, seqs, parts, float(parts * width)),
        out_shape=jax.ShapeDtypeStruct((rows // parts, model), BF16),
        in_specs=[any_spec] * 5 + [vmem] * 8 + [any_spec],
        out_specs=vmem,
        scratch_shapes=scratch,
        compiler_params=pltpu.CompilerParams(
            collective_id=0, has_side_effects=True, vmem_limit_bytes=62 * 1024 * 1024
        ),
    )(
        tokens,
        proj_inner,
        proj_gate,
        proj_bc,
        proj_step,
        conv_inner,
        conv_bc,
        row(offset_inner),
        row(offset_bc),
        row(step_bias),
        row(decay_log),
        row(skip_gain),
        row(norm_weight),
        out_weight,
    )


def solution(mesh):
    body = functools.partial(per_device, mesh.shape["seq"], mesh.shape["head"])
    return jax.shard_map(
        body,
        mesh=mesh,
        in_specs=(
            P("seq", None),
            P(None, "head"),
            P(None, "head"),
            P(),
            P(None, "head"),
            P(None, "head"),
            P(),
            P("head"),
            P(),
            P("head"),
            P("head"),
            P("head"),
            P("head"),
            P("head", None),
        ),
        out_specs=P(("seq", "head"), None),
        check_vma=False,
    )
```

```python
import functools

import jax
import jax.numpy as jnp
from jax import lax
from jax.experimental import pallas as pl
from jax.experimental.pallas import tpu as pltpu
from jax.sharding import PartitionSpec as P

HEADDIM = 64
STATE = 128
KERNEL = 4
SPAN = 128
HALO = 16
CHUNK = 256
BLOCK = 64
WIDE = 512
LOG2E = 1.4426950408889634
EPS = 0.25
MESH = pl.DeviceIdType.MESH
F32 = jnp.float32
BF16 = jnp.bfloat16
LINK = jnp.bfloat16


def silu(v):
    return v / (1.0 + jnp.exp(-v))


def dot(a, b):
    return jnp.dot(a, b, preferred_element_type=F32)


def split(v, count):
    terms = []
    for _ in range(count):
        terms.append(v.astype(BF16))
        v = v - terms[-1].astype(F32)
    return terms


def kernel(
    seqs,
    parts,
    inner_all,
    tokens_hbm,
    wi_hbm,
    wg_hbm,
    wbc_hbm,
    wst_hbm,
    conv_i_hbm,
    conv_b_hbm,
    off_i_hbm,
    off_b_hbm,
    bias_hbm,
    decay_log_hbm,
    skip_hbm,
    norm_hbm,
    wo_hbm,
    out,
    conv_i,
    conv_b,
    off_1,
    off_b,
    bias,
    decay_log,
    skip,
    norm_1,
    tok,
    wa,
    wg,
    wl,
    wst,
    wo,
    raw,
    terms,
    spread,
    w_end,
    xs_ref,
    bc_ref,
    wt_ref,
    cum_ref,
    dt_ref,
    gate,
    part_a,
    part_b,
    prior,
    st_send,
    st_recv,
    dec_send,
    dec_recv,
    pf_send,
    pf_recv,
    s_in,
    gw,
    far_send,
    far_recv,
    own_send,
    own_recv,
    comb_send,
    comb_recv,
    mine,
    sq_send,
    sq_recv,
    load_sem,
    small_sem,
    halo_sem,
    dec_ss,
    dec_rs,
    st_ss,
    st_rs,
    pf_ss,
    pf_rs,
    far_ss,
    far_rs,
    own_ss,
    own_rs,
    comb_ss,
    comb_rs,
    sq_ss,
    sq_rs,
):
    r = lax.axis_index("seq")
    g = lax.axis_index("head")
    rows = tokens_hbm.shape[0]
    width = wi_hbm.shape[1]
    spans = rows // SPAN
    heads = width // HEADDIM
    pairs = heads // 2
    chunks = width // CHUNK
    half = width // 2
    right = lax.rem(g + 1, parts)
    left = lax.rem(g + parts - 1, parts)
    across = lax.rem(g + 2, parts)

    def loaded(src, dst, number):
        return pltpu.make_async_copy(src, dst, load_sem.at[number])

    wides = width // WIDE
    rest = width - wides * WIDE
    tok_load = loaded(tokens_hbm, tok.at[pl.ds(HALO, rows), :], 0)
    wst_load = loaded(wst_hbm, wst, 1)
    wl_load = loaded(wg_hbm.at[:, pl.ds(wides * WIDE, rest)], wl, 2)
    wbc_load = loaded(wbc_hbm, wa.at[0, :, pl.ds(0, 2 * STATE)], 3)
    wr_load = loaded(
        wi_hbm.at[:, pl.ds(wides * WIDE, rest)], wa.at[0, :, pl.ds(2 * STATE, rest)], 4
    )
    wi_load = [
        loaded(wi_hbm.at[:, pl.ds(c * WIDE, WIDE)], wa.at[1 + c], 5 + c) for c in range(wides)
    ]
    wg_load = [
        loaded(wg_hbm.at[:, pl.ds(c * WIDE, WIDE)], wg.at[c], 5 + wides + c) for c in range(wides)
    ]
    wo_load = [
        loaded(wo_hbm.at[:, pl.ds(c * CHUNK, CHUNK)], wo.at[c], 5 + 2 * wides + c)
        for c in range(2 * chunks)
    ]
    small_load = [
        pltpu.make_async_copy(src, dst, small_sem.at[i])
        for i, (src, dst) in enumerate(
            (
                (bias_hbm, bias),
                (decay_log_hbm, decay_log),
                (conv_b_hbm, conv_b),
                (off_b_hbm, off_b),
                (conv_i_hbm, conv_i),
                (off_i_hbm, off_1),
                (skip_hbm, skip),
                (norm_hbm, norm_1),
            )
        )
    ]
    tok_load.start()
    for copy in small_load:
        copy.start()
    wst_load.start()
    wl_load.start()
    wbc_load.start()
    wr_load.start()
    for copy in wi_load:
        copy.start()

    barrier = pltpu.get_barrier_semaphore()

    def greet_seq(i, carry):
        pl.semaphore_signal(
            barrier,
            inc=1,
            device_id={"seq": lax.rem(r + i, seqs), "head": g},
            device_id_type=MESH,
        )
        return carry

    lax.fori_loop(1, seqs, greet_seq, 0)
    for other in (right, left, across):
        pl.semaphore_signal(
            barrier, inc=1, device_id={"seq": r, "head": other}, device_id_type=MESH
        )

    def far_copy(src, dst, ss, rs, seq, head):
        return pltpu.make_async_remote_copy(
            src_ref=src,
            dst_ref=dst,
            send_sem=ss,
            recv_sem=rs,
            device_id={"seq": seq, "head": head},
            device_id_type=MESH,
        )

    for copy in small_load:
        copy.wait()
    off_i = off_1[...].reshape(1, -1)
    norm_w = norm_1[...].reshape(1, -1)
    tok_load.wait()
    pl.semaphore_wait(barrier, seqs + 2)

    halo = far_copy(
        tok.at[pl.ds(rows, HALO), :],
        tok.at[pl.ds(0, HALO), :],
        halo_sem.at[0],
        halo_sem.at[1],
        lax.rem(r + 1, seqs),
        g,
    )

    @pl.when(r < seqs - 1)
    def _():
        halo.start()

    lane = lax.broadcasted_iota(jnp.int32, (SPAN, SPAN), 1)
    sub = lax.broadcasted_iota(jnp.int32, (SPAN, SPAN), 0)
    low = lane < HEADDIM
    low_row = low[:1]
    wst_load.wait()
    wl_load.wait()
    own_rows = pl.ds(HALO, rows)
    step = bias[...] + lax.dot_general(
        tok[own_rows, :], wst[...], (((1,), (1,)), ((), ())), preferred_element_type=F32
    )
    gate_last = dot(tok[own_rows, :], wl[...])
    tail = jnp.exp(-jnp.abs(step))
    up = 1.0 + tail
    log1p = jnp.where(up == 1.0, tail, jnp.log(up) * (tail / jnp.where(up == 1.0, 1.0, up - 1.0)))
    dt = jnp.maximum(step, 0.0) + log1p
    log_a = dt * (-LOG2E * jnp.exp(decay_log[...]))
    dt_ref[...] = jnp.zeros_like(dt_ref)
    terms[...] = jnp.zeros_like(terms)
    dt_ref[:, pl.ds(0, heads)] = dt
    for t, term in enumerate(split(log_a, 3)):
        for k in range(spans):
            terms[pl.ds(t * SPAN, SPAN), pl.ds(k * SPAN, heads)] = term[k * SPAN : (k + 1) * SPAN]
    tri = jnp.where(lane <= sub, 1.0, 0.0).astype(BF16)
    cums = dot(jnp.concatenate([tri, tri, tri], axis=1), terms[...])
    head_of = lax.broadcasted_iota(jnp.int32, (SPAN, width), 1) // HEADDIM
    onto = jnp.where(head_of == lax.broadcasted_iota(jnp.int32, (SPAN, width), 0), 1.0, 0.0)
    spread[pl.ds(0, SPAN), :] = onto.astype(BF16)
    spread[pl.ds(SPAN, SPAN), :] = onto.astype(BF16)
    ends = []
    for k in range(spans):
        at = pl.ds(k * SPAN, SPAN)
        cum = cums[:, k * SPAN : (k + 1) * SPAN]
        cum_ref[at, :] = cum
        end_w = jnp.exp2(jnp.minimum(cum[SPAN - 1 :, :] - cum, 0.0)) * dt_ref[at, :]
        ends.append(jnp.concatenate(split(end_w, 2), axis=1))
    w_end[...] = dot(jnp.concatenate(ends, axis=0), spread[...])

    def gate_store(v, cols):
        gate[:, cols] = silu(v.astype(BF16).astype(F32))

    gate_store(gate_last, pl.ds(wides * WIDE, rest))

    @pl.when(r == 0)
    def _():
        tok[pl.ds(0, HALO), :] = jnp.zeros((HALO, tok.shape[1]), BF16)

    @pl.when(r > 0)
    def _():
        halo.wait_recv()

    @pl.when(r < seqs - 1)
    def _():
        halo.wait_send()

    def raw_chunk(q):
        v = dot(tok[...], wa[q]).astype(BF16).astype(F32)
        for j in range(WIDE // SPAN):
            raw[q, j] = v[:, j * SPAN : (j + 1) * SPAN]

    def conv(q, j, taps, offset, col, dst):
        cols = pl.ds(col, SPAN)
        for b in range(rows // BLOCK):
            acc = offset[:, cols]
            for k in range(KERNEL):
                at = pl.ds(HALO - KERNEL + 1 + k + b * BLOCK, BLOCK)
                acc = acc + taps[pl.ds(k, 1), cols] * raw[q, j, at, :]
            dst[pl.ds(b * BLOCK, BLOCK), cols] = silu(acc).astype(BF16)

    tiles = STATE // 8

    def local_state(col):
        cols = pl.ds(col, SPAN)
        p = col // SPAN
        side, at = divmod(col, half)
        held = jnp.zeros((STATE, SPAN), F32)
        for k in range(spans):
            own = pl.ds(k * SPAN, SPAN)
            last = jnp.exp2(cum_ref[pl.ds(k * SPAN + SPAN - 1, 1), :])
            d = jnp.where(
                low_row,
                jnp.broadcast_to(last[:, 2 * p : 2 * p + 1], (1, SPAN)),
                jnp.broadcast_to(last[:, 2 * p + 1 : 2 * p + 2], (1, SPAN)),
            )
            prior[k, :, cols] = held.astype(BF16)
            scaled = (xs_ref[own, cols].astype(F32) * w_end[own, cols]).astype(BF16)
            held = d * held + dot(wt_ref[k], scaled)
        st_send[side, :, :, pl.ds(at, SPAN)] = held.reshape(tiles, 8, SPAN).astype(LINK)

    wbc_load.wait()
    wr_load.wait()
    raw_chunk(0)
    wi_load[0].wait()
    for copy in wg_load:
        copy.start()
    raw_chunk(1)
    for j in range(2 * STATE // SPAN):
        conv(0, j, conv_b, off_b, j * SPAN, bc_ref)
    for k in range(spans):
        wt_ref[k] = bc_ref[pl.ds(k * SPAN, SPAN), pl.ds(0, STATE)].astype(F32).T.astype(BF16)
    for j in range(rest // SPAN):
        conv(0, 2 * STATE // SPAN + j, conv_i, off_i, wides * WIDE + j * SPAN, xs_ref)
        local_state(wides * WIDE + j * SPAN)
    wi_load[1].wait()
    for copy in wo_load:
        copy.start()
    raw_chunk(2)
    for q in range(wides):
        for j in range(WIDE // SPAN):
            conv(1 + q, j, conv_i, off_i, q * WIDE + j * SPAN, xs_ref)
            local_state(q * WIDE + j * SPAN)

    total = jnp.zeros((1, SPAN), F32)
    for k in range(spans):
        total = total + cum_ref[pl.ds(k * SPAN + SPAN - 1, 1), :]
    total = jnp.exp2(total)
    for p in range(pairs):
        side, at = divmod(p * SPAN, half)
        cols = pl.ds(at, SPAN)
        dec_send[side, :, cols] = jnp.where(
            low_row,
            jnp.broadcast_to(total[:, 2 * p : 2 * p + 1], (1, SPAN)),
            jnp.broadcast_to(total[:, 2 * p + 1 : 2 * p + 2], (1, SPAN)),
        )

    my_tile = r // 2
    my_side = lax.rem(r, 2)

    def partner(i):
        def turn(m):
            return jnp.where(m == 3, 0, jnp.where(m == 2, 3, 2 - m))

        slow = lax.rem(r // 8 + turn(i // 8), 4)
        fast = lax.rem(lax.rem(r // 2, 4) + turn(lax.rem(i // 2, 4)), 4)
        side = lax.rem(r + 1 + i, 2)
        return (slow * 4 + fast) * 2 + side

    def dec_copy(i, src):
        peer = partner(i)
        return far_copy(
            dec_send.at[lax.rem(peer, 2)], dec_recv.at[src], dec_ss.at[i], dec_rs.at[src], peer, g
        )

    def st_copy(i, src):
        peer = partner(i)
        return far_copy(
            st_send.at[lax.rem(peer, 2), peer // 2],
            st_recv.at[src],
            st_ss.at[i],
            st_rs.at[src],
            peer,
            g,
        )

    def send_state(i, carry):
        dec_copy(i, r).start()
        st_copy(i, r).start()
        return carry

    lax.fori_loop(0, seqs - 1, send_state, 0)
    dec_recv[r] = dec_send[my_side]
    st_recv[r] = st_send[my_side, my_tile]

    for c in range(wides):
        wg_load[c].wait()
        gate_store(dot(tok[own_rows, :], wg[c]), pl.ds(c * WIDE, WIDE))

    def within(k, carry):
        at = pl.ds(pl.multiple_of(k * SPAN, SPAN), SPAN)
        cum = cum_ref[at, :]
        cum_t = cum.T
        dt_t = dt_ref[at, :].T
        read = bc_ref[at, pl.ds(STATE, STATE)]
        write_t = wt_ref[k]
        scores = jnp.where(lane <= sub, dot(read, write_t), 0.0)
        base = carry
        for p in range(pairs):
            cols = pl.ds(p * SPAN, SPAN)
            x = xs_ref[at, cols]
            shown = []
            weights = []
            for h in (2 * p, 2 * p + 1):
                spread = jnp.broadcast_to(cum[:, h : h + 1], (SPAN, SPAN))
                shown.append(spread)
                gap = jnp.minimum(spread - cum_t[h : h + 1, :], 0.0)
                weights.append((scores * jnp.exp2(gap) * dt_t[h : h + 1, :]).astype(BF16))
            zero = jnp.zeros_like(x)
            both = jnp.concatenate([jnp.where(low, x, zero), jnp.where(low, zero, x)], axis=0)
            intra = dot(jnp.concatenate(weights, axis=1), both)
            scale = jnp.exp2(jnp.where(low, shown[0], shown[1]))
            inter = scale * dot(read, prior[k, :, cols])
            ahead = jnp.exp2(
                jnp.where(
                    low_row,
                    jnp.broadcast_to(base[:, 2 * p : 2 * p + 1], (1, SPAN)),
                    jnp.broadcast_to(base[:, 2 * p + 1 : 2 * p + 2], (1, SPAN)),
                )
            )
            gain = jnp.where(
                low_row,
                jnp.broadcast_to(skip[:, 2 * p : 2 * p + 1], (1, SPAN)),
                jnp.broadcast_to(skip[:, 2 * p + 1 : 2 * p + 2], (1, SPAN)),
            )
            opened = gate[at, cols]
            part_a[at, cols] = (intra + inter + gain * x.astype(F32)) * opened
            part_b[at, cols] = scale * ahead * opened
        return base + cum[SPAN - 1 :, :]

    def await_state(i, carry):
        src = lax.rem(r + i + 1, seqs)
        dec_copy(i, src).wait_recv()
        st_copy(i, src).wait_recv()
        return carry

    lax.fori_loop(0, seqs - 1, await_state, 0)

    def scan(d, carry):
        pf_send[d] = carry.astype(LINK)
        return dec_recv[d] * carry + st_recv[d].astype(F32)

    lax.fori_loop(0, seqs, scan, jnp.zeros((8, half), F32))

    def pf_copy(i, src):
        peer = partner(i)
        return far_copy(
            pf_send.at[peer],
            pf_recv.at[lax.rem(src, 2), src // 2],
            pf_ss.at[i],
            pf_rs.at[src],
            peer,
            g,
        )

    def send_prefix(i, carry):
        pf_copy(i, r).start()
        return carry

    lax.fori_loop(0, seqs - 1, send_prefix, 0)
    pf_recv[my_side, my_tile] = pf_send[r]
    lax.fori_loop(0, spans, within, jnp.zeros((1, SPAN), F32))

    def drain_state(i, carry):
        dec_copy(i, r).wait_send()
        st_copy(i, r).wait_send()
        return carry

    lax.fori_loop(0, seqs - 1, drain_state, 0)
    for c in range(2 * chunks):
        wo_load[c].wait()

    def await_prefix(i, carry):
        pf_copy(i, lax.rem(r + i + 1, seqs)).wait_recv()
        return carry

    lax.fori_loop(0, seqs - 1, await_prefix, 0)
    for side in range(2):
        s_in[:, pl.ds(side * half, half)] = (
            pf_recv[side].astype(F32).reshape(STATE, half).astype(BF16)
        )

    eye = jnp.where(lane == sub, 1.0, 0.0).astype(F32)

    def gated(slot, block):
        at = pl.ds(pl.multiple_of(block * SPAN, SPAN), SPAN)
        read = bc_ref[at, pl.ds(STATE, STATE)]
        squares = jnp.zeros((SPAN, CHUNK), F32)
        for c in range(chunks):
            cols = pl.ds(c * CHUNK, CHUNK)
            pre = part_a[at, cols] + part_b[at, cols] * dot(read, s_in[:, cols])
            squares = squares + pre * pre
            gw[slot, :, cols] = (pre * norm_w[:, cols]).astype(BF16)
        column = jnp.sum(squares, axis=1, keepdims=True)
        row = jnp.sum(eye * column, axis=0, keepdims=True)
        sq_send[slot] = jnp.broadcast_to(row, (8, SPAN))

    def sq_copy(slot, offset):
        return far_copy(
            sq_send.at[slot],
            sq_recv.at[offset - 1],
            sq_ss.at[offset - 1],
            sq_rs.at[offset - 1],
            r,
            lax.rem(g + offset, parts),
        )

    def stream(send, recv, ss, rs, c, way):
        at = way * chunks + c
        return far_copy(
            send.at[at], recv.at[at], ss.at[at], rs.at[at], r, (right, left)[way]
        )

    def far_step(c, carry):
        for way in range(2):
            far_send[way * chunks + c] = dot(gw[0], wo[way * chunks + c]).astype(BF16)
            stream(far_send, far_recv, far_ss, far_rs, c, way).start()
        return carry

    def own_step(c, carry):
        for way in range(2):
            own_send[way * chunks + c] = dot(gw[1 + way], wo[(1 - way) * chunks + c]).astype(BF16)
            stream(own_send, own_recv, own_ss, own_rs, c, way).start()
        return carry

    def mine_step(c, carry):
        mine[c] = dot(gw[3], wo[c])
        return carry

    def comb_step(c, carry):
        for way in range(2):
            at = way * chunks + c
            value = dot(gw[1 + way], wo[at])
            stream(far_send, far_recv, far_ss, far_rs, c, way).wait_recv()
            comb_send[at] = (value + far_recv[at].astype(F32)).astype(BF16)
            stream(comb_send, comb_recv, comb_ss, comb_rs, c, way).start()
        return carry

    gated(0, across)
    sq_copy(0, 2).start()
    lax.fori_loop(0, chunks, far_step, 0)
    gated(1, right)
    sq_copy(1, 1).start()
    gated(2, left)
    sq_copy(2, 3).start()
    lax.fori_loop(0, chunks, own_step, 0)
    gated(3, g)
    lax.fori_loop(0, 2 * chunks, mine_step, 0)
    lax.fori_loop(0, chunks, comb_step, 0)

    squares = sq_send[3]
    for slot, offset in ((1, 1), (0, 2), (2, 3)):
        sq_copy(slot, offset).wait_recv()
        squares = squares + sq_recv[offset - 1]
    scale_row = 1.0 / jnp.sqrt(squares[:1] * (1.0 / inner_all) + EPS)
    scale = jnp.sum(eye * scale_row, axis=1, keepdims=True)

    for c in range(chunks):
        stream(own_send, own_recv, own_ss, own_rs, c, 1).wait_recv()
        stream(comb_send, comb_recv, comb_ss, comb_rs, c, 0).wait_recv()
        value = mine[c] + own_recv[chunks + c].astype(F32) + comb_recv[c].astype(F32)
        out[:, pl.ds(c * CHUNK, CHUNK)] = (value * scale).astype(BF16)
        stream(own_send, own_recv, own_ss, own_rs, c, 0).wait_recv()
        stream(comb_send, comb_recv, comb_ss, comb_rs, c, 1).wait_recv()
        value = mine[chunks + c] + own_recv[c].astype(F32) + comb_recv[chunks + c].astype(F32)
        out[:, pl.ds((chunks + c) * CHUNK, CHUNK)] = (value * scale).astype(BF16)

    def drain(c, carry):
        for way in range(2):
            stream(far_send, far_recv, far_ss, far_rs, c, way).wait_send()
            stream(own_send, own_recv, own_ss, own_rs, c, way).wait_send()
            stream(comb_send, comb_recv, comb_ss, comb_rs, c, way).wait_send()
        return carry

    lax.fori_loop(0, chunks, drain, 0)
    for slot, offset in ((1, 1), (0, 2), (2, 3)):
        sq_copy(slot, offset).wait_send()

    def drain_prefix(i, carry):
        pf_copy(i, r).wait_send()
        return carry

    lax.fori_loop(0, seqs - 1, drain_prefix, 0)


def per_device(
    seqs,
    parts,
    tokens,
    proj_inner,
    proj_gate,
    proj_bc,
    proj_step,
    conv_inner,
    conv_bc,
    offset_inner,
    offset_bc,
    step_bias,
    decay_log,
    skip_gain,
    norm_weight,
    out_weight,
):
    rows, depth = tokens.shape
    width = proj_inner.shape[1]
    heads = step_bias.shape[0]
    chunks = width // CHUNK
    spans = rows // SPAN
    half = width // 2
    tiles = STATE // 8
    model = out_weight.shape[1]
    any_spec = pl.BlockSpec(memory_space=pl.ANY)
    vmem = pl.BlockSpec(memory_space=pltpu.VMEM)
    dma = pltpu.SemaphoreType.DMA
    streams = [pltpu.VMEM((2 * chunks, SPAN, CHUNK), BF16)] * 6
    scratch = [
        pltpu.VMEM((KERNEL, width), F32),
        pltpu.VMEM((KERNEL, 2 * STATE), F32),
        pltpu.VMEM((width,), F32),
        pltpu.VMEM((1, 2 * STATE), F32),
        pltpu.VMEM((1, heads), F32),
        pltpu.VMEM((1, heads), F32),
        pltpu.VMEM((1, heads), F32),
        pltpu.VMEM((width,), F32),
        pltpu.VMEM((rows + HALO, depth), BF16),
        pltpu.VMEM((1 + width // WIDE, depth, WIDE), BF16),
        pltpu.VMEM((width // WIDE, depth, WIDE), BF16),
        pltpu.VMEM((depth, width % WIDE), BF16),
        pltpu.VMEM((heads, depth), BF16),
        pltpu.VMEM((2 * chunks, width, CHUNK), BF16),
        pltpu.VMEM((1 + width // WIDE, WIDE // SPAN, rows + HALO, SPAN), F32),
        pltpu.VMEM((3 * SPAN, spans * SPAN), BF16),
        pltpu.VMEM((2 * SPAN, width), BF16),
        pltpu.VMEM((rows, width), F32),
        pltpu.VMEM((rows, width), BF16),
        pltpu.VMEM((rows, 2 * STATE), BF16),
        pltpu.VMEM((spans, STATE, SPAN), BF16),
        pltpu.VMEM((rows, SPAN), F32),
        pltpu.VMEM((rows, SPAN), F32),
        pltpu.VMEM((rows, width), F32),
        pltpu.VMEM((rows, width), F32),
        pltpu.VMEM((rows, width), F32),
        pltpu.VMEM((spans, STATE, width), BF16),
        pltpu.VMEM((2, tiles, 8, half), LINK),
        pltpu.VMEM((seqs, 8, half), LINK),
        pltpu.VMEM((2, 1, half), F32),
        pltpu.VMEM((seqs, 1, half), F32),
        pltpu.VMEM((seqs, 8, half), LINK),
        pltpu.VMEM((2, tiles, 8, half), LINK),
        pltpu.VMEM((STATE, width), BF16),
        pltpu.VMEM((4, SPAN, width), BF16),
        *streams,
        pltpu.VMEM((2 * chunks, SPAN, CHUNK), F32),
        pltpu.VMEM((4, 8, SPAN), F32),
        pltpu.VMEM((3, 8, SPAN), F32),
        dma((5 + 2 * (width // WIDE) + 2 * chunks,)),
        dma((8,)),
        dma((2,)),
        *[dma((seqs,))] * 6,
        *[dma((2 * chunks,))] * 6,
        dma((3,)),
        dma((3,)),
    ]
    row = lambda v: v.reshape(1, -1)
    return pl.pallas_call(
        functools.partial(kernel, seqs, parts, float(parts * width)),
        out_shape=pltpu.VMEM((rows // parts, model), BF16),
        in_specs=[any_spec] * 14,
        out_specs=vmem,
        scratch_shapes=scratch,
        compiler_params=pltpu.CompilerParams(
            collective_id=0, has_side_effects=True, vmem_limit_bytes=62 * 1024 * 1024
        ),
    )(
        tokens,
        proj_inner,
        proj_gate,
        proj_bc,
        proj_step.T,
        conv_inner,
        conv_bc,
        offset_inner,
        row(offset_bc),
        row(step_bias),
        row(decay_log),
        row(skip_gain),
        norm_weight,
        out_weight,
    )


def solution(mesh):
    body = functools.partial(per_device, mesh.shape["seq"], mesh.shape["head"])
    return jax.shard_map(
        body,
        mesh=mesh,
        in_specs=(
            P("seq", None),
            P(None, "head"),
            P(None, "head"),
            P(),
            P(None, "head"),
            P(None, "head"),
            P(),
            P("head"),
            P(),
            P("head"),
            P("head"),
            P("head"),
            P("head"),
            P("head", None),
        ),
        out_specs=P(("seq", "head"), None),
        check_vma=False,
    )
```

```python
import functools

import jax
import jax.numpy as jnp
from jax import lax
from jax.experimental import pallas as pl
from jax.experimental.pallas import tpu as pltpu
from jax.sharding import PartitionSpec as P

HEADDIM = 64
STATE = 128
KERNEL = 4
SPAN = 128
HALO = 16
CHUNK = 256
BLOCK = 64
WIDE = 512
LOG2E = 1.4426950408889634
EPS = 0.25
MESH = pl.DeviceIdType.MESH
F32 = jnp.float32
BF16 = jnp.bfloat16
LINK = jnp.bfloat16


def silu(v):
    return v / (1.0 + jnp.exp(-v))


def dot(a, b):
    return jnp.dot(a, b, preferred_element_type=F32)


def split(v, count):
    terms = []
    for _ in range(count):
        terms.append(v.astype(BF16))
        v = v - terms[-1].astype(F32)
    return terms


def kernel(
    seqs,
    parts,
    inner_all,
    tokens_hbm,
    wi_hbm,
    wg_hbm,
    wbc_hbm,
    wst_hbm,
    conv_i_hbm,
    conv_b_hbm,
    off_i_hbm,
    off_b_hbm,
    bias_hbm,
    decay_log_hbm,
    skip_hbm,
    norm_hbm,
    wo_hbm,
    out,
    conv_i,
    conv_b,
    off_1,
    off_b,
    bias,
    decay_log,
    skip,
    norm_1,
    tok,
    wa,
    wg,
    wl,
    wst,
    wo,
    raw,
    terms,
    spread,
    w_end,
    xs_ref,
    bc_ref,
    wt_ref,
    cum_ref,
    dt_ref,
    gate,
    part_a,
    part_b,
    prior,
    st_send,
    st_recv,
    dec_send,
    dec_recv,
    pf_send,
    pf_recv,
    s_in,
    gw,
    far_send,
    far_recv,
    own_send,
    own_recv,
    comb_send,
    comb_recv,
    mine,
    sq_send,
    sq_recv,
    load_sem,
    small_sem,
    halo_sem,
    dec_ss,
    dec_rs,
    st_ss,
    st_rs,
    pf_ss,
    pf_rs,
    far_ss,
    far_rs,
    own_ss,
    own_rs,
    comb_ss,
    comb_rs,
    sq_ss,
    sq_rs,
):
    r = lax.axis_index("seq")
    g = lax.axis_index("head")
    rows = tokens_hbm.shape[0]
    width = wi_hbm.shape[1]
    spans = rows // SPAN
    heads = width // HEADDIM
    pairs = heads // 2
    chunks = width // CHUNK
    half = width // 2
    right = lax.rem(g + 1, parts)
    left = lax.rem(g + parts - 1, parts)
    across = lax.rem(g + 2, parts)

    def loaded(src, dst, number):
        return pltpu.make_async_copy(src, dst, load_sem.at[number])

    wides = width // WIDE
    rest = width - wides * WIDE
    tok_load = loaded(tokens_hbm, tok.at[pl.ds(HALO, rows), :], 0)
    wst_load = loaded(wst_hbm, wst, 1)
    wl_load = loaded(wg_hbm.at[:, pl.ds(wides * WIDE, rest)], wl, 2)
    wbc_load = loaded(wbc_hbm, wa.at[0, :, pl.ds(0, 2 * STATE)], 3)
    wr_load = loaded(
        wi_hbm.at[:, pl.ds(wides * WIDE, rest)], wa.at[0, :, pl.ds(2 * STATE, rest)], 4
    )
    wi_load = [
        loaded(wi_hbm.at[:, pl.ds(c * WIDE, WIDE)], wa.at[1 + c], 5 + c) for c in range(wides)
    ]
    wg_load = [
        loaded(wg_hbm.at[:, pl.ds(c * WIDE, WIDE)], wg.at[c], 5 + wides + c) for c in range(wides)
    ]
    wo_load = [
        loaded(wo_hbm.at[:, pl.ds(c * CHUNK, CHUNK)], wo.at[c], 5 + 2 * wides + c)
        for c in range(2 * chunks)
    ]
    small_load = [
        pltpu.make_async_copy(src, dst, small_sem.at[i])
        for i, (src, dst) in enumerate(
            (
                (bias_hbm, bias),
                (decay_log_hbm, decay_log),
                (conv_b_hbm, conv_b),
                (off_b_hbm, off_b),
                (conv_i_hbm, conv_i),
                (off_i_hbm, off_1),
                (skip_hbm, skip),
                (norm_hbm, norm_1),
            )
        )
    ]
    tok_load.start()
    for copy in small_load:
        copy.start()
    wst_load.start()
    wbc_load.start()
    wr_load.start()

    barrier = pltpu.get_barrier_semaphore()

    def greet_seq(i, carry):
        pl.semaphore_signal(
            barrier,
            inc=1,
            device_id={"seq": lax.rem(r + i, seqs), "head": g},
            device_id_type=MESH,
        )
        return carry

    lax.fori_loop(1, seqs, greet_seq, 0)
    for other in (right, left, across):
        pl.semaphore_signal(
            barrier, inc=1, device_id={"seq": r, "head": other}, device_id_type=MESH
        )

    def far_copy(src, dst, ss, rs, seq, head):
        return pltpu.make_async_remote_copy(
            src_ref=src,
            dst_ref=dst,
            send_sem=ss,
            recv_sem=rs,
            device_id={"seq": seq, "head": head},
            device_id_type=MESH,
        )

    for copy in small_load:
        copy.wait()
    off_i = off_1[...].reshape(1, -1)
    norm_w = norm_1[...].reshape(1, -1)
    tok_load.wait()
    for copy in wi_load:
        copy.start()
    pl.semaphore_wait(barrier, seqs + 2)

    halo = far_copy(
        tok.at[pl.ds(rows, HALO), :],
        tok.at[pl.ds(0, HALO), :],
        halo_sem.at[0],
        halo_sem.at[1],
        lax.rem(r + 1, seqs),
        g,
    )

    @pl.when(r < seqs - 1)
    def _():
        halo.start()

    lane = lax.broadcasted_iota(jnp.int32, (SPAN, SPAN), 1)
    sub = lax.broadcasted_iota(jnp.int32, (SPAN, SPAN), 0)
    low = lane < HEADDIM
    low_row = low[:1]
    wst_load.wait()
    own_rows = pl.ds(HALO, rows)
    step = bias[...] + jnp.concatenate(
        [
            lax.dot_general(
                tok[pl.ds(HALO + side * (rows // 2), rows // 2), :],
                wst[...],
                (((1,), (1,)), ((), ())),
                preferred_element_type=F32,
            )
            for side in range(2)
        ],
        axis=0,
    )
    tail = jnp.exp(-jnp.abs(step))
    up = 1.0 + tail
    log1p = jnp.where(up == 1.0, tail, jnp.log(up) * (tail / jnp.where(up == 1.0, 1.0, up - 1.0)))
    dt = jnp.maximum(step, 0.0) + log1p
    log_a = dt * (-LOG2E * jnp.exp(decay_log[...]))
    dt_ref[...] = jnp.zeros_like(dt_ref)
    terms[...] = jnp.zeros_like(terms)
    dt_ref[:, pl.ds(0, heads)] = dt
    for t, term in enumerate(split(log_a, 3)):
        for k in range(spans):
            terms[pl.ds(t * SPAN, SPAN), pl.ds(k * SPAN, heads)] = term[k * SPAN : (k + 1) * SPAN]
    tri = jnp.where(lane <= sub, 1.0, 0.0).astype(BF16)
    cums = dot(jnp.concatenate([tri, tri, tri], axis=1), terms[...])
    head_of = lax.broadcasted_iota(jnp.int32, (SPAN, width), 1) // HEADDIM
    onto = jnp.where(head_of == lax.broadcasted_iota(jnp.int32, (SPAN, width), 0), 1.0, 0.0)
    spread[pl.ds(0, SPAN), :] = onto.astype(BF16)
    spread[pl.ds(SPAN, SPAN), :] = onto.astype(BF16)
    ends = []
    for k in range(spans):
        at = pl.ds(k * SPAN, SPAN)
        cum = cums[:, k * SPAN : (k + 1) * SPAN]
        cum_ref[at, :] = cum
        end_w = jnp.exp2(jnp.minimum(cum[SPAN - 1 :, :] - cum, 0.0)) * dt_ref[at, :]
        ends.append(jnp.concatenate(split(end_w, 2), axis=1))
    w_end[...] = dot(jnp.concatenate(ends, axis=0), spread[...])

    def gate_store(v, cols):
        gate[:, cols] = silu(v.astype(BF16).astype(F32))

    order = [wides * WIDE + j * SPAN for j in range(rest // SPAN)]
    order += [j * SPAN for j in range(wides * WIDE // SPAN)]
    per_side = len(order) // 2
    place = {col: divmod(n, per_side) for n, col in enumerate(order)}
    my_tile = r // 2
    my_side = lax.rem(r, 2)
    chips = seqs // 2

    def dec_copy(i, src, side, chip):
        return far_copy(
            dec_send.at[side],
            dec_recv.at[src],
            dec_ss.at[side * chips + i],
            dec_rs.at[src],
            chip * 2 + side,
            g,
        )

    def st_copy(i, src, side, chip):
        return far_copy(
            st_send.at[side, chip],
            st_recv.at[src],
            st_ss.at[side * chips + i],
            st_rs.at[src],
            chip * 2 + side,
            g,
        )

    def pf_copy(i, src_side, src_tile, side, chip):
        return far_copy(
            pf_send.at[chip * 2 + side],
            pf_recv.at[src_side, src_tile],
            pf_ss.at[side * chips + i],
            pf_rs.at[src_tile * 2 + src_side],
            chip * 2 + side,
            g,
        )

    def chip_at(i):
        chip = my_tile + i
        return jnp.where(chip >= chips, chip - chips, chip)

    def to_side(side, act):
        def one(i, carry):
            act(i, chip_at(i))
            return carry

        lax.fori_loop(1, chips, one, 0)

        @pl.when(my_side != side)
        def _():
            act(0, my_tile)

    total = jnp.zeros((1, SPAN), F32)
    for k in range(spans):
        total = total + cum_ref[pl.ds(k * SPAN + SPAN - 1, 1), :]
    total = jnp.exp2(total)
    for col, (side, n) in place.items():
        p = col // SPAN
        dec_send[side, :, pl.ds(n * SPAN, SPAN)] = jnp.where(
            low_row,
            jnp.broadcast_to(total[:, 2 * p : 2 * p + 1], (1, SPAN)),
            jnp.broadcast_to(total[:, 2 * p + 1 : 2 * p + 2], (1, SPAN)),
        )
    for side in range(2):
        to_side(side, lambda i, chip, side=side: dec_copy(i, r, side, chip).start())
    dec_recv[r] = dec_send[my_side]

    @pl.when(r == 0)
    def _():
        tok[pl.ds(0, HALO), :] = jnp.zeros((HALO, tok.shape[1]), BF16)

    @pl.when(r > 0)
    def _():
        halo.wait_recv()

    @pl.when(r < seqs - 1)
    def _():
        halo.wait_send()

    def raw_chunk(q):
        v = dot(tok[...], wa[q]).astype(BF16).astype(F32)
        for j in range(WIDE // SPAN):
            raw[q, j] = v[:, j * SPAN : (j + 1) * SPAN]

    def conv(q, j, taps, offset, col, dst):
        cols = pl.ds(col, SPAN)
        for b in range(rows // BLOCK):
            acc = offset[:, cols]
            for k in range(KERNEL):
                at = pl.ds(HALO - KERNEL + 1 + k + b * BLOCK, BLOCK)
                acc = acc + taps[pl.ds(k, 1), cols] * raw[q, j, at, :]
            dst[pl.ds(b * BLOCK, BLOCK), cols] = silu(acc).astype(BF16)

    tiles = STATE // 8

    def local_state(col):
        cols = pl.ds(col, SPAN)
        p = col // SPAN
        side, n = place[col]
        held = jnp.zeros((STATE, SPAN), F32)
        for k in range(spans):
            own = pl.ds(k * SPAN, SPAN)
            last = jnp.exp2(cum_ref[pl.ds(k * SPAN + SPAN - 1, 1), :])
            d = jnp.where(
                low_row,
                jnp.broadcast_to(last[:, 2 * p : 2 * p + 1], (1, SPAN)),
                jnp.broadcast_to(last[:, 2 * p + 1 : 2 * p + 2], (1, SPAN)),
            )
            prior[k, :, cols] = held.astype(BF16)
            scaled = (xs_ref[own, cols].astype(F32) * w_end[own, cols]).astype(BF16)
            held = d * held + dot(wt_ref[k], scaled)
        st_send[side, :, :, pl.ds(n * SPAN, SPAN)] = held.reshape(tiles, 8, SPAN).astype(LINK)
        if n == per_side - 1:
            to_side(side, lambda i, chip: st_copy(i, r, side, chip).start())

            @pl.when(my_side == side)
            def _():
                st_recv[r] = st_send[side, my_tile]

    wbc_load.wait()
    wr_load.wait()
    raw_chunk(0)
    wi_load[0].wait()
    wl_load.start()
    for copy in wg_load:
        copy.start()
    raw_chunk(1)
    for j in range(2 * STATE // SPAN):
        conv(0, j, conv_b, off_b, j * SPAN, bc_ref)
    for k in range(spans):
        wt_ref[k] = bc_ref[pl.ds(k * SPAN, SPAN), pl.ds(0, STATE)].astype(F32).T.astype(BF16)
    for j in range(rest // SPAN):
        conv(0, 2 * STATE // SPAN + j, conv_i, off_i, wides * WIDE + j * SPAN, xs_ref)
        local_state(wides * WIDE + j * SPAN)
    wi_load[1].wait()
    for copy in wo_load:
        copy.start()
    raw_chunk(2)
    for q in range(wides):
        for j in range(WIDE // SPAN):
            conv(1 + q, j, conv_i, off_i, q * WIDE + j * SPAN, xs_ref)
            local_state(q * WIDE + j * SPAN)

    def within(k, carry):
        at = pl.ds(pl.multiple_of(k * SPAN, SPAN), SPAN)
        cum = cum_ref[at, :]
        cum_t = cum.T
        dt_t = dt_ref[at, :].T
        read = bc_ref[at, pl.ds(STATE, STATE)]
        write_t = wt_ref[k]
        scores = jnp.where(lane <= sub, dot(read, write_t), 0.0)
        base = carry
        for p in range(pairs):
            cols = pl.ds(p * SPAN, SPAN)
            x = xs_ref[at, cols]
            shown = []
            weights = []
            for h in (2 * p, 2 * p + 1):
                spread = jnp.broadcast_to(cum[:, h : h + 1], (SPAN, SPAN))
                shown.append(spread)
                gap = jnp.minimum(spread - cum_t[h : h + 1, :], 0.0)
                weights.append((scores * jnp.exp2(gap) * dt_t[h : h + 1, :]).astype(BF16))
            zero = jnp.zeros_like(x)
            both = jnp.concatenate([jnp.where(low, x, zero), jnp.where(low, zero, x)], axis=0)
            intra = dot(jnp.concatenate(weights, axis=1), both)
            scale = jnp.exp2(jnp.where(low, shown[0], shown[1]))
            inter = scale * dot(read, prior[k, :, cols])
            ahead = jnp.exp2(
                jnp.where(
                    low_row,
                    jnp.broadcast_to(base[:, 2 * p : 2 * p + 1], (1, SPAN)),
                    jnp.broadcast_to(base[:, 2 * p + 1 : 2 * p + 2], (1, SPAN)),
                )
            )
            gain = jnp.where(
                low_row,
                jnp.broadcast_to(skip[:, 2 * p : 2 * p + 1], (1, SPAN)),
                jnp.broadcast_to(skip[:, 2 * p + 1 : 2 * p + 2], (1, SPAN)),
            )
            opened = gate[at, cols]
            part_a[at, cols] = (intra + inter + gain * x.astype(F32)) * opened
            part_b[at, cols] = scale * ahead * opened
        return base + cum[SPAN - 1 :, :]

    def own_scan(side):
        @pl.when(my_side == side)
        def _():
            def arrived(src):
                far = far_copy(
                    st_send.at[side, 0], st_recv.at[src], st_ss.at[0], st_rs.at[src], r, g
                )
                near = far_copy(
                    dec_send.at[side], dec_recv.at[src], dec_ss.at[0], dec_rs.at[src], r, g
                )
                far.wait_recv()
                near.wait_recv()

            def await_state(i, carry):
                chip = chip_at(i)
                arrived(chip * 2)
                arrived(chip * 2 + 1)
                return carry

            lax.fori_loop(1, chips, await_state, 0)
            arrived(my_tile * 2 + (1 - side))

            def scan(d, carry):
                pf_send[d] = carry.astype(LINK)
                return dec_recv[d] * carry + st_recv[d].astype(F32)

            lax.fori_loop(0, seqs, scan, jnp.zeros((8, half), F32))
            for other in range(2):
                to_side(
                    other,
                    lambda i, chip, other=other: pf_copy(i, side, my_tile, other, chip).start(),
                )
            pf_recv[side, my_tile] = pf_send[r]

    def gate_wide(c):
        wg_load[c].wait()
        gate_store(dot(tok[own_rows, :], wg[c]), pl.ds(c * WIDE, WIDE))

    gate_wide(0)
    wl_load.wait()
    gate_store(dot(tok[own_rows, :], wl[...]), pl.ds(wides * WIDE, rest))
    own_scan(0)
    gate_wide(1)
    own_scan(1)
    lax.fori_loop(0, spans, within, jnp.zeros((1, SPAN), F32))
    for c in range(2 * chunks):
        wo_load[c].wait()

    def prefix_from(side):
        def await_prefix(i, carry):
            pf_copy(i, side, chip_at(i), 0, 0).wait_recv()
            return carry

        lax.fori_loop(1, chips, await_prefix, 0)

        @pl.when(my_side != side)
        def _():
            pf_copy(0, side, my_tile, 0, 0).wait_recv()

        got = pf_recv[side].astype(F32).reshape(STATE, half).astype(BF16)
        for col, (at, n) in place.items():
            if at == side:
                s_in[:, pl.ds(col, SPAN)] = got[:, n * SPAN : (n + 1) * SPAN]

    prefix_from(0)
    prefix_from(1)

    eye = jnp.where(lane == sub, 1.0, 0.0).astype(F32)

    def gated(slot, block):
        at = pl.ds(pl.multiple_of(block * SPAN, SPAN), SPAN)
        read = bc_ref[at, pl.ds(STATE, STATE)]
        squares = jnp.zeros((SPAN, CHUNK), F32)
        for c in range(chunks):
            cols = pl.ds(c * CHUNK, CHUNK)
            pre = part_a[at, cols] + part_b[at, cols] * dot(read, s_in[:, cols])
            squares = squares + pre * pre
            gw[slot, :, cols] = (pre * norm_w[:, cols]).astype(BF16)
        column = jnp.sum(squares, axis=1, keepdims=True)
        row = jnp.sum(eye * column, axis=0, keepdims=True)
        sq_send[slot] = jnp.broadcast_to(row, (8, SPAN))

    def sq_copy(slot, offset):
        return far_copy(
            sq_send.at[slot],
            sq_recv.at[offset - 1],
            sq_ss.at[offset - 1],
            sq_rs.at[offset - 1],
            r,
            lax.rem(g + offset, parts),
        )

    def stream(send, recv, ss, rs, c, way):
        at = way * chunks + c
        return far_copy(
            send.at[at], recv.at[at], ss.at[at], rs.at[at], r, (right, left)[way]
        )

    def far_step(c, carry):
        for way in range(2):
            far_send[way * chunks + c] = dot(gw[0], wo[way * chunks + c]).astype(BF16)
            stream(far_send, far_recv, far_ss, far_rs, c, way).start()
        return carry

    def own_step(c, carry):
        for way in range(2):
            own_send[way * chunks + c] = dot(gw[1 + way], wo[(1 - way) * chunks + c]).astype(BF16)
            stream(own_send, own_recv, own_ss, own_rs, c, way).start()
        return carry

    def mine_step(c, carry):
        mine[c] = dot(gw[3], wo[c])
        return carry

    def comb_step(c, carry):
        for way in range(2):
            at = way * chunks + c
            value = dot(gw[1 + way], wo[at])
            stream(far_send, far_recv, far_ss, far_rs, c, way).wait_recv()
            comb_send[at] = (value + far_recv[at].astype(F32)).astype(BF16)
            stream(comb_send, comb_recv, comb_ss, comb_rs, c, way).start()
        return carry

    gated(0, across)
    sq_copy(0, 2).start()
    lax.fori_loop(0, chunks, far_step, 0)
    gated(1, right)
    sq_copy(1, 1).start()
    gated(2, left)
    sq_copy(2, 3).start()
    lax.fori_loop(0, chunks, own_step, 0)
    gated(3, g)
    lax.fori_loop(0, 2 * chunks, mine_step, 0)
    lax.fori_loop(0, chunks, comb_step, 0)

    def drain(c, carry):
        for way in range(2):
            stream(far_send, far_recv, far_ss, far_rs, c, way).wait_send()
            stream(own_send, own_recv, own_ss, own_rs, c, way).wait_send()
        return carry

    def drain_comb(c, carry):
        for way in range(2):
            stream(comb_send, comb_recv, comb_ss, comb_rs, c, way).wait_send()
        return carry

    for side in range(2):

        def sent(i, chip, side=side):
            dec_copy(i, r, side, chip).wait_send()
            st_copy(i, r, side, chip).wait_send()
            pf_copy(i, 0, 0, side, chip).wait_send()

        to_side(side, sent)
    for slot, offset in ((1, 1), (0, 2), (2, 3)):
        sq_copy(slot, offset).wait_send()
    lax.fori_loop(0, chunks, drain, 0)

    squares = sq_send[3]
    for slot, offset in ((1, 1), (0, 2), (2, 3)):
        sq_copy(slot, offset).wait_recv()
        squares = squares + sq_recv[offset - 1]
    scale_row = 1.0 / jnp.sqrt(squares[:1] * (1.0 / inner_all) + EPS)
    scale = jnp.sum(eye * scale_row, axis=1, keepdims=True)

    for c in range(chunks):
        stream(own_send, own_recv, own_ss, own_rs, c, 1).wait_recv()
        stream(comb_send, comb_recv, comb_ss, comb_rs, c, 0).wait_recv()
        value = mine[c] + own_recv[chunks + c].astype(F32) + comb_recv[c].astype(F32)
        out[:, pl.ds(c * CHUNK, CHUNK)] = (value * scale).astype(BF16)
        stream(own_send, own_recv, own_ss, own_rs, c, 0).wait_recv()
        stream(comb_send, comb_recv, comb_ss, comb_rs, c, 1).wait_recv()
        value = mine[chunks + c] + own_recv[c].astype(F32) + comb_recv[chunks + c].astype(F32)
        out[:, pl.ds((chunks + c) * CHUNK, CHUNK)] = (value * scale).astype(BF16)

    lax.fori_loop(0, chunks, drain_comb, 0)


def per_device(
    seqs,
    parts,
    tokens,
    proj_inner,
    proj_gate,
    proj_bc,
    proj_step,
    conv_inner,
    conv_bc,
    offset_inner,
    offset_bc,
    step_bias,
    decay_log,
    skip_gain,
    norm_weight,
    out_weight,
):
    rows, depth = tokens.shape
    width = proj_inner.shape[1]
    heads = step_bias.shape[0]
    chunks = width // CHUNK
    spans = rows // SPAN
    half = width // 2
    tiles = STATE // 8
    model = out_weight.shape[1]
    any_spec = pl.BlockSpec(memory_space=pl.ANY)
    vmem = pl.BlockSpec(memory_space=pltpu.VMEM)
    dma = pltpu.SemaphoreType.DMA
    streams = [pltpu.VMEM((2 * chunks, SPAN, CHUNK), BF16)] * 6
    scratch = [
        pltpu.VMEM((KERNEL, width), F32),
        pltpu.VMEM((KERNEL, 2 * STATE), F32),
        pltpu.VMEM((width,), F32),
        pltpu.VMEM((1, 2 * STATE), F32),
        pltpu.VMEM((1, heads), F32),
        pltpu.VMEM((1, heads), F32),
        pltpu.VMEM((1, heads), F32),
        pltpu.VMEM((width,), F32),
        pltpu.VMEM((rows + HALO, depth), BF16),
        pltpu.VMEM((1 + width // WIDE, depth, WIDE), BF16),
        pltpu.VMEM((width // WIDE, depth, WIDE), BF16),
        pltpu.VMEM((depth, width % WIDE), BF16),
        pltpu.VMEM((heads, depth), BF16),
        pltpu.VMEM((2 * chunks, width, CHUNK), BF16),
        pltpu.VMEM((1 + width // WIDE, WIDE // SPAN, rows + HALO, SPAN), F32),
        pltpu.VMEM((3 * SPAN, spans * SPAN), BF16),
        pltpu.VMEM((2 * SPAN, width), BF16),
        pltpu.VMEM((rows, width), F32),
        pltpu.VMEM((rows, width), BF16),
        pltpu.VMEM((rows, 2 * STATE), BF16),
        pltpu.VMEM((spans, STATE, SPAN), BF16),
        pltpu.VMEM((rows, SPAN), F32),
        pltpu.VMEM((rows, SPAN), F32),
        pltpu.VMEM((rows, width), F32),
        pltpu.VMEM((rows, width), F32),
        pltpu.VMEM((rows, width), F32),
        pltpu.VMEM((spans, STATE, width), BF16),
        pltpu.VMEM((2, tiles, 8, half), LINK),
        pltpu.VMEM((seqs, 8, half), LINK),
        pltpu.VMEM((2, 1, half), F32),
        pltpu.VMEM((seqs, 1, half), F32),
        pltpu.VMEM((seqs, 8, half), LINK),
        pltpu.VMEM((2, tiles, 8, half), LINK),
        pltpu.VMEM((STATE, width), BF16),
        pltpu.VMEM((4, SPAN, width), BF16),
        *streams,
        pltpu.VMEM((2 * chunks, SPAN, CHUNK), F32),
        pltpu.VMEM((4, 8, SPAN), F32),
        pltpu.VMEM((3, 8, SPAN), F32),
        dma((5 + 2 * (width // WIDE) + 2 * chunks,)),
        dma((8,)),
        dma((2,)),
        *[dma((seqs,))] * 6,
        *[dma((2 * chunks,))] * 6,
        dma((3,)),
        dma((3,)),
    ]
    row = lambda v: v.reshape(1, -1)
    return pl.pallas_call(
        functools.partial(kernel, seqs, parts, float(parts * width)),
        out_shape=pltpu.VMEM((rows // parts, model), BF16),
        in_specs=[any_spec] * 14,
        out_specs=vmem,
        scratch_shapes=scratch,
        compiler_params=pltpu.CompilerParams(
            collective_id=0, has_side_effects=True, vmem_limit_bytes=62 * 1024 * 1024
        ),
    )(
        tokens,
        proj_inner,
        proj_gate,
        proj_bc,
        proj_step.T,
        conv_inner,
        conv_bc,
        offset_inner,
        row(offset_bc),
        row(step_bias),
        row(decay_log),
        row(skip_gain),
        norm_weight,
        out_weight,
    )


def solution(mesh):
    body = functools.partial(per_device, mesh.shape["seq"], mesh.shape["head"])
    return jax.shard_map(
        body,
        mesh=mesh,
        in_specs=(
            P("seq", None),
            P(None, "head"),
            P(None, "head"),
            P(),
            P(None, "head"),
            P(None, "head"),
            P(),
            P("head"),
            P(),
            P("head"),
            P("head"),
            P("head"),
            P("head"),
            P("head", None),
        ),
        out_specs=P(("seq", "head"), None),
        check_vma=False,
    )
```

```python
import functools

import jax
import jax.numpy as jnp
from jax import lax
from jax.experimental import pallas as pl
from jax.experimental.pallas import tpu as pltpu
from jax.sharding import PartitionSpec as P

HEADDIM = 64
STATE = 128
KERNEL = 4
SPAN = 128
HALO = 8
CHUNK = 256
BLOCK = 64
WIDE = 512
LOG2E = 1.4426950408889634
EPS = 0.25
MESH = pl.DeviceIdType.MESH
F32 = jnp.float32
BF16 = jnp.bfloat16
LINK = jnp.bfloat16


def silu(v):
    return v / (1.0 + jnp.exp(-v))


def dot(a, b):
    return jnp.dot(a, b, preferred_element_type=F32)


def split(v, count):
    terms = []
    for _ in range(count):
        terms.append(v.astype(BF16))
        v = v - terms[-1].astype(F32)
    return terms


def kernel(
    seqs,
    parts,
    inner_all,
    tokens_hbm,
    wi_hbm,
    wg_hbm,
    wbc_hbm,
    wst_hbm,
    conv_i_hbm,
    conv_b_hbm,
    off_i_hbm,
    off_b_hbm,
    bias_hbm,
    decay_log_hbm,
    skip_hbm,
    norm_hbm,
    wo_hbm,
    out,
    conv_i,
    conv_b,
    off_1,
    off_b,
    bias,
    decay_log,
    skip,
    norm_1,
    tok,
    wa,
    wg,
    wl,
    wst,
    wo,
    raw,
    terms,
    spread,
    w_end,
    xs_ref,
    bc_ref,
    wt_ref,
    cum_ref,
    dt_ref,
    gate,
    part_a,
    part_b,
    prior,
    st_send,
    st_recv,
    dec_send,
    dec_recv,
    pf_send,
    pf_recv,
    s_in,
    held_scan,
    gw,
    far_send,
    far_recv,
    own_send,
    own_recv,
    comb_send,
    comb_recv,
    mine,
    sq_send,
    sq_recv,
    load_sem,
    small_sem,
    halo_sem,
    dec_ss,
    dec_rs,
    st_ss,
    st_rs,
    pf_ss,
    pf_rs,
    far_ss,
    far_rs,
    own_ss,
    own_rs,
    comb_ss,
    comb_rs,
    sq_ss,
    sq_rs,
):
    r = lax.axis_index("seq")
    g = lax.axis_index("head")
    rows = tokens_hbm.shape[0]
    width = wi_hbm.shape[1]
    spans = rows // SPAN
    heads = width // HEADDIM
    pairs = heads // 2
    chunks = width // CHUNK
    half = width // 2
    right = lax.rem(g + 1, parts)
    left = lax.rem(g + parts - 1, parts)
    across = lax.rem(g + 2, parts)

    def loaded(src, dst, number):
        return pltpu.make_async_copy(src, dst, load_sem.at[number])

    wides = width // WIDE
    rest = width - wides * WIDE
    tok_load = loaded(tokens_hbm, tok, 0)
    wst_load = loaded(wst_hbm, wst, 1)
    wl_load = loaded(wg_hbm.at[:, pl.ds(wides * WIDE, rest)], wl, 2)
    wbc_load = loaded(wbc_hbm, wa.at[0, :, pl.ds(0, 2 * STATE)], 3)
    wr_load = loaded(
        wi_hbm.at[:, pl.ds(wides * WIDE, rest)], wa.at[0, :, pl.ds(2 * STATE, rest)], 4
    )
    wi_load = [
        loaded(wi_hbm.at[:, pl.ds(c * WIDE, WIDE)], wa.at[1 + c], 5 + c) for c in range(wides)
    ]
    wg_load = [
        loaded(wg_hbm.at[:, pl.ds(c * WIDE, WIDE)], wg.at[c], 5 + wides + c) for c in range(wides)
    ]
    wo_load = [
        loaded(wo_hbm.at[:, pl.ds(c * CHUNK, CHUNK)], wo.at[c], 5 + 2 * wides + c)
        for c in range(2 * chunks)
    ]
    small_load = [
        pltpu.make_async_copy(src, dst, small_sem.at[i])
        for i, (src, dst) in enumerate(
            (
                (bias_hbm, bias),
                (decay_log_hbm, decay_log),
                (conv_b_hbm, conv_b),
                (off_b_hbm, off_b),
                (conv_i_hbm, conv_i),
                (off_i_hbm, off_1),
                (skip_hbm, skip),
                (norm_hbm, norm_1),
            )
        )
    ]
    tok_load.start()
    for copy in small_load:
        copy.start()
    wst_load.start()
    wbc_load.start()
    wr_load.start()

    barrier = pltpu.get_barrier_semaphore()

    def greet_seq(i, carry):
        pl.semaphore_signal(
            barrier,
            inc=1,
            device_id={"seq": lax.rem(r + i, seqs), "head": g},
            device_id_type=MESH,
        )
        return carry

    lax.fori_loop(1, seqs, greet_seq, 0)
    for other in (right, left, across):
        pl.semaphore_signal(
            barrier, inc=1, device_id={"seq": r, "head": other}, device_id_type=MESH
        )

    def far_copy(src, dst, ss, rs, seq, head):
        return pltpu.make_async_remote_copy(
            src_ref=src,
            dst_ref=dst,
            send_sem=ss,
            recv_sem=rs,
            device_id={"seq": seq, "head": head},
            device_id_type=MESH,
        )

    lane = lax.broadcasted_iota(jnp.int32, (SPAN, SPAN), 1)
    sub = lax.broadcasted_iota(jnp.int32, (SPAN, SPAN), 0)
    low = lane < HEADDIM
    low_row = low[:1]
    head_of = lax.broadcasted_iota(jnp.int32, (SPAN, width), 1) // HEADDIM
    onto = jnp.where(head_of == lax.broadcasted_iota(jnp.int32, (SPAN, width), 0), 1.0, 0.0)
    spread[pl.ds(0, SPAN), :] = onto.astype(BF16)
    spread[pl.ds(SPAN, SPAN), :] = onto.astype(BF16)
    terms[...] = jnp.zeros_like(terms)
    dt_ref[...] = jnp.zeros_like(dt_ref)
    wst_load.wait()
    tok_load.wait()
    for copy in wi_load:
        copy.start()
    for side in range(2):
        at = pl.ds(side * (rows // 2), rows // 2)
        dt_ref[at, pl.ds(0, heads)] = lax.dot_general(
            tok[at, :], wst[...], (((1,), (1,)), ((), ())), preferred_element_type=F32
        )

    def raw_chunk(q):
        v = dot(tok[...], wa[q]).astype(BF16).astype(F32)
        for j in range(WIDE // SPAN):
            raw[q, j, pl.ds(HALO, rows), :] = v[:, j * SPAN : (j + 1) * SPAN]

    wbc_load.wait()
    wr_load.wait()
    raw_chunk(0)
    for q in range(wides):
        wi_load[q].wait()
        raw_chunk(1 + q)
    wl_load.start()
    for copy in wg_load:
        copy.start()
    for copy in wo_load:
        copy.start()

    pl.semaphore_wait(barrier, seqs + 2)

    edges = [
        far_copy(
            raw.at[q, :, pl.ds(rows, HALO), :],
            raw.at[q, :, pl.ds(0, HALO), :],
            halo_sem.at[q],
            halo_sem.at[1 + wides + q],
            lax.rem(r + 1, seqs),
            g,
        )
        for q in range(1 + wides)
    ]

    @pl.when(r < seqs - 1)
    def _():
        for edge in edges:
            edge.start()

    for copy in small_load:
        copy.wait()
    off_i = off_1[...].reshape(1, -1)
    norm_w = norm_1[...].reshape(1, -1)

    step = dt_ref[:, pl.ds(0, heads)] + bias[...]
    tail = jnp.exp(-jnp.abs(step))
    up = 1.0 + tail
    log1p = jnp.where(up == 1.0, tail, jnp.log(up) * (tail / jnp.where(up == 1.0, 1.0, up - 1.0)))
    dt = jnp.maximum(step, 0.0) + log1p
    log_a = dt * (-LOG2E * jnp.exp(decay_log[...]))
    dt_ref[:, pl.ds(0, heads)] = dt
    for t, term in enumerate(split(log_a, 3)):
        for k in range(spans):
            terms[pl.ds(t * SPAN, SPAN), pl.ds(k * SPAN, heads)] = term[k * SPAN : (k + 1) * SPAN]
    tri = jnp.where(lane <= sub, 1.0, 0.0).astype(BF16)
    cums = dot(jnp.concatenate([tri, tri, tri], axis=1), terms[...])
    ends = []
    for k in range(spans):
        at = pl.ds(k * SPAN, SPAN)
        cum = cums[:, k * SPAN : (k + 1) * SPAN]
        cum_ref[at, :] = cum
        end_w = jnp.exp2(jnp.minimum(cum[SPAN - 1 :, :] - cum, 0.0)) * dt_ref[at, :]
        ends.append(jnp.concatenate(split(end_w, 2), axis=1))
    w_end[...] = dot(jnp.concatenate(ends, axis=0), spread[...])

    def gate_store(v, cols):
        gate[:, cols] = silu(v.astype(BF16).astype(F32))

    order = [wides * WIDE + j * SPAN for j in range(rest // SPAN)]
    order += [j * SPAN for j in range(wides * WIDE // SPAN)]
    per_side = len(order) // 2
    place = {col: divmod(n, per_side) for n, col in enumerate(order)}
    my_tile = r // 2
    my_side = lax.rem(r, 2)
    chips = seqs // 2

    def dec_copy(dst):
        return far_copy(
            dec_send.at[lax.rem(dst, 2)], dec_recv.at[r], dec_ss.at[dst], dec_rs.at[r], dst, g
        )

    def st_copy(side, chip):
        dst = chip * 2 + side
        return far_copy(
            st_send.at[side, chip], st_recv.at[r], st_ss.at[dst], st_rs.at[r], dst, g
        )

    def pf_copy(dst):
        return far_copy(
            pf_send.at[dst], pf_recv.at[my_side, my_tile], pf_ss.at[dst], pf_rs.at[r], dst, g
        )

    def each(first, last, act):
        def one(d, carry):
            @pl.when(d != r)
            def _():
                act(d)

            return carry

        lax.fori_loop(first, last, one, 0)

    def to_side(side, act):
        def one(i, carry):
            chip = my_tile + i
            act(side, jnp.where(chip >= chips, chip - chips, chip))
            return carry

        lax.fori_loop(1, chips, one, 0)

        @pl.when(my_side != side)
        def _():
            act(side, my_tile)

    total = jnp.zeros((1, SPAN), F32)
    for k in range(spans):
        total = total + cum_ref[pl.ds(k * SPAN + SPAN - 1, 1), :]
    total = jnp.exp2(total)
    for col, (side, n) in place.items():
        p = col // SPAN
        dec_send[side, :, pl.ds(n * SPAN, SPAN)] = jnp.where(
            low_row,
            jnp.broadcast_to(total[:, 2 * p : 2 * p + 1], (1, SPAN)),
            jnp.broadcast_to(total[:, 2 * p + 1 : 2 * p + 2], (1, SPAN)),
        )
    each(0, seqs, lambda d: dec_copy(d).start())
    dec_recv[r] = dec_send[my_side]

    @pl.when(r == 0)
    def _():
        raw[:, :, pl.ds(0, HALO), :] = jnp.zeros((1 + wides, WIDE // SPAN, HALO, SPAN), F32)

    @pl.when(r > 0)
    def _():
        for edge in edges:
            edge.wait_recv()

    def conv(q, j, taps, offset, col, dst):
        cols = pl.ds(col, SPAN)
        for b in range(rows // BLOCK):
            acc = offset[:, cols]
            for k in range(KERNEL):
                at = pl.ds(HALO - KERNEL + 1 + k + b * BLOCK, BLOCK)
                acc = acc + taps[pl.ds(k, 1), cols] * raw[q, j, at, :]
            dst[pl.ds(b * BLOCK, BLOCK), cols] = silu(acc).astype(BF16)

    tiles = STATE // 8

    def local_state(col):
        cols = pl.ds(col, SPAN)
        p = col // SPAN
        side, n = place[col]
        held = jnp.zeros((STATE, SPAN), F32)
        for k in range(spans):
            own = pl.ds(k * SPAN, SPAN)
            last = jnp.exp2(cum_ref[pl.ds(k * SPAN + SPAN - 1, 1), :])
            d = jnp.where(
                low_row,
                jnp.broadcast_to(last[:, 2 * p : 2 * p + 1], (1, SPAN)),
                jnp.broadcast_to(last[:, 2 * p + 1 : 2 * p + 2], (1, SPAN)),
            )
            prior[k, :, cols] = held.astype(BF16)
            scaled = (xs_ref[own, cols].astype(F32) * w_end[own, cols]).astype(BF16)
            held = d * held + dot(wt_ref[k], scaled)
        st_send[side, :, :, pl.ds(n * SPAN, SPAN)] = held.reshape(tiles, 8, SPAN).astype(LINK)
        if n == per_side - 1:
            to_side(side, lambda at, chip: st_copy(at, chip).start())

            @pl.when(my_side == side)
            def _():
                st_recv[r] = st_send[side, my_tile]

    for j in range(2 * STATE // SPAN):
        conv(0, j, conv_b, off_b, j * SPAN, bc_ref)
    for k in range(spans):
        wt_ref[k] = bc_ref[pl.ds(k * SPAN, SPAN), pl.ds(0, STATE)].astype(F32).T.astype(BF16)
    for j in range(rest // SPAN):
        conv(0, 2 * STATE // SPAN + j, conv_i, off_i, wides * WIDE + j * SPAN, xs_ref)
        local_state(wides * WIDE + j * SPAN)
    for q in range(wides):
        for j in range(WIDE // SPAN):
            conv(1 + q, j, conv_i, off_i, q * WIDE + j * SPAN, xs_ref)
            local_state(q * WIDE + j * SPAN)

    def within(k, carry):
        at = pl.ds(pl.multiple_of(k * SPAN, SPAN), SPAN)
        cum = cum_ref[at, :]
        cum_t = cum.T
        dt_t = dt_ref[at, :].T
        read = bc_ref[at, pl.ds(STATE, STATE)]
        write_t = wt_ref[k]
        scores = jnp.where(lane <= sub, dot(read, write_t), 0.0)
        base = carry
        for p in range(pairs):
            cols = pl.ds(p * SPAN, SPAN)
            x = xs_ref[at, cols]
            shown = []
            weights = []
            for h in (2 * p, 2 * p + 1):
                spread = jnp.broadcast_to(cum[:, h : h + 1], (SPAN, SPAN))
                shown.append(spread)
                gap = jnp.minimum(spread - cum_t[h : h + 1, :], 0.0)
                weights.append((scores * jnp.exp2(gap) * dt_t[h : h + 1, :]).astype(BF16))
            zero = jnp.zeros_like(x)
            both = jnp.concatenate([jnp.where(low, x, zero), jnp.where(low, zero, x)], axis=0)
            intra = dot(jnp.concatenate(weights, axis=1), both)
            scale = jnp.exp2(jnp.where(low, shown[0], shown[1]))
            inter = scale * dot(read, prior[k, :, cols])
            ahead = jnp.exp2(
                jnp.where(
                    low_row,
                    jnp.broadcast_to(base[:, 2 * p : 2 * p + 1], (1, SPAN)),
                    jnp.broadcast_to(base[:, 2 * p + 1 : 2 * p + 2], (1, SPAN)),
                )
            )
            gain = jnp.where(
                low_row,
                jnp.broadcast_to(skip[:, 2 * p : 2 * p + 1], (1, SPAN)),
                jnp.broadcast_to(skip[:, 2 * p + 1 : 2 * p + 2], (1, SPAN)),
            )
            opened = gate[at, cols]
            part_a[at, cols] = (intra + inter + gain * x.astype(F32)) * opened
            part_b[at, cols] = scale * ahead * opened
        return base + cum[SPAN - 1 :, :]

    def own_scan(first, last):
        def arrived(src):
            far_copy(
                dec_send.at[my_side], dec_recv.at[src], dec_ss.at[src], dec_rs.at[src], src, g
            ).wait_recv()
            far_copy(
                st_send.at[my_side, 0], st_recv.at[src], st_ss.at[src], st_rs.at[src], src, g
            ).wait_recv()

        each(first, last, arrived)

        def scan(d, carry):
            pf_send[d] = carry.astype(LINK)
            return dec_recv[d] * carry + st_recv[d].astype(F32)

        start = jnp.zeros((8, half), F32) if first == 0 else held_scan[...]
        held_scan[...] = lax.fori_loop(first, last, scan, start)
        each(first, last, lambda d: pf_copy(d).start())

        @pl.when((r >= first) & (r < last))
        def _():
            pf_recv[my_side, my_tile] = pf_send[r]

    def gate_wide(c):
        wg_load[c].wait()
        gate_store(dot(tok[...], wg[c]), pl.ds(c * WIDE, WIDE))

    late = r >= seqs // 2

    @pl.when(late)
    def _():
        own_scan(0, seqs // 2)

    wl_load.wait()
    gate_store(dot(tok[...], wl[...]), pl.ds(wides * WIDE, rest))
    gate_wide(0)
    gate_wide(1)

    @pl.when(late)
    def _():
        own_scan(seqs // 2, seqs)

    @pl.when(jnp.logical_not(late))
    def _():
        own_scan(0, seqs // 2)

    lax.fori_loop(0, spans, within, jnp.zeros((1, SPAN), F32))

    @pl.when(jnp.logical_not(late))
    def _():
        own_scan(seqs // 2, seqs)

    for c in range(2 * chunks):
        wo_load[c].wait()

    def prefix_arrived(src):
        far_copy(
            pf_send.at[0],
            pf_recv.at[lax.rem(src, 2), src // 2],
            pf_ss.at[src],
            pf_rs.at[src],
            src,
            g,
        ).wait_recv()

    each(0, seqs, prefix_arrived)
    for side in range(2):
        got = pf_recv[side].astype(F32).reshape(STATE, half).astype(BF16)
        for col, (at, n) in place.items():
            if at == side:
                s_in[:, pl.ds(col, SPAN)] = got[:, n * SPAN : (n + 1) * SPAN]

    eye = jnp.where(lane == sub, 1.0, 0.0).astype(F32)

    def gated(slot, block):
        at = pl.ds(pl.multiple_of(block * SPAN, SPAN), SPAN)
        read = bc_ref[at, pl.ds(STATE, STATE)]
        squares = jnp.zeros((SPAN, CHUNK), F32)
        for c in range(chunks):
            cols = pl.ds(c * CHUNK, CHUNK)
            pre = part_a[at, cols] + part_b[at, cols] * dot(read, s_in[:, cols])
            squares = squares + pre * pre
            gw[slot, :, cols] = (pre * norm_w[:, cols]).astype(BF16)
        column = jnp.sum(squares, axis=1, keepdims=True)
        row = jnp.sum(eye * column, axis=0, keepdims=True)
        sq_send[slot] = jnp.broadcast_to(row, (8, SPAN))

    def sq_copy(slot, offset):
        return far_copy(
            sq_send.at[slot],
            sq_recv.at[offset - 1],
            sq_ss.at[offset - 1],
            sq_rs.at[offset - 1],
            r,
            lax.rem(g + offset, parts),
        )

    def stream(send, recv, ss, rs, c, way):
        at = way * chunks + c
        return far_copy(
            send.at[at], recv.at[at], ss.at[at], rs.at[at], r, (right, left)[way]
        )

    def far_step(c, carry):
        for way in range(2):
            far_send[way * chunks + c] = dot(gw[0], wo[way * chunks + c]).astype(BF16)
            stream(far_send, far_recv, far_ss, far_rs, c, way).start()
        return carry

    def own_step(c, carry):
        for way in range(2):
            own_send[way * chunks + c] = dot(gw[1 + way], wo[(1 - way) * chunks + c]).astype(BF16)
            stream(own_send, own_recv, own_ss, own_rs, c, way).start()
        return carry

    def mine_step(c, carry):
        mine[c] = dot(gw[3], wo[c])
        return carry

    def comb_step(c, carry):
        for way in range(2):
            at = way * chunks + c
            value = dot(gw[1 + way], wo[at])
            stream(far_send, far_recv, far_ss, far_rs, c, way).wait_recv()
            comb_send[at] = (value + far_recv[at].astype(F32)).astype(BF16)
            stream(comb_send, comb_recv, comb_ss, comb_rs, c, way).start()
        return carry

    gated(0, across)
    sq_copy(0, 2).start()
    lax.fori_loop(0, chunks, far_step, 0)
    gated(1, right)
    sq_copy(1, 1).start()
    gated(2, left)
    sq_copy(2, 3).start()
    lax.fori_loop(0, chunks, own_step, 0)
    gated(3, g)
    lax.fori_loop(0, 2 * chunks, mine_step, 0)
    lax.fori_loop(0, chunks, comb_step, 0)

    def drain(c, carry):
        for way in range(2):
            stream(far_send, far_recv, far_ss, far_rs, c, way).wait_send()
            stream(own_send, own_recv, own_ss, own_rs, c, way).wait_send()
        return carry

    def drain_comb(c, carry):
        for way in range(2):
            stream(comb_send, comb_recv, comb_ss, comb_rs, c, way).wait_send()
        return carry

    def sent(d):
        dec_copy(d).wait_send()
        st_copy(lax.rem(d, 2), d // 2).wait_send()
        pf_copy(d).wait_send()

    each(0, seqs, sent)

    @pl.when(r < seqs - 1)
    def _():
        for edge in edges:
            edge.wait_send()

    for slot, offset in ((1, 1), (0, 2), (2, 3)):
        sq_copy(slot, offset).wait_send()
    lax.fori_loop(0, chunks, drain, 0)

    squares = sq_send[3]
    for slot, offset in ((1, 1), (0, 2), (2, 3)):
        sq_copy(slot, offset).wait_recv()
        squares = squares + sq_recv[offset - 1]
    scale_row = 1.0 / jnp.sqrt(squares[:1] * (1.0 / inner_all) + EPS)
    scale = jnp.sum(eye * scale_row, axis=1, keepdims=True)

    for c in range(chunks):
        stream(own_send, own_recv, own_ss, own_rs, c, 1).wait_recv()
        stream(comb_send, comb_recv, comb_ss, comb_rs, c, 0).wait_recv()
        value = mine[c] + own_recv[chunks + c].astype(F32) + comb_recv[c].astype(F32)
        out[:, pl.ds(c * CHUNK, CHUNK)] = (value * scale).astype(BF16)
        stream(own_send, own_recv, own_ss, own_rs, c, 0).wait_recv()
        stream(comb_send, comb_recv, comb_ss, comb_rs, c, 1).wait_recv()
        value = mine[chunks + c] + own_recv[c].astype(F32) + comb_recv[chunks + c].astype(F32)
        out[:, pl.ds((chunks + c) * CHUNK, CHUNK)] = (value * scale).astype(BF16)

    lax.fori_loop(0, chunks, drain_comb, 0)


def per_device(
    seqs,
    parts,
    tokens,
    proj_inner,
    proj_gate,
    proj_bc,
    proj_step,
    conv_inner,
    conv_bc,
    offset_inner,
    offset_bc,
    step_bias,
    decay_log,
    skip_gain,
    norm_weight,
    out_weight,
):
    rows, depth = tokens.shape
    width = proj_inner.shape[1]
    heads = step_bias.shape[0]
    chunks = width // CHUNK
    spans = rows // SPAN
    half = width // 2
    tiles = STATE // 8
    model = out_weight.shape[1]
    any_spec = pl.BlockSpec(memory_space=pl.ANY)
    vmem = pl.BlockSpec(memory_space=pltpu.VMEM)
    dma = pltpu.SemaphoreType.DMA
    streams = [pltpu.VMEM((2 * chunks, SPAN, CHUNK), BF16)] * 6
    scratch = [
        pltpu.VMEM((KERNEL, width), F32),
        pltpu.VMEM((KERNEL, 2 * STATE), F32),
        pltpu.VMEM((width,), F32),
        pltpu.VMEM((1, 2 * STATE), F32),
        pltpu.VMEM((1, heads), F32),
        pltpu.VMEM((1, heads), F32),
        pltpu.VMEM((1, heads), F32),
        pltpu.VMEM((width,), F32),
        pltpu.VMEM((rows, depth), BF16),
        pltpu.VMEM((1 + width // WIDE, depth, WIDE), BF16),
        pltpu.VMEM((width // WIDE, depth, WIDE), BF16),
        pltpu.VMEM((depth, width % WIDE), BF16),
        pltpu.VMEM((heads, depth), BF16),
        pltpu.VMEM((2 * chunks, width, CHUNK), BF16),
        pltpu.VMEM((1 + width // WIDE, WIDE // SPAN, rows + HALO, SPAN), F32),
        pltpu.VMEM((3 * SPAN, spans * SPAN), BF16),
        pltpu.VMEM((2 * SPAN, width), BF16),
        pltpu.VMEM((rows, width), F32),
        pltpu.VMEM((rows, width), BF16),
        pltpu.VMEM((rows, 2 * STATE), BF16),
        pltpu.VMEM((spans, STATE, SPAN), BF16),
        pltpu.VMEM((rows, SPAN), F32),
        pltpu.VMEM((rows, SPAN), F32),
        pltpu.VMEM((rows, width), F32),
        pltpu.VMEM((rows, width), F32),
        pltpu.VMEM((rows, width), F32),
        pltpu.VMEM((spans, STATE, width), BF16),
        pltpu.VMEM((2, tiles, 8, half), LINK),
        pltpu.VMEM((seqs, 8, half), LINK),
        pltpu.VMEM((2, 1, half), F32),
        pltpu.VMEM((seqs, 1, half), F32),
        pltpu.VMEM((seqs, 8, half), LINK),
        pltpu.VMEM((2, tiles, 8, half), LINK),
        pltpu.VMEM((STATE, width), BF16),
        pltpu.VMEM((8, half), F32),
        pltpu.VMEM((4, SPAN, width), BF16),
        *streams,
        pltpu.VMEM((2 * chunks, SPAN, CHUNK), F32),
        pltpu.VMEM((4, 8, SPAN), F32),
        pltpu.VMEM((3, 8, SPAN), F32),
        dma((5 + 2 * (width // WIDE) + 2 * chunks,)),
        dma((8,)),
        dma((2 + 2 * (width // WIDE),)),
        *[dma((seqs,))] * 6,
        *[dma((2 * chunks,))] * 6,
        dma((3,)),
        dma((3,)),
    ]
    row = lambda v: v.reshape(1, -1)
    return pl.pallas_call(
        functools.partial(kernel, seqs, parts, float(parts * width)),
        out_shape=pltpu.VMEM((rows // parts, model), BF16),
        in_specs=[any_spec] * 14,
        out_specs=vmem,
        scratch_shapes=scratch,
        compiler_params=pltpu.CompilerParams(
            collective_id=0, has_side_effects=True, vmem_limit_bytes=62 * 1024 * 1024
        ),
    )(
        tokens,
        proj_inner,
        proj_gate,
        proj_bc,
        proj_step.T,
        conv_inner,
        conv_bc,
        offset_inner,
        row(offset_bc),
        row(step_bias),
        row(decay_log),
        row(skip_gain),
        norm_weight,
        out_weight,
    )


def solution(mesh):
    body = functools.partial(per_device, mesh.shape["seq"], mesh.shape["head"])
    return jax.shard_map(
        body,
        mesh=mesh,
        in_specs=(
            P("seq", None),
            P(None, "head"),
            P(None, "head"),
            P(),
            P(None, "head"),
            P(None, "head"),
            P(),
            P("head"),
            P(),
            P("head"),
            P("head"),
            P("head"),
            P("head"),
            P("head", None),
        ),
        out_specs=P(("seq", "head"), None),
        check_vma=False,
    )
```

```python
import functools

import jax
import jax.numpy as jnp
from jax import lax
from jax.experimental import pallas as pl
from jax.experimental.pallas import tpu as pltpu
from jax.sharding import PartitionSpec as P

HEADDIM = 64
STATE = 128
KERNEL = 4
SPAN = 128
HALO = 8
CHUNK = 256
BLOCK = 64
WIDE = 512
PIECES = 4
LOG2E = 1.4426950408889634
EPS = 0.25
MESH = pl.DeviceIdType.MESH
F32 = jnp.float32
BF16 = jnp.bfloat16
LINK = jnp.bfloat16


def silu(v):
    return v / (1.0 + jnp.exp(-v))


def dot(a, b):
    return jnp.dot(a, b, preferred_element_type=F32)


def split(v, count):
    terms = []
    for _ in range(count):
        terms.append(v.astype(BF16))
        v = v - terms[-1].astype(F32)
    return terms


def kernel(
    seqs,
    parts,
    inner_all,
    tokens_hbm,
    wi_hbm,
    wg_hbm,
    wbc_hbm,
    wst_hbm,
    conv_i_hbm,
    conv_b_hbm,
    off_i_hbm,
    off_b_hbm,
    bias_hbm,
    decay_log_hbm,
    skip_hbm,
    norm_hbm,
    wo_hbm,
    out,
    conv_i,
    conv_b,
    off_1,
    off_b,
    bias,
    decay_log,
    skip,
    norm_1,
    tok,
    wa,
    wg,
    wl,
    wst,
    wo,
    raw,
    terms,
    spread,
    w_end,
    xs_ref,
    bc_ref,
    wt_ref,
    cum_ref,
    dt_ref,
    gate,
    part_a,
    part_b,
    prior,
    st_send,
    st_recv,
    dec_send,
    dec_recv,
    pf_send,
    pf_recv,
    s_in,
    held_scan,
    gw,
    far_send,
    far_recv,
    own_send,
    own_recv,
    comb_send,
    comb_recv,
    mine,
    sq_send,
    sq_recv,
    load_sem,
    small_sem,
    halo_sem,
    dec_ss,
    dec_rs,
    st_ss,
    st_rs,
    pf_ss,
    pf_rs,
    far_ss,
    far_rs,
    own_ss,
    own_rs,
    comb_ss,
    comb_rs,
    sq_ss,
    sq_rs,
):
    r = lax.axis_index("seq")
    g = lax.axis_index("head")
    rows = tokens_hbm.shape[0]
    width = wi_hbm.shape[1]
    spans = rows // SPAN
    heads = width // HEADDIM
    pairs = heads // 2
    chunks = width // CHUNK
    half = width // 2
    right = lax.rem(g + 1, parts)
    left = lax.rem(g + parts - 1, parts)
    across = lax.rem(g + 2, parts)

    class loaded:
        def __init__(self, src, dst, number):
            self.whole = pltpu.make_async_copy(src, dst, load_sem.at[number])
            block = src.shape[0] // PIECES
            self.pieces = [
                pltpu.make_async_copy(
                    src.at[pl.ds(i * block, block), :],
                    dst.at[pl.ds(i * block, block), :],
                    load_sem.at[number],
                )
                for i in range(PIECES)
            ]

        def start(self):
            for piece in self.pieces:
                piece.start()

        def wait(self):
            self.whole.wait()

    wides = width // WIDE
    rest = width - wides * WIDE
    tok_load = loaded(tokens_hbm, tok, 0)
    wst_load = pltpu.make_async_copy(wst_hbm, wst, load_sem.at[1])
    wl_load = loaded(wg_hbm.at[:, pl.ds(wides * WIDE, rest)], wl, 2)
    wbc_load = loaded(wbc_hbm, wa.at[0, :, pl.ds(0, 2 * STATE)], 3)
    wr_load = loaded(
        wi_hbm.at[:, pl.ds(wides * WIDE, rest)], wa.at[0, :, pl.ds(2 * STATE, rest)], 4
    )
    wi_load = [
        loaded(wi_hbm.at[:, pl.ds(c * WIDE, WIDE)], wa.at[1 + c], 5 + c) for c in range(wides)
    ]
    wg_load = [
        loaded(wg_hbm.at[:, pl.ds(c * WIDE, WIDE)], wg.at[c], 5 + wides + c) for c in range(wides)
    ]
    wo_load = [
        loaded(wo_hbm.at[:, pl.ds(c * CHUNK, CHUNK)], wo.at[c], 5 + 2 * wides + c)
        for c in range(2 * chunks)
    ]
    small_load = [
        pltpu.make_async_copy(src, dst, small_sem.at[i])
        for i, (src, dst) in enumerate(
            (
                (bias_hbm, bias),
                (decay_log_hbm, decay_log),
                (conv_b_hbm, conv_b),
                (off_b_hbm, off_b),
                (conv_i_hbm, conv_i),
                (off_i_hbm, off_1),
                (skip_hbm, skip),
                (norm_hbm, norm_1),
            )
        )
    ]
    tok_load.start()
    for copy in small_load:
        copy.start()
    wst_load.start()
    wbc_load.start()
    wr_load.start()

    barrier = pltpu.get_barrier_semaphore()

    def greet_seq(i, carry):
        pl.semaphore_signal(
            barrier,
            inc=1,
            device_id={"seq": lax.rem(r + i, seqs), "head": g},
            device_id_type=MESH,
        )
        return carry

    lax.fori_loop(1, seqs, greet_seq, 0)
    for other in (right, left, across):
        pl.semaphore_signal(
            barrier, inc=1, device_id={"seq": r, "head": other}, device_id_type=MESH
        )

    def far_copy(src, dst, ss, rs, seq, head):
        return pltpu.make_async_remote_copy(
            src_ref=src,
            dst_ref=dst,
            send_sem=ss,
            recv_sem=rs,
            device_id={"seq": seq, "head": head},
            device_id_type=MESH,
        )

    lane = lax.broadcasted_iota(jnp.int32, (SPAN, SPAN), 1)
    sub = lax.broadcasted_iota(jnp.int32, (SPAN, SPAN), 0)
    low = lane < HEADDIM
    low_row = low[:1]
    head_of = lax.broadcasted_iota(jnp.int32, (SPAN, width), 1) // HEADDIM
    onto = jnp.where(head_of == lax.broadcasted_iota(jnp.int32, (SPAN, width), 0), 1.0, 0.0)
    spread[pl.ds(0, SPAN), :] = onto.astype(BF16)
    spread[pl.ds(SPAN, SPAN), :] = onto.astype(BF16)
    terms[...] = jnp.zeros_like(terms)
    dt_ref[...] = jnp.zeros_like(dt_ref)
    wst_load.wait()
    tok_load.wait()
    for copy in wi_load:
        copy.start()
    for side in range(2):
        at = pl.ds(side * (rows // 2), rows // 2)
        dt_ref[at, pl.ds(0, heads)] = lax.dot_general(
            tok[at, :], wst[...], (((1,), (1,)), ((), ())), preferred_element_type=F32
        )

    def raw_chunk(q):
        v = dot(tok[...], wa[q]).astype(BF16).astype(F32)
        for j in range(WIDE // SPAN):
            raw[q, j, pl.ds(HALO, rows), :] = v[:, j * SPAN : (j + 1) * SPAN]

    wbc_load.wait()
    wr_load.wait()
    raw_chunk(0)
    for q in range(wides):
        wi_load[q].wait()
        raw_chunk(1 + q)
    wl_load.start()
    for copy in wg_load:
        copy.start()
    for copy in wo_load:
        copy.start()

    for copy in small_load:
        copy.wait()
    off_i = off_1[...].reshape(1, -1)
    norm_w = norm_1[...].reshape(1, -1)

    step = dt_ref[:, pl.ds(0, heads)] + bias[...]
    tail = jnp.exp(-jnp.abs(step))
    up = 1.0 + tail
    log1p = jnp.where(up == 1.0, tail, jnp.log(up) * (tail / jnp.where(up == 1.0, 1.0, up - 1.0)))
    dt = jnp.maximum(step, 0.0) + log1p
    log_a = dt * (-LOG2E * jnp.exp(decay_log[...]))
    dt_ref[:, pl.ds(0, heads)] = dt
    for t, term in enumerate(split(log_a, 3)):
        for k in range(spans):
            terms[pl.ds(t * SPAN, SPAN), pl.ds(k * SPAN, heads)] = term[k * SPAN : (k + 1) * SPAN]
    tri = jnp.where(lane <= sub, 1.0, 0.0).astype(BF16)
    cums = dot(jnp.concatenate([tri, tri, tri], axis=1), terms[...])
    ends = []
    for k in range(spans):
        at = pl.ds(k * SPAN, SPAN)
        cum = cums[:, k * SPAN : (k + 1) * SPAN]
        cum_ref[at, :] = cum
        end_w = jnp.exp2(jnp.minimum(cum[SPAN - 1 :, :] - cum, 0.0)) * dt_ref[at, :]
        ends.append(jnp.concatenate(split(end_w, 2), axis=1))
    w_end[...] = dot(jnp.concatenate(ends, axis=0), spread[...])

    pl.semaphore_wait(barrier, seqs + 2)

    edges = [
        far_copy(
            raw.at[q, :, pl.ds(rows, HALO), :],
            raw.at[q, :, pl.ds(0, HALO), :],
            halo_sem.at[q],
            halo_sem.at[1 + wides + q],
            lax.rem(r + 1, seqs),
            g,
        )
        for q in range(1 + wides)
    ]

    @pl.when(r < seqs - 1)
    def _():
        for edge in edges:
            edge.start()

    def gate_store(v, cols):
        gate[:, cols] = silu(v.astype(BF16).astype(F32))

    order = [wides * WIDE + j * SPAN for j in range(rest // SPAN)]
    order += [j * SPAN for j in range(wides * WIDE // SPAN)]
    per_side = len(order) // 2
    place = {col: divmod(n, per_side) for n, col in enumerate(order)}
    my_tile = r // 2
    my_side = lax.rem(r, 2)
    chips = seqs // 2

    def dec_copy(dst):
        return far_copy(
            dec_send.at[lax.rem(dst, 2)], dec_recv.at[r], dec_ss.at[dst], dec_rs.at[r], dst, g
        )

    def st_copy(side, chip):
        dst = chip * 2 + side
        return far_copy(
            st_send.at[side, chip], st_recv.at[r], st_ss.at[dst], st_rs.at[r], dst, g
        )

    def pf_copy(dst):
        return far_copy(
            pf_send.at[dst], pf_recv.at[my_side, my_tile], pf_ss.at[dst], pf_rs.at[r], dst, g
        )

    def each(first, last, act):
        def one(d, carry):
            act(d)
            return carry

        lax.fori_loop(first, jnp.minimum(r, last), one, 0)
        lax.fori_loop(jnp.maximum(r + 1, first), last, one, 0)

    def to_side(side, act):
        def one(i, carry):
            chip = my_tile + i
            act(side, jnp.where(chip >= chips, chip - chips, chip))
            return carry

        lax.fori_loop(1, chips, one, 0)

        @pl.when(my_side != side)
        def _():
            act(side, my_tile)

    total = jnp.zeros((1, SPAN), F32)
    for k in range(spans):
        total = total + cum_ref[pl.ds(k * SPAN + SPAN - 1, 1), :]
    total = jnp.exp2(total)
    for col, (side, n) in place.items():
        p = col // SPAN
        dec_send[side, :, pl.ds(n * SPAN, SPAN)] = jnp.where(
            low_row,
            jnp.broadcast_to(total[:, 2 * p : 2 * p + 1], (1, SPAN)),
            jnp.broadcast_to(total[:, 2 * p + 1 : 2 * p + 2], (1, SPAN)),
        )
    each(0, seqs, lambda d: dec_copy(d).start())
    dec_recv[r] = dec_send[my_side]

    def conv(q, j, taps, offset, col, dst, blocks):
        cols = pl.ds(col, SPAN)
        for b in blocks:
            acc = offset[:, cols]
            for k in range(KERNEL):
                at = pl.ds(HALO - KERNEL + 1 + k + b * BLOCK, BLOCK)
                acc = acc + taps[pl.ds(k, 1), cols] * raw[q, j, at, :]
            dst[pl.ds(b * BLOCK, BLOCK), cols] = silu(acc).astype(BF16)

    tiles = STATE // 8

    def local_state(col):
        cols = pl.ds(col, SPAN)
        p = col // SPAN
        side, n = place[col]
        held = jnp.zeros((STATE, SPAN), F32)
        for k in range(spans):
            own = pl.ds(k * SPAN, SPAN)
            last = jnp.exp2(cum_ref[pl.ds(k * SPAN + SPAN - 1, 1), :])
            d = jnp.where(
                low_row,
                jnp.broadcast_to(last[:, 2 * p : 2 * p + 1], (1, SPAN)),
                jnp.broadcast_to(last[:, 2 * p + 1 : 2 * p + 2], (1, SPAN)),
            )
            prior[k, :, cols] = held.astype(BF16)
            scaled = (xs_ref[own, cols].astype(F32) * w_end[own, cols]).astype(BF16)
            held = d * held + dot(wt_ref[k], scaled)
        st_send[side, :, :, pl.ds(n * SPAN, SPAN)] = held.reshape(tiles, 8, SPAN).astype(LINK)
        if n == per_side - 1:
            to_side(side, lambda at, chip: st_copy(at, chip).start())

            @pl.when(my_side == side)
            def _():
                st_recv[r] = st_send[side, my_tile]

    def gate_wide(c):
        wg_load[c].wait()
        gate_store(dot(tok[...], wg[c]), pl.ds(c * WIDE, WIDE))

    main = range(1, rows // BLOCK)
    convs = [(0, j, conv_b, off_b, j * SPAN, bc_ref) for j in range(2 * STATE // SPAN)]
    for n, col in enumerate(order):
        q, j = divmod(2 * STATE // SPAN + n, WIDE // SPAN)
        convs.append((q, j, conv_i, off_i, col, xs_ref))
    for args in convs:
        conv(*args, main)

    group = seqs // 4
    edge_late = (lax.rem(r, group) == 0) & (r > 0)

    @pl.when(edge_late)
    def _():
        gate_wide(0)

    @pl.when(r == 0)
    def _():
        raw[:, :, pl.ds(0, HALO), :] = jnp.zeros((1 + wides, WIDE // SPAN, HALO, SPAN), F32)

    @pl.when(r > 0)
    def _():
        for edge in edges:
            edge.wait_recv()

    for args in convs:
        conv(*args, range(1))
    for k in range(spans):
        wt_ref[k] = bc_ref[pl.ds(k * SPAN, SPAN), pl.ds(0, STATE)].astype(F32).T.astype(BF16)
    for col in order:
        local_state(col)

    def within(k, carry):
        at = pl.ds(pl.multiple_of(k * SPAN, SPAN), SPAN)
        cum = cum_ref[at, :]
        cum_t = cum.T
        dt_t = dt_ref[at, :].T
        read = bc_ref[at, pl.ds(STATE, STATE)]
        write_t = wt_ref[k]
        scores = jnp.where(lane <= sub, dot(read, write_t), 0.0)
        base = carry
        for p in range(pairs):
            cols = pl.ds(p * SPAN, SPAN)
            x = xs_ref[at, cols]
            shown = []
            weights = []
            for h in (2 * p, 2 * p + 1):
                spread = jnp.broadcast_to(cum[:, h : h + 1], (SPAN, SPAN))
                shown.append(spread)
                gap = jnp.minimum(spread - cum_t[h : h + 1, :], 0.0)
                weights.append((scores * jnp.exp2(gap) * dt_t[h : h + 1, :]).astype(BF16))
            zero = jnp.zeros_like(x)
            both = jnp.concatenate([jnp.where(low, x, zero), jnp.where(low, zero, x)], axis=0)
            intra = dot(jnp.concatenate(weights, axis=1), both)
            scale = jnp.exp2(jnp.where(low, shown[0], shown[1]))
            inter = scale * dot(read, prior[k, :, cols])
            ahead = jnp.exp2(
                jnp.where(
                    low_row,
                    jnp.broadcast_to(base[:, 2 * p : 2 * p + 1], (1, SPAN)),
                    jnp.broadcast_to(base[:, 2 * p + 1 : 2 * p + 2], (1, SPAN)),
                )
            )
            gain = jnp.where(
                low_row,
                jnp.broadcast_to(skip[:, 2 * p : 2 * p + 1], (1, SPAN)),
                jnp.broadcast_to(skip[:, 2 * p + 1 : 2 * p + 2], (1, SPAN)),
            )
            opened = gate[at, cols]
            part_a[at, cols] = (intra + inter + gain * x.astype(F32)) * opened
            part_b[at, cols] = scale * ahead * opened
        return base + cum[SPAN - 1 :, :]

    def own_scan(first, last):
        def arrived(src):
            far_copy(
                dec_send.at[my_side], dec_recv.at[src], dec_ss.at[src], dec_rs.at[src], src, g
            ).wait_recv()
            far_copy(
                st_send.at[my_side, 0], st_recv.at[src], st_ss.at[src], st_rs.at[src], src, g
            ).wait_recv()

        each(first, last, arrived)

        def scan(d, carry):
            pf_send[d] = carry.astype(LINK)
            return dec_recv[d] * carry + st_recv[d].astype(F32)

        held_scan[...] = lax.fori_loop(first, last, scan, held_scan[...])
        each(first, last, lambda d: pf_copy(d).start())

        @pl.when((r >= first) & (r < last))
        def _():
            pf_recv[my_side, my_tile] = pf_send[r]

    row = r // group

    def rounds(before, after):
        def of(done):
            return group * jnp.where(
                row == 0,
                done[0],
                jnp.where(row == 1, done[1], jnp.where(row == 2, done[2], done[3])),
            )

        own_scan(of(before), of(after))

    done = ((0, 0, 0, 0), (0, 0, 1, 1), (0, 1, 2, 2), (1, 2, 3, 4), (2, 4, 4, 4), (4, 4, 4, 4))

    held_scan[...] = jnp.zeros((8, half), F32)

    @pl.when(jnp.logical_not(edge_late))
    def _():
        gate_wide(0)

    rounds(done[0], done[1])
    gate_wide(1)
    rounds(done[1], done[2])
    wl_load.wait()
    gate_store(dot(tok[...], wl[...]), pl.ds(wides * WIDE, rest))
    rounds(done[2], done[3])
    base = lax.fori_loop(0, spans // 2, within, jnp.zeros((1, SPAN), F32))
    rounds(done[3], done[4])
    lax.fori_loop(spans // 2, spans, within, base)
    rounds(done[4], done[5])
    for c in range(2 * chunks):
        wo_load[c].wait()

    def prefix_arrived(src):
        far_copy(
            pf_send.at[0],
            pf_recv.at[lax.rem(src, 2), src // 2],
            pf_ss.at[src],
            pf_rs.at[src],
            src,
            g,
        ).wait_recv()

    each(0, seqs, prefix_arrived)
    for side in range(2):
        got = pf_recv[side].astype(F32).reshape(STATE, half).astype(BF16)
        for col, (at, n) in place.items():
            if at == side:
                s_in[:, pl.ds(col, SPAN)] = got[:, n * SPAN : (n + 1) * SPAN]

    eye = jnp.where(lane == sub, 1.0, 0.0).astype(F32)

    def gated(slot, block):
        at = pl.ds(pl.multiple_of(block * SPAN, SPAN), SPAN)
        read = bc_ref[at, pl.ds(STATE, STATE)]
        squares = jnp.zeros((SPAN, CHUNK), F32)
        for c in range(chunks):
            cols = pl.ds(c * CHUNK, CHUNK)
            pre = part_a[at, cols] + part_b[at, cols] * dot(read, s_in[:, cols])
            squares = squares + pre * pre
            gw[slot, :, cols] = (pre * norm_w[:, cols]).astype(BF16)
        column = jnp.sum(squares, axis=1, keepdims=True)
        row = jnp.sum(eye * column, axis=0, keepdims=True)
        sq_send[slot] = jnp.broadcast_to(row, (8, SPAN))

    def sq_copy(slot, offset):
        return far_copy(
            sq_send.at[slot],
            sq_recv.at[offset - 1],
            sq_ss.at[offset - 1],
            sq_rs.at[offset - 1],
            r,
            lax.rem(g + offset, parts),
        )

    def stream(send, recv, ss, rs, c, way):
        at = way * chunks + c
        return far_copy(
            send.at[at], recv.at[at], ss.at[at], rs.at[at], r, (right, left)[way]
        )

    def far_step(c, carry):
        for way in range(2):
            far_send[way * chunks + c] = dot(gw[0], wo[way * chunks + c]).astype(BF16)
            stream(far_send, far_recv, far_ss, far_rs, c, way).start()
        return carry

    def own_step(c, carry):
        for way in range(2):
            own_send[way * chunks + c] = dot(gw[1 + way], wo[(1 - way) * chunks + c]).astype(BF16)
            stream(own_send, own_recv, own_ss, own_rs, c, way).start()
        return carry

    def mine_step(c, carry):
        mine[c] = dot(gw[3], wo[c])
        return carry

    def comb_step(c, carry):
        for way in range(2):
            at = way * chunks + c
            value = dot(gw[1 + way], wo[at])
            stream(far_send, far_recv, far_ss, far_rs, c, way).wait_recv()
            comb_send[at] = (value + far_recv[at].astype(F32)).astype(BF16)
            stream(comb_send, comb_recv, comb_ss, comb_rs, c, way).start()
        return carry

    gated(0, across)
    sq_copy(0, 2).start()
    lax.fori_loop(0, chunks, far_step, 0)
    gated(1, right)
    sq_copy(1, 1).start()
    gated(2, left)
    sq_copy(2, 3).start()
    lax.fori_loop(0, chunks, own_step, 0)
    gated(3, g)
    lax.fori_loop(0, 2 * chunks, mine_step, 0)
    lax.fori_loop(0, chunks, comb_step, 0)

    def drain(c, carry):
        for way in range(2):
            stream(far_send, far_recv, far_ss, far_rs, c, way).wait_send()
            stream(own_send, own_recv, own_ss, own_rs, c, way).wait_send()
        return carry

    def drain_comb(c, carry):
        for way in range(2):
            stream(comb_send, comb_recv, comb_ss, comb_rs, c, way).wait_send()
        return carry

    def sent(d):
        dec_copy(d).wait_send()
        st_copy(lax.rem(d, 2), d // 2).wait_send()
        pf_copy(d).wait_send()

    each(0, seqs, sent)

    @pl.when(r < seqs - 1)
    def _():
        for edge in edges:
            edge.wait_send()

    for slot, offset in ((1, 1), (0, 2), (2, 3)):
        sq_copy(slot, offset).wait_send()
    lax.fori_loop(0, chunks, drain, 0)

    squares = sq_send[3]
    for slot, offset in ((1, 1), (0, 2), (2, 3)):
        sq_copy(slot, offset).wait_recv()
        squares = squares + sq_recv[offset - 1]
    scale_row = 1.0 / jnp.sqrt(squares[:1] * (1.0 / inner_all) + EPS)
    scale = jnp.sum(eye * scale_row, axis=1, keepdims=True)

    for c in range(chunks):
        stream(own_send, own_recv, own_ss, own_rs, c, 1).wait_recv()
        stream(comb_send, comb_recv, comb_ss, comb_rs, c, 0).wait_recv()
        value = mine[c] + own_recv[chunks + c].astype(F32) + comb_recv[c].astype(F32)
        out[:, pl.ds(c * CHUNK, CHUNK)] = (value * scale).astype(BF16)
        stream(own_send, own_recv, own_ss, own_rs, c, 0).wait_recv()
        stream(comb_send, comb_recv, comb_ss, comb_rs, c, 1).wait_recv()
        value = mine[chunks + c] + own_recv[c].astype(F32) + comb_recv[chunks + c].astype(F32)
        out[:, pl.ds((chunks + c) * CHUNK, CHUNK)] = (value * scale).astype(BF16)

    lax.fori_loop(0, chunks, drain_comb, 0)


def per_device(
    seqs,
    parts,
    tokens,
    proj_inner,
    proj_gate,
    proj_bc,
    proj_step,
    conv_inner,
    conv_bc,
    offset_inner,
    offset_bc,
    step_bias,
    decay_log,
    skip_gain,
    norm_weight,
    out_weight,
):
    rows, depth = tokens.shape
    width = proj_inner.shape[1]
    heads = step_bias.shape[0]
    chunks = width // CHUNK
    spans = rows // SPAN
    half = width // 2
    tiles = STATE // 8
    model = out_weight.shape[1]
    any_spec = pl.BlockSpec(memory_space=pl.ANY)
    vmem = pl.BlockSpec(memory_space=pltpu.VMEM)
    dma = pltpu.SemaphoreType.DMA
    streams = [pltpu.VMEM((2 * chunks, SPAN, CHUNK), BF16)] * 6
    scratch = [
        pltpu.VMEM((KERNEL, width), F32),
        pltpu.VMEM((KERNEL, 2 * STATE), F32),
        pltpu.VMEM((width,), F32),
        pltpu.VMEM((1, 2 * STATE), F32),
        pltpu.VMEM((1, heads), F32),
        pltpu.VMEM((1, heads), F32),
        pltpu.VMEM((1, heads), F32),
        pltpu.VMEM((width,), F32),
        pltpu.VMEM((rows, depth), BF16),
        pltpu.VMEM((1 + width // WIDE, depth, WIDE), BF16),
        pltpu.VMEM((width // WIDE, depth, WIDE), BF16),
        pltpu.VMEM((depth, width % WIDE), BF16),
        pltpu.VMEM((heads, depth), BF16),
        pltpu.VMEM((2 * chunks, width, CHUNK), BF16),
        pltpu.VMEM((1 + width // WIDE, WIDE // SPAN, rows + HALO, SPAN), F32),
        pltpu.VMEM((3 * SPAN, spans * SPAN), BF16),
        pltpu.VMEM((2 * SPAN, width), BF16),
        pltpu.VMEM((rows, width), F32),
        pltpu.VMEM((rows, width), BF16),
        pltpu.VMEM((rows, 2 * STATE), BF16),
        pltpu.VMEM((spans, STATE, SPAN), BF16),
        pltpu.VMEM((rows, SPAN), F32),
        pltpu.VMEM((rows, SPAN), F32),
        pltpu.VMEM((rows, width), F32),
        pltpu.VMEM((rows, width), F32),
        pltpu.VMEM((rows, width), F32),
        pltpu.VMEM((spans, STATE, width), BF16),
        pltpu.VMEM((2, tiles, 8, half), LINK),
        pltpu.VMEM((seqs, 8, half), LINK),
        pltpu.VMEM((2, 1, half), F32),
        pltpu.VMEM((seqs, 1, half), F32),
        pltpu.VMEM((seqs, 8, half), LINK),
        pltpu.VMEM((2, tiles, 8, half), LINK),
        pltpu.VMEM((STATE, width), BF16),
        pltpu.VMEM((8, half), F32),
        pltpu.VMEM((4, SPAN, width), BF16),
        *streams,
        pltpu.VMEM((2 * chunks, SPAN, CHUNK), F32),
        pltpu.VMEM((4, 8, SPAN), F32),
        pltpu.VMEM((3, 8, SPAN), F32),
        dma((5 + 2 * (width // WIDE) + 2 * chunks,)),
        dma((8,)),
        dma((2 + 2 * (width // WIDE),)),
        *[dma((seqs,))] * 6,
        *[dma((2 * chunks,))] * 6,
        dma((3,)),
        dma((3,)),
    ]
    row = lambda v: v.reshape(1, -1)
    return pl.pallas_call(
        functools.partial(kernel, seqs, parts, float(parts * width)),
        out_shape=pltpu.VMEM((rows // parts, model), BF16),
        in_specs=[any_spec] * 14,
        out_specs=vmem,
        scratch_shapes=scratch,
        compiler_params=pltpu.CompilerParams(
            collective_id=0, has_side_effects=True, vmem_limit_bytes=62 * 1024 * 1024
        ),
    )(
        tokens,
        proj_inner,
        proj_gate,
        proj_bc,
        proj_step.T,
        conv_inner,
        conv_bc,
        offset_inner,
        row(offset_bc),
        row(step_bias),
        row(decay_log),
        row(skip_gain),
        norm_weight,
        out_weight,
    )


def solution(mesh):
    body = functools.partial(per_device, mesh.shape["seq"], mesh.shape["head"])
    return jax.shard_map(
        body,
        mesh=mesh,
        in_specs=(
            P("seq", None),
            P(None, "head"),
            P(None, "head"),
            P(),
            P(None, "head"),
            P(None, "head"),
            P(),
            P("head"),
            P(),
            P("head"),
            P("head"),
            P("head"),
            P("head"),
            P("head", None),
        ),
        out_specs=P(("seq", "head"), None),
        check_vma=False,
    )
```

```python
import functools

import jax
import jax.numpy as jnp
from jax import lax
from jax.experimental import pallas as pl
from jax.experimental.pallas import tpu as pltpu
from jax.sharding import PartitionSpec as P

HEADDIM = 64
STATE = 128
KERNEL = 4
SPAN = 128
HALO = 8
CHUNK = 256
BLOCK = 64
WIDE = 512
PIECES = 4
LOG2E = 1.4426950408889634
EPS = 0.25
MESH = pl.DeviceIdType.MESH
F32 = jnp.float32
BF16 = jnp.bfloat16
LINK = jnp.bfloat16


def silu(v):
    return v / (1.0 + jnp.exp(-v))


def dot(a, b):
    return jnp.dot(a, b, preferred_element_type=F32)


def split(v, count):
    terms = []
    for _ in range(count):
        terms.append(v.astype(BF16))
        v = v - terms[-1].astype(F32)
    return terms


def kernel(
    seqs,
    parts,
    inner_all,
    tokens_hbm,
    wi_hbm,
    wg_hbm,
    wbc_hbm,
    wst_hbm,
    conv_i_hbm,
    conv_b_hbm,
    off_i_hbm,
    off_b_hbm,
    bias_hbm,
    decay_log_hbm,
    skip_hbm,
    norm_hbm,
    wo_hbm,
    out,
    conv_i,
    conv_b,
    off_1,
    off_b,
    bias,
    decay_log,
    skip,
    norm_1,
    tok,
    wa,
    wg,
    wl,
    wst,
    wo,
    raw,
    terms,
    spread,
    w_end,
    xs_ref,
    bc_ref,
    wt_ref,
    cum_ref,
    dt_ref,
    gate,
    part_a,
    part_b,
    prior,
    st_send,
    st_recv,
    dec_send,
    dec_recv,
    pf_send,
    pf_recv,
    s_in,
    held_scan,
    gw,
    far_send,
    far_recv,
    own_send,
    own_recv,
    comb_send,
    comb_recv,
    mine,
    sq_send,
    sq_recv,
    load_sem,
    small_sem,
    halo_sem,
    dec_ss,
    dec_rs,
    st_ss,
    st_rs,
    pf_ss,
    pf_rs,
    far_ss,
    far_rs,
    own_ss,
    own_rs,
    comb_ss,
    comb_rs,
    sq_ss,
    sq_rs,
):
    r = lax.axis_index("seq")
    g = lax.axis_index("head")
    rows = tokens_hbm.shape[0]
    width = wi_hbm.shape[1]
    spans = rows // SPAN
    heads = width // HEADDIM
    pairs = heads // 2
    chunks = width // CHUNK
    half = width // 2
    right = lax.rem(g + 1, parts)
    left = lax.rem(g + parts - 1, parts)
    across = lax.rem(g + 2, parts)

    class loaded:
        def __init__(self, src, dst, number):
            self.whole = pltpu.make_async_copy(src, dst, load_sem.at[number])
            block = src.shape[0] // PIECES
            self.pieces = [
                pltpu.make_async_copy(
                    src.at[pl.ds(i * block, block), :],
                    dst.at[pl.ds(i * block, block), :],
                    load_sem.at[number],
                )
                for i in range(PIECES)
            ]

        def start(self):
            for piece in self.pieces:
                piece.start()

        def wait(self):
            self.whole.wait()

    wides = width // WIDE
    rest = width - wides * WIDE
    tok_load = loaded(tokens_hbm, tok, 0)
    wst_load = pltpu.make_async_copy(wst_hbm, wst, load_sem.at[1])
    wl_load = loaded(wg_hbm.at[:, pl.ds(wides * WIDE, rest)], wl, 2)
    wbc_load = loaded(wbc_hbm, wa.at[0, :, pl.ds(0, 2 * STATE)], 3)
    wr_load = loaded(
        wi_hbm.at[:, pl.ds(wides * WIDE, rest)], wa.at[0, :, pl.ds(2 * STATE, rest)], 4
    )
    wi_load = [
        loaded(wi_hbm.at[:, pl.ds(c * WIDE, WIDE)], wa.at[1 + c], 5 + c) for c in range(wides)
    ]
    wg_load = [
        loaded(wg_hbm.at[:, pl.ds(c * WIDE, WIDE)], wg.at[c], 5 + wides + c) for c in range(wides)
    ]
    wo_load = [
        pltpu.make_async_copy(
            wo_hbm.at[:, pl.ds(c * CHUNK, CHUNK)], wo.at[c], load_sem.at[5 + 2 * wides]
        )
        for c in range(2 * chunks)
    ]
    small_load = [
        pltpu.make_async_copy(src, dst, small_sem.at[i])
        for i, (src, dst) in enumerate(
            (
                (bias_hbm, bias),
                (decay_log_hbm, decay_log),
                (conv_b_hbm, conv_b),
                (off_b_hbm, off_b),
                (conv_i_hbm, conv_i),
                (off_i_hbm, off_1),
                (skip_hbm, skip),
                (norm_hbm, norm_1),
            )
        )
    ]
    tok_load.start()
    for copy in small_load:
        copy.start()
    wst_load.start()
    wbc_load.start()
    wr_load.start()

    barrier = pltpu.get_barrier_semaphore()

    def greet_seq(i, carry):
        pl.semaphore_signal(
            barrier,
            inc=1,
            device_id={"seq": lax.rem(r + i, seqs), "head": g},
            device_id_type=MESH,
        )
        return carry

    lax.fori_loop(1, seqs, greet_seq, 0)
    for other in (right, left, across):
        pl.semaphore_signal(
            barrier, inc=1, device_id={"seq": r, "head": other}, device_id_type=MESH
        )

    def far_copy(src, dst, ss, rs, seq, head):
        return pltpu.make_async_remote_copy(
            src_ref=src,
            dst_ref=dst,
            send_sem=ss,
            recv_sem=rs,
            device_id={"seq": seq, "head": head},
            device_id_type=MESH,
        )

    lane = lax.broadcasted_iota(jnp.int32, (SPAN, SPAN), 1)
    sub = lax.broadcasted_iota(jnp.int32, (SPAN, SPAN), 0)
    low = lane < HEADDIM
    low_row = low[:1]
    head_of = lax.broadcasted_iota(jnp.int32, (SPAN, width), 1) // HEADDIM
    onto = jnp.where(head_of == lax.broadcasted_iota(jnp.int32, (SPAN, width), 0), 1.0, 0.0)
    spread[pl.ds(0, SPAN), :] = onto.astype(BF16)
    spread[pl.ds(SPAN, SPAN), :] = onto.astype(BF16)
    terms[...] = jnp.zeros_like(terms)
    dt_ref[...] = jnp.zeros_like(dt_ref)
    wst_load.wait()
    tok_load.wait()
    for copy in wi_load:
        copy.start()
    for side in range(2):
        at = pl.ds(side * (rows // 2), rows // 2)
        dt_ref[at, pl.ds(0, heads)] = lax.dot_general(
            tok[at, :], wst[...], (((1,), (1,)), ((), ())), preferred_element_type=F32
        )

    def raw_chunk(q):
        v = dot(tok[...], wa[q]).astype(BF16).astype(F32)
        for j in range(WIDE // SPAN):
            raw[q, j, pl.ds(HALO, rows), :] = v[:, j * SPAN : (j + 1) * SPAN]

    wbc_load.wait()
    wr_load.wait()
    raw_chunk(0)
    for q in range(wides):
        wi_load[q].wait()
        raw_chunk(1 + q)
    wl_load.start()
    for copy in wg_load:
        copy.start()
    for copy in wo_load:
        copy.start()

    for copy in small_load:
        copy.wait()
    off_i = off_1[...].reshape(1, -1)
    norm_w = norm_1[...].reshape(1, -1)

    step = dt_ref[:, pl.ds(0, heads)] + bias[...]
    tail = jnp.exp(-jnp.abs(step))
    up = 1.0 + tail
    log1p = jnp.where(up == 1.0, tail, jnp.log(up) * (tail / jnp.where(up == 1.0, 1.0, up - 1.0)))
    dt = jnp.maximum(step, 0.0) + log1p
    log_a = dt * (-LOG2E * jnp.exp(decay_log[...]))
    dt_ref[:, pl.ds(0, heads)] = dt
    for t, term in enumerate(split(log_a, 3)):
        for k in range(spans):
            terms[pl.ds(t * SPAN, SPAN), pl.ds(k * SPAN, heads)] = term[k * SPAN : (k + 1) * SPAN]
    tri = jnp.where(lane <= sub, 1.0, 0.0).astype(BF16)
    cums = dot(jnp.concatenate([tri, tri, tri], axis=1), terms[...])
    ends = []
    for k in range(spans):
        at = pl.ds(k * SPAN, SPAN)
        cum = cums[:, k * SPAN : (k + 1) * SPAN]
        cum_ref[at, :] = cum
        end_w = jnp.exp2(jnp.minimum(cum[SPAN - 1 :, :] - cum, 0.0)) * dt_ref[at, :]
        ends.append(jnp.concatenate(split(end_w, 2), axis=1))
    w_end[...] = dot(jnp.concatenate(ends, axis=0), spread[...])

    pl.semaphore_wait(barrier, seqs + 2)

    edges = [
        far_copy(
            raw.at[q, :, pl.ds(rows, HALO), :],
            raw.at[q, :, pl.ds(0, HALO), :],
            halo_sem.at[q],
            halo_sem.at[1 + wides + q],
            lax.rem(r + 1, seqs),
            g,
        )
        for q in range(1 + wides)
    ]

    @pl.when(r < seqs - 1)
    def _():
        for edge in edges:
            edge.start()

    def gate_store(v, cols):
        gate[:, cols] = silu(v.astype(BF16).astype(F32))

    order = [wides * WIDE + j * SPAN for j in range(rest // SPAN)]
    order += [j * SPAN for j in range(wides * WIDE // SPAN)]
    per_side = len(order) // 2
    place = {col: divmod(n, per_side) for n, col in enumerate(order)}
    my_tile = r // 2
    my_side = lax.rem(r, 2)
    chips = seqs // 2

    group = seqs // 4
    row = r // group

    def dec_copy(dst):
        return far_copy(
            dec_send.at[lax.rem(dst, 2)], dec_recv.at[r], dec_ss.at[0], dec_rs.at[row], dst, g
        )

    def st_copy(side, chip):
        return far_copy(
            st_send.at[side, chip],
            st_recv.at[r],
            st_ss.at[0],
            st_rs.at[row],
            chip * 2 + side,
            g,
        )

    def pf_copy(dst):
        return far_copy(
            pf_send.at[dst], pf_recv.at[my_side, my_tile], pf_ss.at[0], pf_rs.at[0], dst, g
        )

    def bulk(ref, ss, rs):
        return far_copy(ref, ref, ss, rs, r, g)

    def each(first, last, act):
        def one(d, carry):
            act(d)
            return carry

        lax.fori_loop(first, jnp.minimum(r, last), one, 0)
        lax.fori_loop(jnp.maximum(r + 1, first), last, one, 0)

    def to_side(side, act):
        def one(i, carry):
            chip = my_tile + i
            act(side, jnp.where(chip >= chips, chip - chips, chip))
            return carry

        lax.fori_loop(1, chips, one, 0)

        @pl.when(my_side != side)
        def _():
            act(side, my_tile)

    total = jnp.zeros((1, SPAN), F32)
    for k in range(spans):
        total = total + cum_ref[pl.ds(k * SPAN + SPAN - 1, 1), :]
    total = jnp.exp2(total)
    for col, (side, n) in place.items():
        p = col // SPAN
        dec_send[side, :, pl.ds(n * SPAN, SPAN)] = jnp.where(
            low_row,
            jnp.broadcast_to(total[:, 2 * p : 2 * p + 1], (1, SPAN)),
            jnp.broadcast_to(total[:, 2 * p + 1 : 2 * p + 2], (1, SPAN)),
        )
    each(0, seqs, lambda d: dec_copy(d).start())
    dec_recv[r] = dec_send[my_side]

    def conv(q, j, taps, offset, col, dst, blocks):
        cols = pl.ds(col, SPAN)
        for b in blocks:
            acc = offset[:, cols]
            for k in range(KERNEL):
                at = pl.ds(HALO - KERNEL + 1 + k + b * BLOCK, BLOCK)
                acc = acc + taps[pl.ds(k, 1), cols] * raw[q, j, at, :]
            dst[pl.ds(b * BLOCK, BLOCK), cols] = silu(acc).astype(BF16)

    tiles = STATE // 8

    def local_state(col):
        cols = pl.ds(col, SPAN)
        p = col // SPAN
        side, n = place[col]
        held = jnp.zeros((STATE, SPAN), F32)
        for k in range(spans):
            own = pl.ds(k * SPAN, SPAN)
            last = jnp.exp2(cum_ref[pl.ds(k * SPAN + SPAN - 1, 1), :])
            d = jnp.where(
                low_row,
                jnp.broadcast_to(last[:, 2 * p : 2 * p + 1], (1, SPAN)),
                jnp.broadcast_to(last[:, 2 * p + 1 : 2 * p + 2], (1, SPAN)),
            )
            prior[k, :, cols] = held.astype(BF16)
            scaled = (xs_ref[own, cols].astype(F32) * w_end[own, cols]).astype(BF16)
            held = d * held + dot(wt_ref[k], scaled)
        st_send[side, :, :, pl.ds(n * SPAN, SPAN)] = held.reshape(tiles, 8, SPAN).astype(LINK)
        if n == per_side - 1:
            to_side(side, lambda at, chip: st_copy(at, chip).start())

            @pl.when(my_side == side)
            def _():
                st_recv[r] = st_send[side, my_tile]

    def gate_wide(c):
        wg_load[c].wait()
        gate_store(dot(tok[...], wg[c]), pl.ds(c * WIDE, WIDE))

    main = range(1, rows // BLOCK)
    convs = [(0, j, conv_b, off_b, j * SPAN, bc_ref) for j in range(2 * STATE // SPAN)]
    for n, col in enumerate(order):
        q, j = divmod(2 * STATE // SPAN + n, WIDE // SPAN)
        convs.append((q, j, conv_i, off_i, col, xs_ref))
    for args in convs:
        conv(*args, main)

    edge_late = (lax.rem(r, group) == 0) & (r > 0)

    @pl.when(edge_late)
    def _():
        gate_wide(0)

    @pl.when(r == 0)
    def _():
        raw[:, :, pl.ds(0, HALO), :] = jnp.zeros((1 + wides, WIDE // SPAN, HALO, SPAN), F32)

    @pl.when(r > 0)
    def _():
        for edge in edges:
            edge.wait_recv()

    for args in convs:
        conv(*args, range(1))
    for k in range(spans):
        wt_ref[k] = bc_ref[pl.ds(k * SPAN, SPAN), pl.ds(0, STATE)].astype(F32).T.astype(BF16)
    for col in order:
        local_state(col)

    def within(k, carry):
        at = pl.ds(pl.multiple_of(k * SPAN, SPAN), SPAN)
        cum = cum_ref[at, :]
        cum_t = cum.T
        dt_t = dt_ref[at, :].T
        read = bc_ref[at, pl.ds(STATE, STATE)]
        write_t = wt_ref[k]
        scores = jnp.where(lane <= sub, dot(read, write_t), 0.0)
        base = carry
        for p in range(pairs):
            cols = pl.ds(p * SPAN, SPAN)
            x = xs_ref[at, cols]
            shown = []
            weights = []
            for h in (2 * p, 2 * p + 1):
                spread = jnp.broadcast_to(cum[:, h : h + 1], (SPAN, SPAN))
                shown.append(spread)
                gap = jnp.minimum(spread - cum_t[h : h + 1, :], 0.0)
                weights.append((scores * jnp.exp2(gap) * dt_t[h : h + 1, :]).astype(BF16))
            zero = jnp.zeros_like(x)
            both = jnp.concatenate([jnp.where(low, x, zero), jnp.where(low, zero, x)], axis=0)
            intra = dot(jnp.concatenate(weights, axis=1), both)
            scale = jnp.exp2(jnp.where(low, shown[0], shown[1]))
            inter = scale * dot(read, prior[k, :, cols])
            ahead = jnp.exp2(
                jnp.where(
                    low_row,
                    jnp.broadcast_to(base[:, 2 * p : 2 * p + 1], (1, SPAN)),
                    jnp.broadcast_to(base[:, 2 * p + 1 : 2 * p + 2], (1, SPAN)),
                )
            )
            gain = jnp.where(
                low_row,
                jnp.broadcast_to(skip[:, 2 * p : 2 * p + 1], (1, SPAN)),
                jnp.broadcast_to(skip[:, 2 * p + 1 : 2 * p + 2], (1, SPAN)),
            )
            opened = gate[at, cols]
            part_a[at, cols] = (intra + inter + gain * x.astype(F32)) * opened
            part_b[at, cols] = scale * ahead * opened
        return base + cum[SPAN - 1 :, :]

    def own_scan(begin, end):
        def arrived(q, count):
            at = pl.ds(q * group, count)
            bulk(dec_recv.at[at], dec_ss.at[0], dec_rs.at[q]).wait_recv()
            bulk(st_recv.at[at], st_ss.at[0], st_rs.at[q]).wait_recv()

        def await_group(q, carry):
            @pl.when(q == row)
            def _():
                arrived(q, group - 1)

            @pl.when(q != row)
            def _():
                arrived(q, group)

            return carry

        lax.fori_loop(begin, end, await_group, 0)
        first, last = begin * group, end * group

        def scan(d, carry):
            pf_send[d] = carry.astype(LINK)
            return dec_recv[d] * carry + st_recv[d].astype(F32)

        held_scan[...] = lax.fori_loop(first, last, scan, held_scan[...])
        each(first, last, lambda d: pf_copy(d).start())

        @pl.when((r >= first) & (r < last))
        def _():
            pf_recv[my_side, my_tile] = pf_send[r]

    def rounds(before, after):
        def of(done):
            return jnp.where(
                row == 0,
                done[0],
                jnp.where(row == 1, done[1], jnp.where(row == 2, done[2], done[3])),
            )

        own_scan(of(before), of(after))

    done = ((0, 0, 0, 0), (0, 0, 1, 1), (0, 1, 2, 2), (1, 2, 3, 4), (2, 4, 4, 4), (4, 4, 4, 4))

    held_scan[...] = jnp.zeros((8, half), F32)

    @pl.when(jnp.logical_not(edge_late))
    def _():
        gate_wide(0)

    rounds(done[0], done[1])
    gate_wide(1)
    rounds(done[1], done[2])
    wl_load.wait()
    gate_store(dot(tok[...], wl[...]), pl.ds(wides * WIDE, rest))
    rounds(done[2], done[3])
    base = lax.fori_loop(0, spans // 2, within, jnp.zeros((1, SPAN), F32))
    rounds(done[3], done[4])
    lax.fori_loop(spans // 2, spans, within, base)
    rounds(done[4], done[5])
    pltpu.make_async_copy(wo, wo, load_sem.at[5 + 2 * wides]).wait()

    bulk(pf_send.at[pl.ds(0, seqs - 1)], pf_ss.at[0], pf_rs.at[0]).wait_recv()
    for side in range(2):
        got = pf_recv[side].astype(F32).reshape(STATE, half).astype(BF16)
        for col, (at, n) in place.items():
            if at == side:
                s_in[:, pl.ds(col, SPAN)] = got[:, n * SPAN : (n + 1) * SPAN]

    eye = jnp.where(lane == sub, 1.0, 0.0).astype(F32)

    def gated(slot, block):
        at = pl.ds(pl.multiple_of(block * SPAN, SPAN), SPAN)
        read = bc_ref[at, pl.ds(STATE, STATE)]
        squares = jnp.zeros((SPAN, CHUNK), F32)
        for c in range(chunks):
            cols = pl.ds(c * CHUNK, CHUNK)
            pre = part_a[at, cols] + part_b[at, cols] * dot(read, s_in[:, cols])
            squares = squares + pre * pre
            gw[slot, :, cols] = (pre * norm_w[:, cols]).astype(BF16)
        column = jnp.sum(squares, axis=1, keepdims=True)
        row = jnp.sum(eye * column, axis=0, keepdims=True)
        sq_send[slot] = jnp.broadcast_to(row, (8, SPAN))

    def sq_copy(slot, offset):
        return far_copy(
            sq_send.at[slot],
            sq_recv.at[offset - 1],
            sq_ss.at[0],
            sq_rs.at[0],
            r,
            lax.rem(g + offset, parts),
        )

    def stream(send, recv, ss, rs, c, way):
        at = way * chunks + c
        return far_copy(
            send.at[at],
            recv.at[at],
            ss.at[0],
            rs.at[0] if rs is own_rs else rs.at[at],
            r,
            (right, left)[way],
        )

    def far_step(c, carry):
        for way in range(2):
            far_send[way * chunks + c] = dot(gw[0], wo[way * chunks + c]).astype(BF16)
            stream(far_send, far_recv, far_ss, far_rs, c, way).start()
        return carry

    def own_step(c, carry):
        for way in range(2):
            own_send[way * chunks + c] = dot(gw[1 + way], wo[(1 - way) * chunks + c]).astype(BF16)
            stream(own_send, own_recv, own_ss, own_rs, c, way).start()
        return carry

    def mine_step(c, carry):
        mine[c] = dot(gw[3], wo[c])
        return carry

    def comb_step(c, carry):
        for way in range(2):
            at = way * chunks + c
            value = dot(gw[1 + way], wo[at])
            stream(far_send, far_recv, far_ss, far_rs, c, way).wait_recv()
            comb_send[at] = (value + far_recv[at].astype(F32)).astype(BF16)
            stream(comb_send, comb_recv, comb_ss, comb_rs, c, way).start()
        return carry

    gated(0, across)
    sq_copy(0, 2).start()
    lax.fori_loop(0, chunks, far_step, 0)
    gated(1, right)
    sq_copy(1, 1).start()
    gated(2, left)
    sq_copy(2, 3).start()
    lax.fori_loop(0, chunks, own_step, 0)
    gated(3, g)
    lax.fori_loop(0, 2 * chunks, mine_step, 0)
    lax.fori_loop(0, chunks, comb_step, 0)

    others = pl.ds(0, seqs - 1)
    bulk(dec_recv.at[others], dec_ss.at[0], dec_rs.at[0]).wait_send()
    bulk(st_recv.at[others], st_ss.at[0], st_rs.at[0]).wait_send()
    bulk(pf_send.at[others], pf_ss.at[0], pf_rs.at[0]).wait_send()

    @pl.when(r < seqs - 1)
    def _():
        for edge in edges:
            edge.wait_send()

    bulk(sq_recv, sq_ss.at[0], sq_rs.at[0]).wait_send()
    bulk(far_send, far_ss.at[0], far_rs.at[0]).wait_send()
    bulk(own_send, own_ss.at[0], own_rs.at[0]).wait_send()

    bulk(sq_recv, sq_ss.at[0], sq_rs.at[0]).wait_recv()
    squares = sq_send[3] + sq_recv[0] + sq_recv[1] + sq_recv[2]
    scale_row = 1.0 / jnp.sqrt(squares[:1] * (1.0 / inner_all) + EPS)
    scale = jnp.sum(eye * scale_row, axis=1, keepdims=True)

    bulk(own_recv, own_ss.at[0], own_rs.at[0]).wait_recv()
    for c in range(chunks):
        stream(comb_send, comb_recv, comb_ss, comb_rs, c, 0).wait_recv()
        value = mine[c] + own_recv[chunks + c].astype(F32) + comb_recv[c].astype(F32)
        out[:, pl.ds(c * CHUNK, CHUNK)] = (value * scale).astype(BF16)
        stream(comb_send, comb_recv, comb_ss, comb_rs, c, 1).wait_recv()
        value = mine[chunks + c] + own_recv[c].astype(F32) + comb_recv[chunks + c].astype(F32)
        out[:, pl.ds((chunks + c) * CHUNK, CHUNK)] = (value * scale).astype(BF16)

    bulk(comb_send, comb_ss.at[0], comb_rs.at[0]).wait_send()


def per_device(
    seqs,
    parts,
    tokens,
    proj_inner,
    proj_gate,
    proj_bc,
    proj_step,
    conv_inner,
    conv_bc,
    offset_inner,
    offset_bc,
    step_bias,
    decay_log,
    skip_gain,
    norm_weight,
    out_weight,
):
    rows, depth = tokens.shape
    width = proj_inner.shape[1]
    heads = step_bias.shape[0]
    chunks = width // CHUNK
    spans = rows // SPAN
    half = width // 2
    tiles = STATE // 8
    model = out_weight.shape[1]
    any_spec = pl.BlockSpec(memory_space=pl.ANY)
    vmem = pl.BlockSpec(memory_space=pltpu.VMEM)
    dma = pltpu.SemaphoreType.DMA
    streams = [pltpu.VMEM((2 * chunks, SPAN, CHUNK), BF16)] * 6
    scratch = [
        pltpu.VMEM((KERNEL, width), F32),
        pltpu.VMEM((KERNEL, 2 * STATE), F32),
        pltpu.VMEM((width,), F32),
        pltpu.VMEM((1, 2 * STATE), F32),
        pltpu.VMEM((1, heads), F32),
        pltpu.VMEM((1, heads), F32),
        pltpu.VMEM((1, heads), F32),
        pltpu.VMEM((width,), F32),
        pltpu.VMEM((rows, depth), BF16),
        pltpu.VMEM((1 + width // WIDE, depth, WIDE), BF16),
        pltpu.VMEM((width // WIDE, depth, WIDE), BF16),
        pltpu.VMEM((depth, width % WIDE), BF16),
        pltpu.VMEM((heads, depth), BF16),
        pltpu.VMEM((2 * chunks, width, CHUNK), BF16),
        pltpu.VMEM((1 + width // WIDE, WIDE // SPAN, rows + HALO, SPAN), F32),
        pltpu.VMEM((3 * SPAN, spans * SPAN), BF16),
        pltpu.VMEM((2 * SPAN, width), BF16),
        pltpu.VMEM((rows, width), F32),
        pltpu.VMEM((rows, width), BF16),
        pltpu.VMEM((rows, 2 * STATE), BF16),
        pltpu.VMEM((spans, STATE, SPAN), BF16),
        pltpu.VMEM((rows, SPAN), F32),
        pltpu.VMEM((rows, SPAN), F32),
        pltpu.VMEM((rows, width), F32),
        pltpu.VMEM((rows, width), F32),
        pltpu.VMEM((rows, width), F32),
        pltpu.VMEM((spans, STATE, width), BF16),
        pltpu.VMEM((2, tiles, 8, half), LINK),
        pltpu.VMEM((seqs, 8, half), LINK),
        pltpu.VMEM((2, 1, half), F32),
        pltpu.VMEM((seqs, 1, half), F32),
        pltpu.VMEM((seqs, 8, half), LINK),
        pltpu.VMEM((2, tiles, 8, half), LINK),
        pltpu.VMEM((STATE, width), BF16),
        pltpu.VMEM((8, half), F32),
        pltpu.VMEM((4, SPAN, width), BF16),
        *streams,
        pltpu.VMEM((2 * chunks, SPAN, CHUNK), F32),
        pltpu.VMEM((4, 8, SPAN), F32),
        pltpu.VMEM((3, 8, SPAN), F32),
        dma((6 + 2 * (width // WIDE),)),
        dma((8,)),
        dma((2 + 2 * (width // WIDE),)),
        dma((1,)),
        dma((4,)),
        dma((1,)),
        dma((4,)),
        dma((1,)),
        dma((1,)),
        dma((1,)),
        dma((2 * chunks,)),
        dma((1,)),
        dma((1,)),
        dma((1,)),
        dma((2 * chunks,)),
        dma((1,)),
        dma((1,)),
    ]
    row = lambda v: v.reshape(1, -1)
    return pl.pallas_call(
        functools.partial(kernel, seqs, parts, float(parts * width)),
        out_shape=pltpu.VMEM((rows // parts, model), BF16),
        in_specs=[any_spec] * 14,
        out_specs=vmem,
        scratch_shapes=scratch,
        compiler_params=pltpu.CompilerParams(
            collective_id=0, has_side_effects=True, vmem_limit_bytes=62 * 1024 * 1024
        ),
    )(
        tokens,
        proj_inner,
        proj_gate,
        proj_bc,
        proj_step.T,
        conv_inner,
        conv_bc,
        offset_inner,
        row(offset_bc),
        row(step_bias),
        row(decay_log),
        row(skip_gain),
        norm_weight,
        out_weight,
    )


def solution(mesh):
    body = functools.partial(per_device, mesh.shape["seq"], mesh.shape["head"])
    return jax.shard_map(
        body,
        mesh=mesh,
        in_specs=(
            P("seq", None),
            P(None, "head"),
            P(None, "head"),
            P(),
            P(None, "head"),
            P(None, "head"),
            P(),
            P("head"),
            P(),
            P("head"),
            P("head"),
            P("head"),
            P("head"),
            P("head", None),
        ),
        out_specs=P(("seq", "head"), None),
        check_vma=False,
    )
```

```python
import functools

import jax
import jax.numpy as jnp
from jax import lax
from jax.experimental import pallas as pl
from jax.experimental.pallas import tpu as pltpu
from jax.sharding import PartitionSpec as P

HEADDIM = 64
STATE = 128
KERNEL = 4
SPAN = 128
HALO = 8
CHUNK = 256
BLOCK = 64
WIDE = 512
PIECES = 4
LOG2E = 1.4426950408889634
EPS = 0.25
MESH = pl.DeviceIdType.MESH
F32 = jnp.float32
BF16 = jnp.bfloat16
LINK = jnp.bfloat16


def silu(v):
    return v / (1.0 + jnp.exp(-v))


def dot(a, b):
    return jnp.dot(a, b, preferred_element_type=F32)


def split(v, count):
    terms = []
    for _ in range(count):
        terms.append(v.astype(BF16))
        v = v - terms[-1].astype(F32)
    return terms


def kernel(
    seqs,
    parts,
    inner_all,
    tokens_hbm,
    wi_hbm,
    wg_hbm,
    wbc_hbm,
    wst_hbm,
    conv_i_hbm,
    conv_b_hbm,
    off_i_hbm,
    off_b_hbm,
    bias_hbm,
    decay_log_hbm,
    skip_hbm,
    norm_hbm,
    wo_hbm,
    out,
    conv_i,
    conv_b,
    off_1,
    off_b,
    bias,
    decay_log,
    skip,
    norm_1,
    tok,
    wa,
    wg,
    wl,
    wst,
    wo,
    raw,
    terms,
    spread,
    w_end,
    xs_ref,
    bc_ref,
    wt_ref,
    cum_ref,
    dt_ref,
    gate,
    part_a,
    part_b,
    prior,
    st_send,
    st_recv,
    dec_send,
    dec_recv,
    pf_send,
    pf_recv,
    s_in,
    held_scan,
    gw,
    far_send,
    far_recv,
    own_send,
    own_recv,
    comb_send,
    comb_recv,
    mine,
    sq_send,
    sq_recv,
    load_sem,
    small_sem,
    halo_sem,
    dec_ss,
    dec_rs,
    st_ss,
    st_rs,
    pf_ss,
    pf_rs,
    far_ss,
    far_rs,
    own_ss,
    own_rs,
    comb_ss,
    comb_rs,
    sq_ss,
    sq_rs,
):
    r = lax.axis_index("seq")
    g = lax.axis_index("head")
    rows = tokens_hbm.shape[0]
    width = wi_hbm.shape[1]
    spans = rows // SPAN
    heads = width // HEADDIM
    pairs = heads // 2
    chunks = width // CHUNK
    half = width // 2
    right = lax.rem(g + 1, parts)
    left = lax.rem(g + parts - 1, parts)
    across = lax.rem(g + 2, parts)

    class loaded:
        def __init__(self, src, dst, number):
            self.whole = pltpu.make_async_copy(src, dst, load_sem.at[number])
            block = src.shape[0] // PIECES
            self.pieces = [
                pltpu.make_async_copy(
                    src.at[pl.ds(i * block, block), :],
                    dst.at[pl.ds(i * block, block), :],
                    load_sem.at[number],
                )
                for i in range(PIECES)
            ]

        def start(self):
            for piece in self.pieces:
                piece.start()

        def wait(self):
            self.whole.wait()

    wides = width // WIDE
    rest = width - wides * WIDE
    tok_load = loaded(tokens_hbm, tok, 0)
    wst_load = pltpu.make_async_copy(wst_hbm, wst, load_sem.at[1])
    wl_load = loaded(wg_hbm.at[:, pl.ds(wides * WIDE, rest)], wl, 2)
    wbc_load = loaded(wbc_hbm, wa.at[0, :, pl.ds(0, 2 * STATE)], 3)
    wr_load = loaded(
        wi_hbm.at[:, pl.ds(wides * WIDE, rest)], wa.at[0, :, pl.ds(2 * STATE, rest)], 4
    )
    wi_load = [
        loaded(wi_hbm.at[:, pl.ds(c * WIDE, WIDE)], wa.at[1 + c], 5 + c) for c in range(wides)
    ]
    wg_load = [
        loaded(wg_hbm.at[:, pl.ds(c * WIDE, WIDE)], wg.at[c], 5 + wides + c) for c in range(wides)
    ]
    wo_load = [
        pltpu.make_async_copy(
            wo_hbm.at[:, pl.ds(c * CHUNK, CHUNK)], wo.at[c], load_sem.at[5 + 2 * wides]
        )
        for c in range(2 * chunks)
    ]
    small_load = [
        pltpu.make_async_copy(src, dst, small_sem.at[i])
        for i, (src, dst) in enumerate(
            (
                (bias_hbm, bias),
                (decay_log_hbm, decay_log),
                (conv_b_hbm, conv_b),
                (off_b_hbm, off_b),
                (conv_i_hbm, conv_i),
                (off_i_hbm, off_1),
                (skip_hbm, skip),
                (norm_hbm, norm_1),
            )
        )
    ]
    for copy in small_load:
        copy.start()
    tok_load.start()
    wst_load.start()
    wbc_load.start()
    wr_load.start()

    barrier = pltpu.get_barrier_semaphore()

    def greet_seq(i, carry):
        pl.semaphore_signal(
            barrier,
            inc=1,
            device_id={"seq": lax.rem(r + i, seqs), "head": g},
            device_id_type=MESH,
        )
        return carry

    lax.fori_loop(1, seqs, greet_seq, 0)
    for other in (right, left, across):
        pl.semaphore_signal(
            barrier, inc=1, device_id={"seq": r, "head": other}, device_id_type=MESH
        )

    def far_copy(src, dst, ss, rs, seq, head):
        return pltpu.make_async_remote_copy(
            src_ref=src,
            dst_ref=dst,
            send_sem=ss,
            recv_sem=rs,
            device_id={"seq": seq, "head": head},
            device_id_type=MESH,
        )

    lane = lax.broadcasted_iota(jnp.int32, (SPAN, SPAN), 1)
    sub = lax.broadcasted_iota(jnp.int32, (SPAN, SPAN), 0)
    low = lane < HEADDIM
    low_row = low[:1]
    head_of = lax.broadcasted_iota(jnp.int32, (SPAN, width), 1) // HEADDIM
    onto = jnp.where(head_of == lax.broadcasted_iota(jnp.int32, (SPAN, width), 0), 1.0, 0.0)
    spread[pl.ds(0, SPAN), :] = onto.astype(BF16)
    spread[pl.ds(SPAN, SPAN), :] = onto.astype(BF16)
    terms[...] = jnp.zeros_like(terms)
    dt_ref[...] = jnp.zeros_like(dt_ref)
    wst_load.wait()
    tok_load.wait()
    for copy in wi_load:
        copy.start()
    for side in range(2):
        at = pl.ds(side * (rows // 2), rows // 2)
        dt_ref[at, pl.ds(0, heads)] = lax.dot_general(
            tok[at, :], wst[...], (((1,), (1,)), ((), ())), preferred_element_type=F32
        )

    def raw_part(q, m):
        at = rows // 2 * m
        v = dot(tok[pl.ds(at, rows // 2), :], wa[q]).astype(BF16).astype(F32)
        for j in range(WIDE // SPAN):
            raw[q, j, pl.ds(HALO + at, rows // 2), :] = v[:, j * SPAN : (j + 1) * SPAN]

    wbc_load.wait()
    wr_load.wait()
    raw_part(0, 1)
    for copy in small_load:
        copy.wait()
    off_i = off_1[...].reshape(1, -1)
    norm_w = norm_1[...].reshape(1, -1)
    step = dt_ref[:, pl.ds(0, heads)] + bias[...]
    tail = jnp.exp(-jnp.abs(step))
    up = 1.0 + tail
    log1p = jnp.where(up == 1.0, tail, jnp.log(up) * (tail / jnp.where(up == 1.0, 1.0, up - 1.0)))
    dt = jnp.maximum(step, 0.0) + log1p
    log_a = dt * (-LOG2E * jnp.exp(decay_log[...]))
    dt_ref[:, pl.ds(0, heads)] = dt
    for t, term in enumerate(split(log_a, 3)):
        for k in range(spans):
            terms[pl.ds(t * SPAN, SPAN), pl.ds(k * SPAN, heads)] = term[k * SPAN : (k + 1) * SPAN]
    tri = jnp.where(lane <= sub, 1.0, 0.0).astype(BF16)
    wi_load[0].wait()
    raw_part(1, 1)
    cums = dot(jnp.concatenate([tri, tri, tri], axis=1), terms[...])
    ends = []
    for k in range(spans):
        at = pl.ds(k * SPAN, SPAN)
        cum = cums[:, k * SPAN : (k + 1) * SPAN]
        cum_ref[at, :] = cum
        end_w = jnp.exp2(jnp.minimum(cum[SPAN - 1 :, :] - cum, 0.0)) * dt_ref[at, :]
        ends.append(jnp.concatenate(split(end_w, 2), axis=1))
    w_end[...] = dot(jnp.concatenate(ends, axis=0), spread[...])

    for q in range(1, wides):
        wi_load[q].wait()
        raw_part(1 + q, 1)
    wl_load.start()
    for copy in wg_load:
        copy.start()
    for copy in wo_load:
        copy.start()

    pl.semaphore_wait(barrier, seqs + 2)

    edge = far_copy(
        raw.at[:, :, pl.ds(rows, HALO), :],
        raw.at[:, :, pl.ds(0, HALO), :],
        halo_sem.at[0],
        halo_sem.at[1],
        lax.rem(r + 1, seqs),
        g,
    )

    @pl.when(r < seqs - 1)
    def _():
        edge.start()

    def gate_store(v, cols):
        gate[:, cols] = silu(v.astype(BF16).astype(F32))

    order = [wides * WIDE + j * SPAN for j in range(rest // SPAN)]
    order += [j * SPAN for j in range(wides * WIDE // SPAN)]
    per_side = len(order) // 2
    place = {col: divmod(n, per_side) for n, col in enumerate(order)}
    my_tile = r // 2
    my_side = lax.rem(r, 2)
    chips = seqs // 2

    group = seqs // 4
    row = r // group

    def dec_copy(dst):
        return far_copy(
            dec_send.at[lax.rem(dst, 2)], dec_recv.at[r], dec_ss.at[0], dec_rs.at[row], dst, g
        )

    def st_copy(side, chip):
        return far_copy(
            st_send.at[side, chip],
            st_recv.at[r],
            st_ss.at[0],
            st_rs.at[row],
            chip * 2 + side,
            g,
        )

    def pf_copy(dst):
        return far_copy(
            pf_send.at[dst], pf_recv.at[my_side, my_tile], pf_ss.at[0], pf_rs.at[0], dst, g
        )

    def bulk(ref, ss, rs):
        return far_copy(ref, ref, ss, rs, r, g)

    def each(first, last, act):
        def one(d, carry):
            act(d)
            return carry

        lax.fori_loop(first, jnp.minimum(r, last), one, 0)
        lax.fori_loop(jnp.maximum(r + 1, first), last, one, 0)

    def to_side(side, act):
        def one(i, carry):
            chip = my_tile + i
            act(side, jnp.where(chip >= chips, chip - chips, chip))
            return carry

        lax.fori_loop(1, chips, one, 0)

        @pl.when(my_side != side)
        def _():
            act(side, my_tile)

    total = jnp.zeros((1, SPAN), F32)
    for k in range(spans):
        total = total + cum_ref[pl.ds(k * SPAN + SPAN - 1, 1), :]
    total = jnp.exp2(total)
    for col, (side, n) in place.items():
        p = col // SPAN
        dec_send[side, :, pl.ds(n * SPAN, SPAN)] = jnp.where(
            low_row,
            jnp.broadcast_to(total[:, 2 * p : 2 * p + 1], (1, SPAN)),
            jnp.broadcast_to(total[:, 2 * p + 1 : 2 * p + 2], (1, SPAN)),
        )
    each(0, seqs, lambda d: dec_copy(d).start())
    dec_recv[r] = dec_send[my_side]

    def conv(q, j, taps, offset, col, dst, blocks):
        cols = pl.ds(col, SPAN)
        for b in blocks:
            acc = offset[:, cols]
            for k in range(KERNEL):
                at = pl.ds(HALO - KERNEL + 1 + k + b * BLOCK, BLOCK)
                acc = acc + taps[pl.ds(k, 1), cols] * raw[q, j, at, :]
            dst[pl.ds(b * BLOCK, BLOCK), cols] = silu(acc).astype(BF16)

    tiles = STATE // 8

    def local_state(col):
        cols = pl.ds(col, SPAN)
        p = col // SPAN
        side, n = place[col]
        held = jnp.zeros((STATE, SPAN), F32)
        for k in range(spans):
            own = pl.ds(k * SPAN, SPAN)
            last = jnp.exp2(cum_ref[pl.ds(k * SPAN + SPAN - 1, 1), :])
            d = jnp.where(
                low_row,
                jnp.broadcast_to(last[:, 2 * p : 2 * p + 1], (1, SPAN)),
                jnp.broadcast_to(last[:, 2 * p + 1 : 2 * p + 2], (1, SPAN)),
            )
            prior[k, :, cols] = held.astype(BF16)
            scaled = (xs_ref[own, cols].astype(F32) * w_end[own, cols]).astype(BF16)
            held = d * held + dot(wt_ref[k], scaled)
        st_send[side, :, :, pl.ds(n * SPAN, SPAN)] = held.reshape(tiles, 8, SPAN).astype(LINK)
        if n == per_side - 1:
            to_side(side, lambda at, chip: st_copy(at, chip).start())

            @pl.when(my_side == side)
            def _():
                st_recv[r] = st_send[side, my_tile]

    def gate_wide(c):
        wg_load[c].wait()
        gate_store(dot(tok[...], wg[c]), pl.ds(c * WIDE, WIDE))

    convs = [(0, j, conv_b, off_b, j * SPAN, bc_ref) for j in range(2 * STATE // SPAN)]
    for n, col in enumerate(order):
        q, j = divmod(2 * STATE // SPAN + n, WIDE // SPAN)
        convs.append((q, j, conv_i, off_i, col, xs_ref))
    middle = rows // BLOCK // 2
    upper = range(middle + 1, rows // BLOCK)
    lower = range(1, middle + 1)
    per_part = WIDE // SPAN
    raw_part(0, 0)
    for args in convs:
        conv(*args, upper)
    for q in range(1, 1 + wides):
        raw_part(q, 0)
        for args in convs[(q - 1) * per_part : q * per_part]:
            conv(*args, lower)
    for args in convs[wides * per_part :]:
        conv(*args, lower)

    @pl.when(r == 0)
    def _():
        raw[:, :, pl.ds(0, HALO), :] = jnp.zeros((1 + wides, WIDE // SPAN, HALO, SPAN), F32)

    @pl.when(r > 0)
    def _():
        edge.wait_recv()

    for args in convs:
        conv(*args, range(1))
    for k in range(spans):
        wt_ref[k] = bc_ref[pl.ds(k * SPAN, SPAN), pl.ds(0, STATE)].astype(F32).T.astype(BF16)
    for col in order:
        local_state(col)

    def within(k, carry):
        at = pl.ds(pl.multiple_of(k * SPAN, SPAN), SPAN)
        cum = cum_ref[at, :]
        cum_t = cum.T
        dt_t = dt_ref[at, :].T
        read = bc_ref[at, pl.ds(STATE, STATE)]
        write_t = wt_ref[k]
        scores = jnp.where(lane <= sub, dot(read, write_t), 0.0)
        base = carry
        for p in range(pairs):
            cols = pl.ds(p * SPAN, SPAN)
            x = xs_ref[at, cols]
            shown = []
            weights = []
            for h in (2 * p, 2 * p + 1):
                spread = jnp.broadcast_to(cum[:, h : h + 1], (SPAN, SPAN))
                shown.append(spread)
                gap = jnp.minimum(spread - cum_t[h : h + 1, :], 0.0)
                weights.append((scores * jnp.exp2(gap) * dt_t[h : h + 1, :]).astype(BF16))
            zero = jnp.zeros_like(x)
            both = jnp.concatenate([jnp.where(low, x, zero), jnp.where(low, zero, x)], axis=0)
            intra = dot(jnp.concatenate(weights, axis=1), both)
            scale = jnp.exp2(jnp.where(low, shown[0], shown[1]))
            inter = scale * dot(read, prior[k, :, cols])
            ahead = jnp.exp2(
                jnp.where(
                    low_row,
                    jnp.broadcast_to(base[:, 2 * p : 2 * p + 1], (1, SPAN)),
                    jnp.broadcast_to(base[:, 2 * p + 1 : 2 * p + 2], (1, SPAN)),
                )
            )
            gain = jnp.where(
                low_row,
                jnp.broadcast_to(skip[:, 2 * p : 2 * p + 1], (1, SPAN)),
                jnp.broadcast_to(skip[:, 2 * p + 1 : 2 * p + 2], (1, SPAN)),
            )
            opened = gate[at, cols]
            part_a[at, cols] = (intra + inter + gain * x.astype(F32)) * opened
            part_b[at, cols] = scale * ahead * opened
        return base + cum[SPAN - 1 :, :]

    def own_scan(begin, end):
        def arrived(q, count):
            at = pl.ds(q * group, count)
            bulk(dec_recv.at[at], dec_ss.at[0], dec_rs.at[q]).wait_recv()
            bulk(st_recv.at[at], st_ss.at[0], st_rs.at[q]).wait_recv()

        def scan(d, carry):
            pf_send[d] = carry.astype(LINK)
            return dec_recv[d] * carry + st_recv[d].astype(F32)

        def one_group(q, carry):
            @pl.when(q == row)
            def _():
                arrived(q, group - 1)

            @pl.when(q != row)
            def _():
                arrived(q, group)

            first, last = q * group, (q + 1) * group
            held_scan[...] = lax.fori_loop(first, last, scan, held_scan[...])
            each(first, last, lambda d: pf_copy(d).start())

            @pl.when(q == row)
            def _():
                pf_recv[my_side, my_tile] = pf_send[r]

            return carry

        lax.fori_loop(begin, end, one_group, 0)

    def rounds(before, after):
        def of(done):
            return jnp.where(
                row == 0,
                done[0],
                jnp.where(row == 1, done[1], jnp.where(row == 2, done[2], done[3])),
            )

        own_scan(of(before), of(after))

    done = ((0, 0, 0, 0), (0, 0, 1, 1), (1, 2, 4, 4), (4, 4, 4, 4))

    held_scan[...] = jnp.zeros((8, half), F32)

    gate_wide(0)
    gate_wide(1)
    rounds(done[0], done[1])
    wl_load.wait()
    gate_store(dot(tok[...], wl[...]), pl.ds(wides * WIDE, rest))
    rounds(done[1], done[2])
    base = lax.fori_loop(0, spans // 2, within, jnp.zeros((1, SPAN), F32))
    rounds(done[2], done[3])
    lax.fori_loop(spans // 2, spans, within, base)
    pltpu.make_async_copy(wo, wo, load_sem.at[5 + 2 * wides]).wait()

    bulk(pf_send.at[pl.ds(0, seqs - 1)], pf_ss.at[0], pf_rs.at[0]).wait_recv()
    for side in range(2):
        got = pf_recv[side].astype(F32).reshape(STATE, half).astype(BF16)
        for col, (at, n) in place.items():
            if at == side:
                s_in[:, pl.ds(col, SPAN)] = got[:, n * SPAN : (n + 1) * SPAN]

    eye = jnp.where(lane == sub, 1.0, 0.0).astype(F32)

    def gated(slot, block):
        at = pl.ds(pl.multiple_of(block * SPAN, SPAN), SPAN)
        read = bc_ref[at, pl.ds(STATE, STATE)]
        squares = jnp.zeros((SPAN, CHUNK), F32)
        for c in range(chunks):
            cols = pl.ds(c * CHUNK, CHUNK)
            pre = part_a[at, cols] + part_b[at, cols] * dot(read, s_in[:, cols])
            squares = squares + pre * pre
            gw[slot, :, cols] = (pre * norm_w[:, cols]).astype(BF16)
        column = jnp.sum(squares, axis=1, keepdims=True)
        row = jnp.sum(eye * column, axis=0, keepdims=True)
        sq_send[slot] = jnp.broadcast_to(row, (8, SPAN))

    def sq_copy(slot, offset):
        return far_copy(
            sq_send.at[slot],
            sq_recv.at[offset - 1],
            sq_ss.at[0],
            sq_rs.at[0],
            r,
            lax.rem(g + offset, parts),
        )

    def stream(send, recv, ss, rs, c, way):
        at = way * chunks + c
        return far_copy(
            send.at[at],
            recv.at[at],
            ss.at[0],
            rs.at[0] if rs is not comb_rs else rs.at[c // (chunks - 1)],
            r,
            (right, left)[way],
        )

    def far_step(c, carry):
        for way in range(2):
            far_send[way * chunks + c] = dot(gw[0], wo[way * chunks + c]).astype(BF16)
            stream(far_send, far_recv, far_ss, far_rs, c, way).start()
        return carry

    def own_step(c, carry):
        for way in range(2):
            own_send[way * chunks + c] = dot(gw[1 + way], wo[(1 - way) * chunks + c]).astype(BF16)
            stream(own_send, own_recv, own_ss, own_rs, c, way).start()
        return carry

    def mine_step(c, carry):
        mine[c] = dot(gw[3], wo[c])
        return carry

    def comb_step(c, carry):
        for way in range(2):
            at = way * chunks + c
            value = dot(gw[1 + way], wo[at])
            comb_send[at] = (value + far_recv[at].astype(F32)).astype(BF16)
            stream(comb_send, comb_recv, comb_ss, comb_rs, c, way).start()
        return carry

    gated(0, across)
    sq_copy(0, 2).start()
    lax.fori_loop(0, chunks, far_step, 0)
    gated(1, right)
    sq_copy(1, 1).start()
    gated(2, left)
    sq_copy(2, 3).start()
    lax.fori_loop(0, chunks, own_step, 0)
    gated(3, g)
    lax.fori_loop(0, 2 * chunks, mine_step, 0)
    bulk(far_recv, far_ss.at[0], far_rs.at[0]).wait_recv()
    lax.fori_loop(0, chunks, comb_step, 0)

    others = pl.ds(0, seqs - 1)
    bulk(dec_recv.at[others], dec_ss.at[0], dec_rs.at[0]).wait_send()
    bulk(st_recv.at[others], st_ss.at[0], st_rs.at[0]).wait_send()
    bulk(pf_send.at[others], pf_ss.at[0], pf_rs.at[0]).wait_send()

    @pl.when(r < seqs - 1)
    def _():
        edge.wait_send()

    bulk(sq_recv, sq_ss.at[0], sq_rs.at[0]).wait_send()
    bulk(far_send, far_ss.at[0], far_rs.at[0]).wait_send()
    bulk(own_send, own_ss.at[0], own_rs.at[0]).wait_send()

    bulk(sq_recv, sq_ss.at[0], sq_rs.at[0]).wait_recv()
    squares = sq_send[3] + sq_recv[0] + sq_recv[1] + sq_recv[2]
    scale_row = 1.0 / jnp.sqrt(squares[:1] * (1.0 / inner_all) + EPS)
    scale = jnp.sum(eye * scale_row, axis=1, keepdims=True)

    bulk(own_recv, own_ss.at[0], own_rs.at[0]).wait_recv()
    for c in range(chunks):
        if c == 0:
            bulk(comb_recv.at[pl.ds(0, 2 * chunks - 2)], comb_ss.at[0], comb_rs.at[0]).wait_recv()
        if c == chunks - 1:
            bulk(comb_recv.at[pl.ds(0, 2)], comb_ss.at[0], comb_rs.at[1]).wait_recv()
        value = mine[c] + own_recv[chunks + c].astype(F32) + comb_recv[c].astype(F32)
        out[:, pl.ds(c * CHUNK, CHUNK)] = (value * scale).astype(BF16)
        value = mine[chunks + c] + own_recv[c].astype(F32) + comb_recv[chunks + c].astype(F32)
        out[:, pl.ds((chunks + c) * CHUNK, CHUNK)] = (value * scale).astype(BF16)

    bulk(comb_send, comb_ss.at[0], comb_rs.at[0]).wait_send()


def per_device(
    seqs,
    parts,
    tokens,
    proj_inner,
    proj_gate,
    proj_bc,
    proj_step,
    conv_inner,
    conv_bc,
    offset_inner,
    offset_bc,
    step_bias,
    decay_log,
    skip_gain,
    norm_weight,
    out_weight,
):
    rows, depth = tokens.shape
    width = proj_inner.shape[1]
    heads = step_bias.shape[0]
    chunks = width // CHUNK
    spans = rows // SPAN
    half = width // 2
    tiles = STATE // 8
    model = out_weight.shape[1]
    any_spec = pl.BlockSpec(memory_space=pl.ANY)
    vmem = pl.BlockSpec(memory_space=pltpu.VMEM)
    dma = pltpu.SemaphoreType.DMA
    streams = [pltpu.VMEM((2 * chunks, SPAN, CHUNK), BF16)] * 6
    scratch = [
        pltpu.VMEM((KERNEL, width), F32),
        pltpu.VMEM((KERNEL, 2 * STATE), F32),
        pltpu.VMEM((width,), F32),
        pltpu.VMEM((1, 2 * STATE), F32),
        pltpu.VMEM((1, heads), F32),
        pltpu.VMEM((1, heads), F32),
        pltpu.VMEM((1, heads), F32),
        pltpu.VMEM((width,), F32),
        pltpu.VMEM((rows, depth), BF16),
        pltpu.VMEM((1 + width // WIDE, depth, WIDE), BF16),
        pltpu.VMEM((width // WIDE, depth, WIDE), BF16),
        pltpu.VMEM((depth, width % WIDE), BF16),
        pltpu.VMEM((heads, depth), BF16),
        pltpu.VMEM((2 * chunks, width, CHUNK), BF16),
        pltpu.VMEM((1 + width // WIDE, WIDE // SPAN, rows + HALO, SPAN), F32),
        pltpu.VMEM((3 * SPAN, spans * SPAN), BF16),
        pltpu.VMEM((2 * SPAN, width), BF16),
        pltpu.VMEM((rows, width), F32),
        pltpu.VMEM((rows, width), BF16),
        pltpu.VMEM((rows, 2 * STATE), BF16),
        pltpu.VMEM((spans, STATE, SPAN), BF16),
        pltpu.VMEM((rows, SPAN), F32),
        pltpu.VMEM((rows, SPAN), F32),
        pltpu.VMEM((rows, width), F32),
        pltpu.VMEM((rows, width), F32),
        pltpu.VMEM((rows, width), F32),
        pltpu.VMEM((spans, STATE, width), BF16),
        pltpu.VMEM((2, tiles, 8, half), LINK),
        pltpu.VMEM((seqs, 8, half), LINK),
        pltpu.VMEM((2, 1, half), F32),
        pltpu.VMEM((seqs, 1, half), F32),
        pltpu.VMEM((seqs, 8, half), LINK),
        pltpu.VMEM((2, tiles, 8, half), LINK),
        pltpu.VMEM((STATE, width), BF16),
        pltpu.VMEM((8, half), F32),
        pltpu.VMEM((4, SPAN, width), BF16),
        *streams,
        pltpu.VMEM((2 * chunks, SPAN, CHUNK), F32),
        pltpu.VMEM((4, 8, SPAN), F32),
        pltpu.VMEM((3, 8, SPAN), F32),
        dma((6 + 2 * (width // WIDE),)),
        dma((8,)),
        dma((2,)),
        dma((1,)),
        dma((4,)),
        dma((1,)),
        dma((4,)),
        dma((1,)),
        dma((1,)),
        dma((1,)),
        dma((1,)),
        dma((1,)),
        dma((1,)),
        dma((1,)),
        dma((2,)),
        dma((1,)),
        dma((1,)),
    ]
    row = lambda v: v.reshape(1, -1)
    return pl.pallas_call(
        functools.partial(kernel, seqs, parts, float(parts * width)),
        out_shape=pltpu.VMEM((rows // parts, model), BF16),
        in_specs=[any_spec] * 14,
        out_specs=vmem,
        scratch_shapes=scratch,
        compiler_params=pltpu.CompilerParams(
            collective_id=0, has_side_effects=True, vmem_limit_bytes=62 * 1024 * 1024
        ),
    )(
        tokens,
        proj_inner,
        proj_gate,
        proj_bc,
        proj_step.T,
        conv_inner,
        conv_bc,
        offset_inner,
        row(offset_bc),
        row(step_bias),
        row(decay_log),
        row(skip_gain),
        norm_weight,
        out_weight,
    )


def solution(mesh):
    body = functools.partial(per_device, mesh.shape["seq"], mesh.shape["head"])
    return jax.shard_map(
        body,
        mesh=mesh,
        in_specs=(
            P("seq", None),
            P(None, "head"),
            P(None, "head"),
            P(),
            P(None, "head"),
            P(None, "head"),
            P(),
            P("head"),
            P(),
            P("head"),
            P("head"),
            P("head"),
            P("head"),
            P("head", None),
        ),
        out_specs=P(("seq", "head"), None),
        check_vma=False,
    )
```

```python
import functools

import jax
import jax.numpy as jnp
from jax import lax
from jax.experimental import pallas as pl
from jax.experimental.pallas import tpu as pltpu
from jax.sharding import PartitionSpec as P

HEADDIM = 64
STATE = 128
KERNEL = 4
SPAN = 128
HALO = 8
CHUNK = 256
BLOCK = 64
WIDE = 512
PIECES = 4
LOG2E = 1.4426950408889634
EPS = 0.25
MESH = pl.DeviceIdType.MESH
F32 = jnp.float32
BF16 = jnp.bfloat16
LINK = jnp.bfloat16


def silu(v):
    return v / (1.0 + jnp.exp(-v))


def dot(a, b):
    return jnp.dot(a, b, preferred_element_type=F32)


def split(v, count):
    terms = []
    for _ in range(count):
        terms.append(v.astype(BF16))
        v = v - terms[-1].astype(F32)
    return terms


def kernel(
    seqs,
    parts,
    inner_all,
    tokens_hbm,
    wi_hbm,
    wg_hbm,
    wbc_hbm,
    wst_hbm,
    conv_i_hbm,
    conv_b_hbm,
    off_i_hbm,
    off_b_hbm,
    bias_hbm,
    decay_log_hbm,
    skip_hbm,
    norm_hbm,
    wo_hbm,
    out,
    conv_i,
    conv_b,
    off_1,
    off_b,
    bias,
    decay_log,
    skip,
    norm_1,
    tok,
    wa,
    wg,
    wl,
    wst,
    wo,
    raw,
    terms,
    spread,
    w_end,
    xs_ref,
    bc_ref,
    wt_ref,
    cum_ref,
    dt_ref,
    gate,
    part_a,
    part_b,
    prior,
    st_send,
    st_recv,
    dec_send,
    dec_recv,
    pf_send,
    pf_recv,
    s_in,
    held_scan,
    gw,
    far_send,
    far_recv,
    own_send,
    own_recv,
    comb_send,
    comb_recv,
    mine,
    sq_send,
    sq_recv,
    load_sem,
    small_sem,
    halo_sem,
    dec_ss,
    dec_rs,
    st_ss,
    st_rs,
    pf_ss,
    pf_rs,
    far_ss,
    far_rs,
    own_ss,
    own_rs,
    comb_ss,
    comb_rs,
    sq_ss,
    sq_rs,
):
    r = lax.axis_index("seq")
    g = lax.axis_index("head")
    rows = tokens_hbm.shape[0]
    width = wi_hbm.shape[1]
    spans = rows // SPAN
    heads = width // HEADDIM
    pairs = heads // 2
    chunks = width // CHUNK
    half = width // 2
    right = lax.rem(g + 1, parts)
    left = lax.rem(g + parts - 1, parts)
    across = lax.rem(g + 2, parts)

    class loaded:
        def __init__(self, src, dst, number):
            self.whole = pltpu.make_async_copy(src, dst, load_sem.at[number])
            block = src.shape[0] // PIECES
            self.pieces = [
                pltpu.make_async_copy(
                    src.at[pl.ds(i * block, block), :],
                    dst.at[pl.ds(i * block, block), :],
                    load_sem.at[number],
                )
                for i in range(PIECES)
            ]

        def start(self):
            for piece in self.pieces:
                piece.start()

        def wait(self):
            self.whole.wait()

    wides = width // WIDE
    rest = width - wides * WIDE
    tok_load = loaded(tokens_hbm, tok, 0)
    wst_load = pltpu.make_async_copy(wst_hbm, wst, load_sem.at[1])
    wl_load = loaded(wg_hbm.at[:, pl.ds(wides * WIDE, rest)], wl, 2)
    wbc_load = loaded(wbc_hbm, wa.at[0, :, pl.ds(0, 2 * STATE)], 3)
    wr_load = loaded(
        wi_hbm.at[:, pl.ds(wides * WIDE, rest)], wa.at[0, :, pl.ds(2 * STATE, rest)], 4
    )
    wi_load = [
        loaded(wi_hbm.at[:, pl.ds(c * WIDE, WIDE)], wa.at[1 + c], 5 + c) for c in range(wides)
    ]
    wg_load = [
        loaded(wg_hbm.at[:, pl.ds(c * WIDE, WIDE)], wg.at[c], 5 + wides + c) for c in range(wides)
    ]
    wo_load = [
        pltpu.make_async_copy(
            wo_hbm.at[:, pl.ds(c * CHUNK, CHUNK)], wo.at[c], load_sem.at[5 + 2 * wides]
        )
        for c in range(2 * chunks)
    ]
    small_load = [
        pltpu.make_async_copy(src, dst, small_sem.at[i])
        for i, (src, dst) in enumerate(
            (
                (bias_hbm, bias),
                (decay_log_hbm, decay_log),
                (conv_b_hbm, conv_b),
                (off_b_hbm, off_b),
                (conv_i_hbm, conv_i),
                (off_i_hbm, off_1),
                (skip_hbm, skip),
                (norm_hbm, norm_1),
            )
        )
    ]
    for copy in small_load:
        copy.start()
    tok_load.start()
    wst_load.start()
    wbc_load.start()
    wr_load.start()

    barrier = pltpu.get_barrier_semaphore()

    def greet_seq(i, carry):
        pl.semaphore_signal(
            barrier,
            inc=1,
            device_id={"seq": lax.rem(r + i, seqs), "head": g},
            device_id_type=MESH,
        )
        return carry

    lax.fori_loop(1, seqs, greet_seq, 0)
    for other in (right, left, across):
        pl.semaphore_signal(
            barrier, inc=1, device_id={"seq": r, "head": other}, device_id_type=MESH
        )

    def far_copy(src, dst, ss, rs, seq, head):
        return pltpu.make_async_remote_copy(
            src_ref=src,
            dst_ref=dst,
            send_sem=ss,
            recv_sem=rs,
            device_id={"seq": seq, "head": head},
            device_id_type=MESH,
        )

    lane = lax.broadcasted_iota(jnp.int32, (SPAN, SPAN), 1)
    sub = lax.broadcasted_iota(jnp.int32, (SPAN, SPAN), 0)
    low = lane < HEADDIM
    low_row = low[:1]
    head_of = lax.broadcasted_iota(jnp.int32, (SPAN, width), 1) // HEADDIM
    onto = jnp.where(head_of == lax.broadcasted_iota(jnp.int32, (SPAN, width), 0), 1.0, 0.0)
    spread[pl.ds(0, SPAN), :] = onto.astype(BF16)
    spread[pl.ds(SPAN, SPAN), :] = onto.astype(BF16)
    terms[...] = jnp.zeros_like(terms)
    dt_ref[...] = jnp.zeros_like(dt_ref)
    wst_load.wait()
    tok_load.wait()
    for copy in wi_load:
        copy.start()
    for side in range(2):
        at = pl.ds(side * (rows // 2), rows // 2)
        dt_ref[at, pl.ds(0, heads)] = lax.dot_general(
            tok[at, :], wst[...], (((1,), (1,)), ((), ())), preferred_element_type=F32
        )

    def raw_part(q, m):
        at = rows // 2 * m
        v = dot(tok[pl.ds(at, rows // 2), :], wa[q]).astype(BF16).astype(F32)
        for j in range(WIDE // SPAN):
            raw[q, j, pl.ds(HALO + at, rows // 2), :] = v[:, j * SPAN : (j + 1) * SPAN]

    wbc_load.wait()
    wr_load.wait()
    raw_part(0, 1)
    for copy in small_load:
        copy.wait()
    off_i = off_1[...].reshape(1, -1)
    norm_w = norm_1[...].reshape(1, -1)
    step = dt_ref[:, pl.ds(0, heads)] + bias[...]
    tail = jnp.exp(-jnp.abs(step))
    up = 1.0 + tail
    log1p = jnp.where(up == 1.0, tail, jnp.log(up) * (tail / jnp.where(up == 1.0, 1.0, up - 1.0)))
    dt = jnp.maximum(step, 0.0) + log1p
    log_a = dt * (-LOG2E * jnp.exp(decay_log[...]))
    dt_ref[:, pl.ds(0, heads)] = dt
    for t, term in enumerate(split(log_a, 3)):
        for k in range(spans):
            terms[pl.ds(t * SPAN, SPAN), pl.ds(k * SPAN, heads)] = term[k * SPAN : (k + 1) * SPAN]
    tri = jnp.where(lane <= sub, 1.0, 0.0).astype(BF16)
    wi_load[0].wait()
    raw_part(1, 1)
    cums = dot(jnp.concatenate([tri, tri, tri], axis=1), terms[...])
    ends = []
    for k in range(spans):
        at = pl.ds(k * SPAN, SPAN)
        cum = cums[:, k * SPAN : (k + 1) * SPAN]
        cum_ref[at, :] = cum
        end_w = jnp.exp2(jnp.minimum(cum[SPAN - 1 :, :] - cum, 0.0)) * dt_ref[at, :]
        ends.append(jnp.concatenate(split(end_w, 2), axis=1))
    w_end[...] = dot(jnp.concatenate(ends, axis=0), spread[...])

    for q in range(1, wides):
        wi_load[q].wait()
        raw_part(1 + q, 1)
    wl_load.start()
    for copy in wg_load:
        copy.start()
    for copy in wo_load:
        copy.start()

    pl.semaphore_wait(barrier, seqs + 2)

    edge = far_copy(
        raw.at[:, :, pl.ds(rows, HALO), :],
        raw.at[:, :, pl.ds(0, HALO), :],
        halo_sem.at[0],
        halo_sem.at[1],
        lax.rem(r + 1, seqs),
        g,
    )

    @pl.when(r < seqs - 1)
    def _():
        edge.start()

    def gate_store(v, cols):
        gate[:, cols] = silu(v.astype(BF16).astype(F32))

    order = [wides * WIDE + j * SPAN for j in range(rest // SPAN)]
    order += [j * SPAN for j in range(wides * WIDE // SPAN)]
    per_side = len(order) // 2
    place = {col: divmod(n, per_side) for n, col in enumerate(order)}
    my_tile = r // 2
    my_side = lax.rem(r, 2)
    chips = seqs // 2

    group = seqs // 4
    row = r // group

    def dec_copy(side, chip):
        return far_copy(
            dec_send.at[side], dec_recv.at[r], dec_ss.at[0], dec_rs.at[row], chip * 2 + side, g
        )

    def st_copy(side, chip):
        return far_copy(
            st_send.at[side, chip],
            st_recv.at[r],
            st_ss.at[0],
            st_rs.at[row],
            chip * 2 + side,
            g,
        )

    def pf_copy(dst):
        return far_copy(
            pf_send.at[dst], pf_recv.at[my_side, my_tile], pf_ss.at[0], pf_rs.at[0], dst, g
        )

    def bulk(ref, ss, rs):
        return far_copy(ref, ref, ss, rs, r, g)

    def each(first, last, act):
        def one(d, carry):
            act(d)
            return carry

        lax.fori_loop(first, jnp.minimum(r, last), one, 0)
        lax.fori_loop(jnp.maximum(r + 1, first), last, one, 0)

    def to_side(side, act):
        def one(i, carry):
            chip = my_tile + i
            act(side, jnp.where(chip >= chips, chip - chips, chip))
            return carry

        for i in range(1, chips):
            one(i, 0)

        @pl.when(my_side != side)
        def _():
            act(side, my_tile)

    total = jnp.zeros((1, SPAN), F32)
    for k in range(spans):
        total = total + cum_ref[pl.ds(k * SPAN + SPAN - 1, 1), :]
    total = jnp.exp2(total)
    for col, (side, n) in place.items():
        p = col // SPAN
        dec_send[side, :, pl.ds(n * SPAN, SPAN)] = jnp.where(
            low_row,
            jnp.broadcast_to(total[:, 2 * p : 2 * p + 1], (1, SPAN)),
            jnp.broadcast_to(total[:, 2 * p + 1 : 2 * p + 2], (1, SPAN)),
        )
    for side in range(2):
        to_side(side, lambda at, chip: dec_copy(at, chip).start())
    dec_recv[r] = dec_send[my_side]

    def conv(q, j, taps, offset, col, dst, blocks):
        cols = pl.ds(col, SPAN)
        for b in blocks:
            acc = offset[:, cols]
            for k in range(KERNEL):
                at = pl.ds(HALO - KERNEL + 1 + k + b * BLOCK, BLOCK)
                acc = acc + taps[pl.ds(k, 1), cols] * raw[q, j, at, :]
            dst[pl.ds(b * BLOCK, BLOCK), cols] = silu(acc).astype(BF16)

    tiles = STATE // 8

    def local_state(col):
        cols = pl.ds(col, SPAN)
        p = col // SPAN
        side, n = place[col]
        held = jnp.zeros((STATE, SPAN), F32)
        for k in range(spans):
            own = pl.ds(k * SPAN, SPAN)
            last = jnp.exp2(cum_ref[pl.ds(k * SPAN + SPAN - 1, 1), :])
            d = jnp.where(
                low_row,
                jnp.broadcast_to(last[:, 2 * p : 2 * p + 1], (1, SPAN)),
                jnp.broadcast_to(last[:, 2 * p + 1 : 2 * p + 2], (1, SPAN)),
            )
            prior[k, :, cols] = held.astype(BF16)
            scaled = (xs_ref[own, cols].astype(F32) * w_end[own, cols]).astype(BF16)
            held = d * held + dot(wt_ref[k], scaled)
        st_send[side, :, :, pl.ds(n * SPAN, SPAN)] = held.reshape(tiles, 8, SPAN).astype(LINK)
        if n == per_side - 1:
            to_side(side, lambda at, chip: st_copy(at, chip).start())

            @pl.when(my_side == side)
            def _():
                st_recv[r] = st_send[side, my_tile]

    def gate_wide(c):
        wg_load[c].wait()
        gate_store(dot(tok[...], wg[c]), pl.ds(c * WIDE, WIDE))

    convs = [(0, j, conv_b, off_b, j * SPAN, bc_ref) for j in range(2 * STATE // SPAN)]
    for n, col in enumerate(order):
        q, j = divmod(2 * STATE // SPAN + n, WIDE // SPAN)
        convs.append((q, j, conv_i, off_i, col, xs_ref))
    middle = rows // BLOCK // 2
    upper = range(middle + 1, rows // BLOCK)
    lower = range(1, middle + 1)
    per_part = WIDE // SPAN
    later = convs.pop(1)
    raw_part(0, 0)
    for args in convs:
        conv(*args, upper)
    for q in range(1, 1 + wides):
        raw_part(q, 0)
        for args in convs[max((q - 1) * per_part - 1, 0) : q * per_part - 1]:
            conv(*args, lower)
    for args in convs[wides * per_part - 1 :]:
        conv(*args, lower)

    @pl.when(r == 0)
    def _():
        raw[:, :, pl.ds(0, HALO), :] = jnp.zeros((1 + wides, WIDE // SPAN, HALO, SPAN), F32)

    @pl.when(r > 0)
    def _():
        edge.wait_recv()

    for args in convs:
        conv(*args, range(1))
    for k in range(spans):
        wt_ref[k] = bc_ref[pl.ds(k * SPAN, SPAN), pl.ds(0, STATE)].astype(F32).T.astype(BF16)
    for col in order:
        local_state(col)
    conv(*later, range(rows // BLOCK))

    def within(k, carry):
        at = pl.ds(pl.multiple_of(k * SPAN, SPAN), SPAN)
        cum = cum_ref[at, :]
        cum_t = cum.T
        dt_t = dt_ref[at, :].T
        read = bc_ref[at, pl.ds(STATE, STATE)]
        write_t = wt_ref[k]
        scores = jnp.where(lane <= sub, dot(read, write_t), 0.0)
        base = carry
        for p in range(pairs):
            cols = pl.ds(p * SPAN, SPAN)
            x = xs_ref[at, cols]
            shown = []
            weights = []
            for h in (2 * p, 2 * p + 1):
                spread = jnp.broadcast_to(cum[:, h : h + 1], (SPAN, SPAN))
                shown.append(spread)
                gap = jnp.minimum(spread - cum_t[h : h + 1, :], 0.0)
                weights.append((scores * jnp.exp2(gap) * dt_t[h : h + 1, :]).astype(BF16))
            zero = jnp.zeros_like(x)
            both = jnp.concatenate([jnp.where(low, x, zero), jnp.where(low, zero, x)], axis=0)
            intra = dot(jnp.concatenate(weights, axis=1), both)
            scale = jnp.exp2(jnp.where(low, shown[0], shown[1]))
            inter = scale * dot(read, prior[k, :, cols])
            ahead = jnp.exp2(
                jnp.where(
                    low_row,
                    jnp.broadcast_to(base[:, 2 * p : 2 * p + 1], (1, SPAN)),
                    jnp.broadcast_to(base[:, 2 * p + 1 : 2 * p + 2], (1, SPAN)),
                )
            )
            gain = jnp.where(
                low_row,
                jnp.broadcast_to(skip[:, 2 * p : 2 * p + 1], (1, SPAN)),
                jnp.broadcast_to(skip[:, 2 * p + 1 : 2 * p + 2], (1, SPAN)),
            )
            opened = gate[at, cols]
            part_a[at, cols] = (intra + inter + gain * x.astype(F32)) * opened
            part_b[at, cols] = scale * ahead * opened
        return base + cum[SPAN - 1 :, :]

    def own_scan(begin, end):
        def arrived(q, count):
            at = pl.ds(q * group, count)
            bulk(dec_recv.at[at], dec_ss.at[0], dec_rs.at[q]).wait_recv()
            bulk(st_recv.at[at], st_ss.at[0], st_rs.at[q]).wait_recv()

        def scan(d, carry):
            pf_send[d] = carry.astype(LINK)
            return dec_recv[d] * carry + st_recv[d].astype(F32)

        def one_group(q, carry):
            @pl.when(q == row)
            def _():
                arrived(q, group - 1)

            @pl.when(q != row)
            def _():
                arrived(q, group)

            first, last = q * group, (q + 1) * group
            held_scan[...] = lax.fori_loop(first, last, scan, held_scan[...])
            each(first, last, lambda d: pf_copy(d).start())

            @pl.when(q == row)
            def _():
                pf_recv[my_side, my_tile] = pf_send[r]

            return carry

        lax.fori_loop(begin, end, one_group, 0)

    def rounds(before, after):
        def of(done):
            return jnp.where(
                row == 0,
                done[0],
                jnp.where(row == 1, done[1], jnp.where(row == 2, done[2], done[3])),
            )

        own_scan(of(before), of(after))

    done = ((0, 0, 0, 0), (0, 0, 1, 1), (1, 2, 4, 4), (4, 4, 4, 4))

    held_scan[...] = jnp.zeros((8, half), F32)

    gate_wide(0)
    gate_wide(1)
    rounds(done[0], done[1])
    wl_load.wait()
    gate_store(dot(tok[...], wl[...]), pl.ds(wides * WIDE, rest))
    rounds(done[1], done[2])
    base = lax.fori_loop(0, spans // 2, within, jnp.zeros((1, SPAN), F32))
    rounds(done[2], done[3])
    lax.fori_loop(spans // 2, spans, within, base)
    pltpu.make_async_copy(wo, wo, load_sem.at[5 + 2 * wides]).wait()

    bulk(pf_send.at[pl.ds(0, seqs - 1)], pf_ss.at[0], pf_rs.at[0]).wait_recv()
    for side in range(2):
        got = pf_recv[side].astype(F32).reshape(STATE, half).astype(BF16)
        for col, (at, n) in place.items():
            if at == side:
                s_in[:, pl.ds(col, SPAN)] = got[:, n * SPAN : (n + 1) * SPAN]

    eye = jnp.where(lane == sub, 1.0, 0.0).astype(F32)

    def gated(slot, block):
        at = pl.ds(pl.multiple_of(block * SPAN, SPAN), SPAN)
        read = bc_ref[at, pl.ds(STATE, STATE)]
        squares = jnp.zeros((SPAN, CHUNK), F32)
        for c in range(chunks):
            cols = pl.ds(c * CHUNK, CHUNK)
            pre = part_a[at, cols] + part_b[at, cols] * dot(read, s_in[:, cols])
            squares = squares + pre * pre
            gw[slot, :, cols] = (pre * norm_w[:, cols]).astype(BF16)
        column = jnp.sum(squares, axis=1, keepdims=True)
        row = jnp.sum(eye * column, axis=0, keepdims=True)
        sq_send[slot] = jnp.broadcast_to(row, (8, SPAN))

    def sq_copy(slot, offset):
        return far_copy(
            sq_send.at[slot],
            sq_recv.at[offset - 1],
            sq_ss.at[0],
            sq_rs.at[0],
            r,
            lax.rem(g + offset, parts),
        )

    def stream(send, recv, ss, rs, c, way):
        at = way * chunks + c
        return far_copy(
            send.at[at],
            recv.at[at],
            ss.at[0],
            rs.at[0] if rs is not comb_rs else rs.at[c // (chunks - 1)],
            r,
            (right, left)[way],
        )

    def far_step(c, carry):
        for way in range(2):
            far_send[way * chunks + c] = dot(gw[0], wo[way * chunks + c]).astype(BF16)
            stream(far_send, far_recv, far_ss, far_rs, c, way).start()
        return carry

    def own_step(c, carry):
        for way in range(2):
            own_send[way * chunks + c] = dot(gw[1 + way], wo[(1 - way) * chunks + c]).astype(BF16)
            stream(own_send, own_recv, own_ss, own_rs, c, way).start()
        return carry

    def mine_step(c, carry):
        mine[c] = dot(gw[3], wo[c])
        return carry

    def comb_step(c, carry):
        for way in range(2):
            at = way * chunks + c
            value = dot(gw[1 + way], wo[at])
            comb_send[at] = (value + far_recv[at].astype(F32)).astype(BF16)
            stream(comb_send, comb_recv, comb_ss, comb_rs, c, way).start()
        return carry

    gated(0, across)
    sq_copy(0, 2).start()
    lax.fori_loop(0, chunks, far_step, 0)
    gated(1, right)
    sq_copy(1, 1).start()
    gated(2, left)
    sq_copy(2, 3).start()
    lax.fori_loop(0, chunks, own_step, 0)
    gated(3, g)
    lax.fori_loop(0, 2 * chunks, mine_step, 0)
    bulk(far_recv, far_ss.at[0], far_rs.at[0]).wait_recv()
    lax.fori_loop(0, chunks, comb_step, 0)

    others = pl.ds(0, seqs - 1)
    bulk(dec_recv.at[others], dec_ss.at[0], dec_rs.at[0]).wait_send()
    bulk(st_recv.at[others], st_ss.at[0], st_rs.at[0]).wait_send()
    bulk(pf_send.at[others], pf_ss.at[0], pf_rs.at[0]).wait_send()

    @pl.when(r < seqs - 1)
    def _():
        edge.wait_send()

    bulk(sq_recv, sq_ss.at[0], sq_rs.at[0]).wait_send()
    bulk(far_send, far_ss.at[0], far_rs.at[0]).wait_send()
    bulk(own_send, own_ss.at[0], own_rs.at[0]).wait_send()

    bulk(sq_recv, sq_ss.at[0], sq_rs.at[0]).wait_recv()
    squares = sq_send[3] + sq_recv[0] + sq_recv[1] + sq_recv[2]
    scale_row = 1.0 / jnp.sqrt(squares[:1] * (1.0 / inner_all) + EPS)
    scale = jnp.sum(eye * scale_row, axis=1, keepdims=True)

    bulk(own_recv, own_ss.at[0], own_rs.at[0]).wait_recv()
    for c in range(chunks):
        if c == 0:
            bulk(comb_recv.at[pl.ds(0, 2 * chunks - 2)], comb_ss.at[0], comb_rs.at[0]).wait_recv()
        if c == chunks - 1:
            bulk(comb_recv.at[pl.ds(0, 2)], comb_ss.at[0], comb_rs.at[1]).wait_recv()
        value = mine[c] + own_recv[chunks + c].astype(F32) + comb_recv[c].astype(F32)
        out[:, pl.ds(c * CHUNK, CHUNK)] = (value * scale).astype(BF16)
        value = mine[chunks + c] + own_recv[c].astype(F32) + comb_recv[chunks + c].astype(F32)
        out[:, pl.ds((chunks + c) * CHUNK, CHUNK)] = (value * scale).astype(BF16)

    bulk(comb_send, comb_ss.at[0], comb_rs.at[0]).wait_send()


def per_device(
    seqs,
    parts,
    tokens,
    proj_inner,
    proj_gate,
    proj_bc,
    proj_step,
    conv_inner,
    conv_bc,
    offset_inner,
    offset_bc,
    step_bias,
    decay_log,
    skip_gain,
    norm_weight,
    out_weight,
):
    rows, depth = tokens.shape
    width = proj_inner.shape[1]
    heads = step_bias.shape[0]
    chunks = width // CHUNK
    spans = rows // SPAN
    half = width // 2
    tiles = STATE // 8
    model = out_weight.shape[1]
    any_spec = pl.BlockSpec(memory_space=pl.ANY)
    vmem = pl.BlockSpec(memory_space=pltpu.VMEM)
    dma = pltpu.SemaphoreType.DMA
    streams = [pltpu.VMEM((2 * chunks, SPAN, CHUNK), BF16)] * 6
    scratch = [
        pltpu.VMEM((KERNEL, width), F32),
        pltpu.VMEM((KERNEL, 2 * STATE), F32),
        pltpu.VMEM((width,), F32),
        pltpu.VMEM((1, 2 * STATE), F32),
        pltpu.VMEM((1, heads), F32),
        pltpu.VMEM((1, heads), F32),
        pltpu.VMEM((1, heads), F32),
        pltpu.VMEM((width,), F32),
        pltpu.VMEM((rows, depth), BF16),
        pltpu.VMEM((1 + width // WIDE, depth, WIDE), BF16),
        pltpu.VMEM((width // WIDE, depth, WIDE), BF16),
        pltpu.VMEM((depth, width % WIDE), BF16),
        pltpu.VMEM((heads, depth), BF16),
        pltpu.VMEM((2 * chunks, width, CHUNK), BF16),
        pltpu.VMEM((1 + width // WIDE, WIDE // SPAN, rows + HALO, SPAN), F32),
        pltpu.VMEM((3 * SPAN, spans * SPAN), BF16),
        pltpu.VMEM((2 * SPAN, width), BF16),
        pltpu.VMEM((rows, width), F32),
        pltpu.VMEM((rows, width), BF16),
        pltpu.VMEM((rows, 2 * STATE), BF16),
        pltpu.VMEM((spans, STATE, SPAN), BF16),
        pltpu.VMEM((rows, SPAN), F32),
        pltpu.VMEM((rows, SPAN), F32),
        pltpu.VMEM((rows, width), F32),
        pltpu.VMEM((rows, width), F32),
        pltpu.VMEM((rows, width), F32),
        pltpu.VMEM((spans, STATE, width), BF16),
        pltpu.VMEM((2, tiles, 8, half), LINK),
        pltpu.VMEM((seqs, 8, half), LINK),
        pltpu.VMEM((2, 1, half), F32),
        pltpu.VMEM((seqs, 1, half), F32),
        pltpu.VMEM((seqs, 8, half), LINK),
        pltpu.VMEM((2, tiles, 8, half), LINK),
        pltpu.VMEM((STATE, width), BF16),
        pltpu.VMEM((8, half), F32),
        pltpu.VMEM((4, SPAN, width), BF16),
        *streams,
        pltpu.VMEM((2 * chunks, SPAN, CHUNK), F32),
        pltpu.VMEM((4, 8, SPAN), F32),
        pltpu.VMEM((3, 8, SPAN), F32),
        dma((6 + 2 * (width // WIDE),)),
        dma((8,)),
        dma((2,)),
        dma((1,)),
        dma((4,)),
        dma((1,)),
        dma((4,)),
        dma((1,)),
        dma((1,)),
        dma((1,)),
        dma((1,)),
        dma((1,)),
        dma((1,)),
        dma((1,)),
        dma((2,)),
        dma((1,)),
        dma((1,)),
    ]
    row = lambda v: v.reshape(1, -1)
    return pl.pallas_call(
        functools.partial(kernel, seqs, parts, float(parts * width)),
        out_shape=pltpu.VMEM((rows // parts, model), BF16),
        in_specs=[any_spec] * 14,
        out_specs=vmem,
        scratch_shapes=scratch,
        compiler_params=pltpu.CompilerParams(
            collective_id=0, has_side_effects=True, vmem_limit_bytes=62 * 1024 * 1024
        ),
    )(
        tokens,
        proj_inner,
        proj_gate,
        proj_bc,
        proj_step.T,
        conv_inner,
        conv_bc,
        offset_inner,
        row(offset_bc),
        row(step_bias),
        row(decay_log),
        row(skip_gain),
        norm_weight,
        out_weight,
    )


def solution(mesh):
    body = functools.partial(per_device, mesh.shape["seq"], mesh.shape["head"])
    return jax.shard_map(
        body,
        mesh=mesh,
        in_specs=(
            P("seq", None),
            P(None, "head"),
            P(None, "head"),
            P(),
            P(None, "head"),
            P(None, "head"),
            P(),
            P("head"),
            P(),
            P("head"),
            P("head"),
            P("head"),
            P("head"),
            P("head", None),
        ),
        out_specs=P(("seq", "head"), None),
        check_vma=False,
    )
```

```python
import functools

import jax
import jax.numpy as jnp
from jax import lax
from jax.experimental import pallas as pl
from jax.experimental.pallas import tpu as pltpu
from jax.sharding import PartitionSpec as P

HEADDIM = 64
STATE = 128
KERNEL = 4
SPAN = 128
HALO = 8
CHUNK = 256
BLOCK = 64
WIDE = 512
PIECES = 4
LOG2E = 1.4426950408889634
EPS = 0.25
MESH = pl.DeviceIdType.MESH
F32 = jnp.float32
BF16 = jnp.bfloat16
LINK = jnp.bfloat16


def silu(v):
    return v / (1.0 + jnp.exp(-v))


def dot(a, b):
    return jnp.dot(a, b, preferred_element_type=F32)


def split(v, count):
    terms = []
    for _ in range(count):
        terms.append(v.astype(BF16))
        v = v - terms[-1].astype(F32)
    return terms


def kernel(
    seqs,
    parts,
    inner_all,
    tokens_hbm,
    wi_hbm,
    wg_hbm,
    wbc_hbm,
    wst_hbm,
    conv_i_hbm,
    conv_b_hbm,
    off_i_hbm,
    off_b_hbm,
    bias_hbm,
    decay_log_hbm,
    skip_hbm,
    norm_hbm,
    wo_hbm,
    out,
    conv_i,
    conv_b,
    off_1,
    off_b,
    bias,
    decay_log,
    skip,
    norm_1,
    tok,
    wa,
    wg,
    wl,
    wst,
    wo,
    raw,
    terms,
    spread,
    w_end,
    xs_ref,
    bc_ref,
    wt_ref,
    cum_ref,
    dt_ref,
    gate,
    part_a,
    part_b,
    prior,
    st_send,
    st_recv,
    dec_send,
    dec_recv,
    pf_send,
    pf_recv,
    s_in,
    held_scan,
    gw,
    far_send,
    far_recv,
    own_send,
    own_recv,
    comb_send,
    comb_recv,
    mine,
    sq_send,
    sq_recv,
    load_sem,
    small_sem,
    halo_sem,
    dec_ss,
    dec_rs,
    st_ss,
    st_rs,
    pf_ss,
    pf_rs,
    far_ss,
    far_rs,
    own_ss,
    own_rs,
    comb_ss,
    comb_rs,
    sq_ss,
    sq_rs,
):
    r = lax.axis_index("seq")
    g = lax.axis_index("head")
    rows = tokens_hbm.shape[0]
    width = wi_hbm.shape[1]
    spans = rows // SPAN
    heads = width // HEADDIM
    pairs = heads // 2
    chunks = width // CHUNK
    half = width // 2
    right = lax.rem(g + 1, parts)
    left = lax.rem(g + parts - 1, parts)
    across = lax.rem(g + 2, parts)

    class loaded:
        def __init__(self, src, dst, number):
            self.whole = pltpu.make_async_copy(src, dst, load_sem.at[number])
            block = src.shape[0] // PIECES
            self.pieces = [
                pltpu.make_async_copy(
                    src.at[pl.ds(i * block, block), :],
                    dst.at[pl.ds(i * block, block), :],
                    load_sem.at[number],
                )
                for i in range(PIECES)
            ]

        def start(self):
            for piece in self.pieces:
                piece.start()

        def wait(self):
            self.whole.wait()

    wides = width // WIDE
    rest = width - wides * WIDE
    tok_load = loaded(tokens_hbm, tok, 0)
    wst_load = pltpu.make_async_copy(wst_hbm, wst, load_sem.at[1])
    wl_load = loaded(wg_hbm.at[:, pl.ds(wides * WIDE, rest)], wl, 2)
    wbc_load = loaded(wbc_hbm, wa.at[0, :, pl.ds(0, 2 * STATE)], 3)
    wr_load = loaded(
        wi_hbm.at[:, pl.ds(wides * WIDE, rest)], wa.at[0, :, pl.ds(2 * STATE, rest)], 4
    )
    wi_load = [
        loaded(wi_hbm.at[:, pl.ds(c * WIDE, WIDE)], wa.at[1 + c], 5 + c) for c in range(wides)
    ]
    wg_load = [
        loaded(wg_hbm.at[:, pl.ds(c * WIDE, WIDE)], wg.at[c], 5 + wides + c) for c in range(wides)
    ]
    wo_load = [
        pltpu.make_async_copy(
            wo_hbm.at[:, pl.ds(c * CHUNK, CHUNK)], wo.at[c], load_sem.at[5 + 2 * wides]
        )
        for c in range(2 * chunks)
    ]
    small_load = [
        pltpu.make_async_copy(src, dst, small_sem.at[i])
        for i, (src, dst) in enumerate(
            (
                (bias_hbm, bias),
                (decay_log_hbm, decay_log),
                (conv_b_hbm, conv_b),
                (off_b_hbm, off_b),
                (conv_i_hbm, conv_i),
                (off_i_hbm, off_1),
                (skip_hbm, skip),
                (norm_hbm, norm_1),
            )
        )
    ]
    tok_load.start()
    wst_load.start()

    barrier = pltpu.get_barrier_semaphore()

    for i in range(1, seqs):
        peer = jnp.where(r + i >= seqs, r + i - seqs, r + i)
        pl.semaphore_signal(
            barrier, inc=1, device_id={"seq": peer, "head": g}, device_id_type=MESH
        )
    for other in (right, left, across):
        pl.semaphore_signal(
            barrier, inc=1, device_id={"seq": r, "head": other}, device_id_type=MESH
        )

    for copy in small_load:
        copy.start()
    wbc_load.start()
    wr_load.start()

    def far_copy(src, dst, ss, rs, seq, head):
        return pltpu.make_async_remote_copy(
            src_ref=src,
            dst_ref=dst,
            send_sem=ss,
            recv_sem=rs,
            device_id={"seq": seq, "head": head},
            device_id_type=MESH,
        )

    lane = lax.broadcasted_iota(jnp.int32, (SPAN, SPAN), 1)
    sub = lax.broadcasted_iota(jnp.int32, (SPAN, SPAN), 0)
    low = lane < HEADDIM
    low_row = low[:1]
    head_of = lax.broadcasted_iota(jnp.int32, (SPAN, width), 1) // HEADDIM
    onto = jnp.where(head_of == lax.broadcasted_iota(jnp.int32, (SPAN, width), 0), 1.0, 0.0)
    spread[pl.ds(0, SPAN), :] = onto.astype(BF16)
    spread[pl.ds(SPAN, SPAN), :] = onto.astype(BF16)
    terms[...] = jnp.zeros_like(terms)
    dt_ref[...] = jnp.zeros_like(dt_ref)
    wst_load.wait()
    tok_load.wait()
    for copy in wi_load:
        copy.start()
    for side in range(2):
        at = pl.ds(side * (rows // 2), rows // 2)
        dt_ref[at, pl.ds(0, heads)] = lax.dot_general(
            tok[at, :], wst[...], (((1,), (1,)), ((), ())), preferred_element_type=F32
        )

    def raw_part(q, m):
        at = rows // 2 * m
        v = dot(tok[pl.ds(at, rows // 2), :], wa[q]).astype(BF16).astype(F32)
        for j in range(WIDE // SPAN):
            raw[q, j, pl.ds(HALO + at, rows // 2), :] = v[:, j * SPAN : (j + 1) * SPAN]

    wbc_load.wait()
    wr_load.wait()
    raw_part(0, 1)
    for copy in small_load:
        copy.wait()
    off_i = off_1[...].reshape(1, -1)
    norm_w = norm_1[...].reshape(1, -1)
    step = dt_ref[:, pl.ds(0, heads)] + bias[...]
    tail = jnp.exp(-jnp.abs(step))
    up = 1.0 + tail
    log1p = jnp.where(up == 1.0, tail, jnp.log(up) * (tail / jnp.where(up == 1.0, 1.0, up - 1.0)))
    dt = jnp.maximum(step, 0.0) + log1p
    log_a = dt * (-LOG2E * jnp.exp(decay_log[...]))
    dt_ref[:, pl.ds(0, heads)] = dt
    for t, term in enumerate(split(log_a, 3)):
        for k in range(spans):
            terms[pl.ds(t * SPAN, SPAN), pl.ds(k * SPAN, heads)] = term[k * SPAN : (k + 1) * SPAN]
    tri = jnp.where(lane <= sub, 1.0, 0.0).astype(BF16)
    wi_load[0].wait()
    raw_part(1, 1)
    cums = dot(jnp.concatenate([tri, tri, tri], axis=1), terms[...])
    ends = []
    for k in range(spans):
        at = pl.ds(k * SPAN, SPAN)
        cum = cums[:, k * SPAN : (k + 1) * SPAN]
        cum_ref[at, :] = cum
        end_w = jnp.exp2(jnp.minimum(cum[SPAN - 1 :, :] - cum, 0.0)) * dt_ref[at, :]
        ends.append(jnp.concatenate(split(end_w, 2), axis=1))
    w_end[...] = dot(jnp.concatenate(ends, axis=0), spread[...])

    for q in range(1, wides):
        wi_load[q].wait()
        raw_part(1 + q, 1)
    wl_load.start()
    for copy in wg_load:
        copy.start()
    for copy in wo_load:
        copy.start()

    pl.semaphore_wait(barrier, seqs + 2)

    edge = far_copy(
        raw.at[:, :, pl.ds(rows, HALO), :],
        raw.at[:, :, pl.ds(0, HALO), :],
        halo_sem.at[0],
        halo_sem.at[1],
        lax.rem(r + 1, seqs),
        g,
    )

    @pl.when(r < seqs - 1)
    def _():
        edge.start()

    def gate_store(v, cols):
        gate[:, cols] = silu(v.astype(BF16).astype(F32))

    order = [wides * WIDE + j * SPAN for j in range(rest // SPAN)]
    order += [j * SPAN for j in range(wides * WIDE // SPAN)]
    per_side = len(order) // 2
    place = {col: divmod(n, per_side) for n, col in enumerate(order)}
    my_tile = r // 2
    my_side = lax.rem(r, 2)
    chips = seqs // 2

    group = seqs // 4
    row = r // group

    def dec_copy(side, chip):
        return far_copy(
            dec_send.at[side], dec_recv.at[r], dec_ss.at[0], dec_rs.at[row], chip * 2 + side, g
        )

    def st_copy(side, chip):
        return far_copy(
            st_send.at[side, chip],
            st_recv.at[r],
            st_ss.at[0],
            st_rs.at[row],
            chip * 2 + side,
            g,
        )

    def pf_copy(dst):
        return far_copy(
            pf_send.at[dst], pf_recv.at[my_side, my_tile], pf_ss.at[0], pf_rs.at[0], dst, g
        )

    def bulk(ref, ss, rs):
        return far_copy(ref, ref, ss, rs, r, g)

    def each(first, last, act):
        def one(d, carry):
            act(d)
            return carry

        lax.fori_loop(first, jnp.minimum(r, last), one, 0)
        lax.fori_loop(jnp.maximum(r + 1, first), last, one, 0)

    def to_side(side, act):
        def one(i, carry):
            chip = my_tile + i
            act(side, jnp.where(chip >= chips, chip - chips, chip))
            return carry

        for i in range(1, chips):
            one(i, 0)

        @pl.when(my_side != side)
        def _():
            act(side, my_tile)

    total = jnp.zeros((1, SPAN), F32)
    for k in range(spans):
        total = total + cum_ref[pl.ds(k * SPAN + SPAN - 1, 1), :]
    total = jnp.exp2(total)
    for col, (side, n) in place.items():
        p = col // SPAN
        dec_send[side, :, pl.ds(n * SPAN, SPAN)] = jnp.where(
            low_row,
            jnp.broadcast_to(total[:, 2 * p : 2 * p + 1], (1, SPAN)),
            jnp.broadcast_to(total[:, 2 * p + 1 : 2 * p + 2], (1, SPAN)),
        )
    for side in range(2):
        to_side(side, lambda at, chip: dec_copy(at, chip).start())
    dec_recv[r] = dec_send[my_side]

    def conv(q, j, taps, offset, col, dst, blocks):
        cols = pl.ds(col, SPAN)
        for b in blocks:
            acc = offset[:, cols]
            for k in range(KERNEL):
                at = pl.ds(HALO - KERNEL + 1 + k + b * BLOCK, BLOCK)
                acc = acc + taps[pl.ds(k, 1), cols] * raw[q, j, at, :]
            dst[pl.ds(b * BLOCK, BLOCK), cols] = silu(acc).astype(BF16)

    tiles = STATE // 8

    def local_state(col):
        cols = pl.ds(col, SPAN)
        p = col // SPAN
        side, n = place[col]
        held = jnp.zeros((STATE, SPAN), F32)
        for k in range(spans):
            own = pl.ds(k * SPAN, SPAN)
            last = jnp.exp2(cum_ref[pl.ds(k * SPAN + SPAN - 1, 1), :])
            d = jnp.where(
                low_row,
                jnp.broadcast_to(last[:, 2 * p : 2 * p + 1], (1, SPAN)),
                jnp.broadcast_to(last[:, 2 * p + 1 : 2 * p + 2], (1, SPAN)),
            )
            prior[k, :, cols] = held.astype(BF16)
            scaled = (xs_ref[own, cols].astype(F32) * w_end[own, cols]).astype(BF16)
            held = d * held + dot(wt_ref[k], scaled)
        st_send[side, :, :, pl.ds(n * SPAN, SPAN)] = held.reshape(tiles, 8, SPAN).astype(LINK)
        if n == per_side - 1:
            to_side(side, lambda at, chip: st_copy(at, chip).start())

            @pl.when(my_side == side)
            def _():
                st_recv[r] = st_send[side, my_tile]

    def gate_wide(c):
        wg_load[c].wait()
        gate_store(dot(tok[...], wg[c]), pl.ds(c * WIDE, WIDE))

    convs = [(0, j, conv_b, off_b, j * SPAN, bc_ref) for j in range(2 * STATE // SPAN)]
    for n, col in enumerate(order):
        q, j = divmod(2 * STATE // SPAN + n, WIDE // SPAN)
        convs.append((q, j, conv_i, off_i, col, xs_ref))
    middle = rows // BLOCK // 2
    upper = range(middle + 1, rows // BLOCK)
    lower = range(1, middle + 1)
    per_part = WIDE // SPAN
    later = convs.pop(1)
    raw_part(0, 0)
    for args in convs:
        conv(*args, upper)
    for q in range(1, 1 + wides):
        raw_part(q, 0)
        for args in convs[max((q - 1) * per_part - 1, 0) : q * per_part - 1]:
            conv(*args, lower)
    for args in convs[wides * per_part - 1 :]:
        conv(*args, lower)

    @pl.when(r == 0)
    def _():
        raw[:, :, pl.ds(0, HALO), :] = jnp.zeros((1 + wides, WIDE // SPAN, HALO, SPAN), F32)

    @pl.when(r > 0)
    def _():
        edge.wait_recv()

    for args in convs:
        conv(*args, range(1))
    for k in range(spans):
        wt_ref[k] = bc_ref[pl.ds(k * SPAN, SPAN), pl.ds(0, STATE)].astype(F32).T.astype(BF16)
    for col in order:
        local_state(col)
    conv(*later, range(rows // BLOCK))

    def within(k, carry):
        at = pl.ds(pl.multiple_of(k * SPAN, SPAN), SPAN)
        cum = cum_ref[at, :]
        cum_t = cum.T
        dt_t = dt_ref[at, :].T
        read = bc_ref[at, pl.ds(STATE, STATE)]
        write_t = wt_ref[k]
        scores = jnp.where(lane <= sub, dot(read, write_t), 0.0)
        base = carry
        for p in range(pairs):
            cols = pl.ds(p * SPAN, SPAN)
            x = xs_ref[at, cols]
            shown = []
            weights = []
            for h in (2 * p, 2 * p + 1):
                spread = jnp.broadcast_to(cum[:, h : h + 1], (SPAN, SPAN))
                shown.append(spread)
                gap = jnp.minimum(spread - cum_t[h : h + 1, :], 0.0)
                weights.append((scores * jnp.exp2(gap) * dt_t[h : h + 1, :]).astype(BF16))
            zero = jnp.zeros_like(x)
            both = jnp.concatenate([jnp.where(low, x, zero), jnp.where(low, zero, x)], axis=0)
            intra = dot(jnp.concatenate(weights, axis=1), both)
            scale = jnp.exp2(jnp.where(low, shown[0], shown[1]))
            inter = scale * dot(read, prior[k, :, cols])
            ahead = jnp.exp2(
                jnp.where(
                    low_row,
                    jnp.broadcast_to(base[:, 2 * p : 2 * p + 1], (1, SPAN)),
                    jnp.broadcast_to(base[:, 2 * p + 1 : 2 * p + 2], (1, SPAN)),
                )
            )
            gain = jnp.where(
                low_row,
                jnp.broadcast_to(skip[:, 2 * p : 2 * p + 1], (1, SPAN)),
                jnp.broadcast_to(skip[:, 2 * p + 1 : 2 * p + 2], (1, SPAN)),
            )
            opened = gate[at, cols]
            part_a[at, cols] = (intra + inter + gain * x.astype(F32)) * opened
            part_b[at, cols] = scale * ahead * opened
        return base + cum[SPAN - 1 :, :]

    def own_scan(begin, end):
        def arrived(q, count):
            at = pl.ds(q * group, count)
            bulk(dec_recv.at[at], dec_ss.at[0], dec_rs.at[q]).wait_recv()
            bulk(st_recv.at[at], st_ss.at[0], st_rs.at[q]).wait_recv()

        def scan(d, carry):
            pf_send[d] = carry.astype(LINK)
            return dec_recv[d] * carry + st_recv[d].astype(F32)

        def one_group(q, carry):
            @pl.when(q == row)
            def _():
                arrived(q, group - 1)

            @pl.when(q != row)
            def _():
                arrived(q, group)

            first, last = q * group, (q + 1) * group
            held_scan[...] = lax.fori_loop(first, last, scan, held_scan[...])
            each(first, last, lambda d: pf_copy(d).start())

            @pl.when(q == row)
            def _():
                pf_recv[my_side, my_tile] = pf_send[r]

            return carry

        lax.fori_loop(begin, end, one_group, 0)

    def rounds(before, after):
        def of(done):
            return jnp.where(
                row == 0,
                done[0],
                jnp.where(row == 1, done[1], jnp.where(row == 2, done[2], done[3])),
            )

        own_scan(of(before), of(after))

    done = ((0, 0, 0, 0), (0, 0, 1, 2), (1, 2, 4, 4), (4, 4, 4, 4))

    held_scan[...] = jnp.zeros((8, half), F32)

    gate_wide(0)
    gate_wide(1)
    rounds(done[0], done[1])
    wl_load.wait()
    gate_store(dot(tok[...], wl[...]), pl.ds(wides * WIDE, rest))
    rounds(done[1], done[2])
    base = lax.fori_loop(0, spans // 2, within, jnp.zeros((1, SPAN), F32))
    rounds(done[2], done[3])
    lax.fori_loop(spans // 2, spans, within, base)
    pltpu.make_async_copy(wo, wo, load_sem.at[5 + 2 * wides]).wait()

    bulk(pf_send.at[pl.ds(0, seqs - 1)], pf_ss.at[0], pf_rs.at[0]).wait_recv()
    for side in range(2):
        got = pf_recv[side].astype(F32).reshape(STATE, half).astype(BF16)
        for col, (at, n) in place.items():
            if at == side:
                s_in[:, pl.ds(col, SPAN)] = got[:, n * SPAN : (n + 1) * SPAN]

    eye = jnp.where(lane == sub, 1.0, 0.0).astype(F32)

    def gated(slot, block):
        at = pl.ds(pl.multiple_of(block * SPAN, SPAN), SPAN)
        read = bc_ref[at, pl.ds(STATE, STATE)]
        squares = jnp.zeros((SPAN, CHUNK), F32)
        for c in range(chunks):
            cols = pl.ds(c * CHUNK, CHUNK)
            pre = part_a[at, cols] + part_b[at, cols] * dot(read, s_in[:, cols])
            squares = squares + pre * pre
            gw[slot, :, cols] = (pre * norm_w[:, cols]).astype(BF16)
        column = jnp.sum(squares, axis=1, keepdims=True)
        row = jnp.sum(eye * column, axis=0, keepdims=True)
        sq_send[slot] = jnp.broadcast_to(row, (8, SPAN))

    def sq_copy(slot, offset):
        return far_copy(
            sq_send.at[slot],
            sq_recv.at[offset - 1],
            sq_ss.at[0],
            sq_rs.at[0],
            r,
            lax.rem(g + offset, parts),
        )

    def stream(send, recv, ss, rs, c, way):
        at = way * chunks + c
        return far_copy(
            send.at[at],
            recv.at[at],
            ss.at[0],
            rs.at[0] if rs is not comb_rs else rs.at[c // (chunks - 1)],
            r,
            (right, left)[way],
        )

    def far_step(c, carry):
        for way in range(2):
            far_send[way * chunks + c] = dot(gw[0], wo[way * chunks + c]).astype(BF16)
            stream(far_send, far_recv, far_ss, far_rs, c, way).start()
        return carry

    def own_step(c, carry):
        for way in range(2):
            own_send[way * chunks + c] = dot(gw[1 + way], wo[(1 - way) * chunks + c]).astype(BF16)
            stream(own_send, own_recv, own_ss, own_rs, c, way).start()
        return carry

    def mine_step(c, carry):
        mine[c] = dot(gw[3], wo[c])
        return carry

    def comb_step(c, carry):
        for way in range(2):
            at = way * chunks + c
            value = dot(gw[1 + way], wo[at])
            comb_send[at] = (value + far_recv[at].astype(F32)).astype(BF16)
            stream(comb_send, comb_recv, comb_ss, comb_rs, c, way).start()
        return carry

    gated(0, across)
    sq_copy(0, 2).start()
    lax.fori_loop(0, chunks, far_step, 0)
    gated(1, right)
    sq_copy(1, 1).start()
    gated(2, left)
    sq_copy(2, 3).start()
    lax.fori_loop(0, chunks, own_step, 0)
    gated(3, g)
    lax.fori_loop(0, 2 * chunks, mine_step, 0)
    bulk(far_recv, far_ss.at[0], far_rs.at[0]).wait_recv()
    lax.fori_loop(0, chunks, comb_step, 0)

    others = pl.ds(0, seqs - 1)
    bulk(dec_recv.at[others], dec_ss.at[0], dec_rs.at[0]).wait_send()
    bulk(st_recv.at[others], st_ss.at[0], st_rs.at[0]).wait_send()
    bulk(pf_send.at[others], pf_ss.at[0], pf_rs.at[0]).wait_send()

    @pl.when(r < seqs - 1)
    def _():
        edge.wait_send()

    bulk(sq_recv, sq_ss.at[0], sq_rs.at[0]).wait_send()
    bulk(far_send, far_ss.at[0], far_rs.at[0]).wait_send()
    bulk(own_send, own_ss.at[0], own_rs.at[0]).wait_send()

    bulk(sq_recv, sq_ss.at[0], sq_rs.at[0]).wait_recv()
    squares = sq_send[3] + sq_recv[0] + sq_recv[1] + sq_recv[2]
    scale_row = 1.0 / jnp.sqrt(squares[:1] * (1.0 / inner_all) + EPS)
    scale = jnp.sum(eye * scale_row, axis=1, keepdims=True)

    bulk(own_recv, own_ss.at[0], own_rs.at[0]).wait_recv()
    for c in range(chunks):
        if c == 0:
            bulk(comb_recv.at[pl.ds(0, 2 * chunks - 2)], comb_ss.at[0], comb_rs.at[0]).wait_recv()
        if c == chunks - 1:
            bulk(comb_recv.at[pl.ds(0, 2)], comb_ss.at[0], comb_rs.at[1]).wait_recv()
        value = mine[c] + own_recv[chunks + c].astype(F32) + comb_recv[c].astype(F32)
        out[:, pl.ds(c * CHUNK, CHUNK)] = (value * scale).astype(BF16)
        value = mine[chunks + c] + own_recv[c].astype(F32) + comb_recv[chunks + c].astype(F32)
        out[:, pl.ds((chunks + c) * CHUNK, CHUNK)] = (value * scale).astype(BF16)

    bulk(comb_send, comb_ss.at[0], comb_rs.at[0]).wait_send()


def per_device(
    seqs,
    parts,
    tokens,
    proj_inner,
    proj_gate,
    proj_bc,
    proj_step,
    conv_inner,
    conv_bc,
    offset_inner,
    offset_bc,
    step_bias,
    decay_log,
    skip_gain,
    norm_weight,
    out_weight,
):
    rows, depth = tokens.shape
    width = proj_inner.shape[1]
    heads = step_bias.shape[0]
    chunks = width // CHUNK
    spans = rows // SPAN
    half = width // 2
    tiles = STATE // 8
    model = out_weight.shape[1]
    any_spec = pl.BlockSpec(memory_space=pl.ANY)
    vmem = pl.BlockSpec(memory_space=pltpu.VMEM)
    dma = pltpu.SemaphoreType.DMA
    streams = [pltpu.VMEM((2 * chunks, SPAN, CHUNK), BF16)] * 6
    scratch = [
        pltpu.VMEM((KERNEL, width), F32),
        pltpu.VMEM((KERNEL, 2 * STATE), F32),
        pltpu.VMEM((width,), F32),
        pltpu.VMEM((1, 2 * STATE), F32),
        pltpu.VMEM((1, heads), F32),
        pltpu.VMEM((1, heads), F32),
        pltpu.VMEM((1, heads), F32),
        pltpu.VMEM((width,), F32),
        pltpu.VMEM((rows, depth), BF16),
        pltpu.VMEM((1 + width // WIDE, depth, WIDE), BF16),
        pltpu.VMEM((width // WIDE, depth, WIDE), BF16),
        pltpu.VMEM((depth, width % WIDE), BF16),
        pltpu.VMEM((heads, depth), BF16),
        pltpu.VMEM((2 * chunks, width, CHUNK), BF16),
        pltpu.VMEM((1 + width // WIDE, WIDE // SPAN, rows + HALO, SPAN), F32),
        pltpu.VMEM((3 * SPAN, spans * SPAN), BF16),
        pltpu.VMEM((2 * SPAN, width), BF16),
        pltpu.VMEM((rows, width), F32),
        pltpu.VMEM((rows, width), BF16),
        pltpu.VMEM((rows, 2 * STATE), BF16),
        pltpu.VMEM((spans, STATE, SPAN), BF16),
        pltpu.VMEM((rows, SPAN), F32),
        pltpu.VMEM((rows, SPAN), F32),
        pltpu.VMEM((rows, width), F32),
        pltpu.VMEM((rows, width), F32),
        pltpu.VMEM((rows, width), F32),
        pltpu.VMEM((spans, STATE, width), BF16),
        pltpu.VMEM((2, tiles, 8, half), LINK),
        pltpu.VMEM((seqs, 8, half), LINK),
        pltpu.VMEM((2, 1, half), F32),
        pltpu.VMEM((seqs, 1, half), F32),
        pltpu.VMEM((seqs, 8, half), LINK),
        pltpu.VMEM((2, tiles, 8, half), LINK),
        pltpu.VMEM((STATE, width), BF16),
        pltpu.VMEM((8, half), F32),
        pltpu.VMEM((4, SPAN, width), BF16),
        *streams,
        pltpu.VMEM((2 * chunks, SPAN, CHUNK), F32),
        pltpu.VMEM((4, 8, SPAN), F32),
        pltpu.VMEM((3, 8, SPAN), F32),
        dma((6 + 2 * (width // WIDE),)),
        dma((8,)),
        dma((2,)),
        dma((1,)),
        dma((4,)),
        dma((1,)),
        dma((4,)),
        dma((1,)),
        dma((1,)),
        dma((1,)),
        dma((1,)),
        dma((1,)),
        dma((1,)),
        dma((1,)),
        dma((2,)),
        dma((1,)),
        dma((1,)),
    ]
    row = lambda v: v.reshape(1, -1)
    return pl.pallas_call(
        functools.partial(kernel, seqs, parts, float(parts * width)),
        out_shape=pltpu.VMEM((rows // parts, model), BF16),
        in_specs=[any_spec] * 14,
        out_specs=vmem,
        scratch_shapes=scratch,
        compiler_params=pltpu.CompilerParams(
            collective_id=0, has_side_effects=True, vmem_limit_bytes=62 * 1024 * 1024
        ),
    )(
        tokens,
        proj_inner,
        proj_gate,
        proj_bc,
        proj_step.T,
        conv_inner,
        conv_bc,
        offset_inner,
        row(offset_bc),
        row(step_bias),
        row(decay_log),
        row(skip_gain),
        norm_weight,
        out_weight,
    )


def solution(mesh):
    body = functools.partial(per_device, mesh.shape["seq"], mesh.shape["head"])
    return jax.shard_map(
        body,
        mesh=mesh,
        in_specs=(
            P("seq", None),
            P(None, "head"),
            P(None, "head"),
            P(),
            P(None, "head"),
            P(None, "head"),
            P(),
            P("head"),
            P(),
            P("head"),
            P("head"),
            P("head"),
            P("head"),
            P("head", None),
        ),
        out_specs=P(("seq", "head"), None),
        check_vma=False,
    )
```

```python
import functools

import jax
import jax.numpy as jnp
from jax import lax
from jax.experimental import pallas as pl
from jax.experimental.pallas import tpu as pltpu
from jax.sharding import PartitionSpec as P

HEADDIM = 64
STATE = 128
KERNEL = 4
SPAN = 128
HALO = 8
CHUNK = 256
BLOCK = 32
WIDE = 512
PIECES = 4
LOG2E = 1.4426950408889634
EPS = 0.25
MESH = pl.DeviceIdType.MESH
F32 = jnp.float32
BF16 = jnp.bfloat16
LINK = jnp.bfloat16


def silu(v):
    return v / (1.0 + jnp.exp(-v))


def dot(a, b):
    return jnp.dot(a, b, preferred_element_type=F32)


def split(v, count):
    terms = []
    for _ in range(count):
        terms.append(v.astype(BF16))
        v = v - terms[-1].astype(F32)
    return terms


def kernel(
    seqs,
    parts,
    inner_all,
    tokens_hbm,
    wi_hbm,
    wg_hbm,
    wbc_hbm,
    wst_hbm,
    conv_i_hbm,
    conv_b_hbm,
    off_i_hbm,
    off_b_hbm,
    bias_hbm,
    decay_log_hbm,
    skip_hbm,
    norm_hbm,
    wo_hbm,
    out,
    conv_i,
    conv_b,
    off_1,
    off_b,
    bias,
    decay_log,
    skip,
    norm_1,
    tok,
    wa,
    wg,
    wl,
    wst,
    wo,
    raw,
    terms,
    spread,
    w_end,
    xs_ref,
    bc_ref,
    wt_ref,
    cum_ref,
    dt_ref,
    gate,
    part_a,
    part_b,
    prior,
    st_send,
    st_recv,
    dec_send,
    dec_recv,
    pf_send,
    pf_recv,
    s_in,
    held_scan,
    gw,
    far_send,
    far_recv,
    own_send,
    own_recv,
    comb_send,
    comb_recv,
    mine,
    sq_send,
    sq_recv,
    load_sem,
    small_sem,
    halo_sem,
    dec_ss,
    dec_rs,
    st_ss,
    st_rs,
    pf_ss,
    pf_rs,
    far_ss,
    far_rs,
    own_ss,
    own_rs,
    comb_ss,
    comb_rs,
    sq_ss,
    sq_rs,
):
    r = lax.axis_index("seq")
    g = lax.axis_index("head")
    rows = tokens_hbm.shape[0]
    width = wi_hbm.shape[1]
    spans = rows // SPAN
    heads = width // HEADDIM
    pairs = heads // 2
    chunks = width // CHUNK
    half = width // 2
    right = lax.rem(g + 1, parts)
    left = lax.rem(g + parts - 1, parts)
    across = lax.rem(g + 2, parts)

    class loaded:
        def __init__(self, src, dst, number):
            self.whole = pltpu.make_async_copy(src, dst, load_sem.at[number])
            block = src.shape[0] // PIECES
            self.pieces = [
                pltpu.make_async_copy(
                    src.at[pl.ds(i * block, block), :],
                    dst.at[pl.ds(i * block, block), :],
                    load_sem.at[number],
                )
                for i in range(PIECES)
            ]

        def start(self):
            for piece in self.pieces:
                piece.start()

        def wait(self):
            self.whole.wait()

    wides = width // WIDE
    rest = width - wides * WIDE
    tok_load = loaded(tokens_hbm, tok, 0)
    wst_load = pltpu.make_async_copy(wst_hbm, wst, load_sem.at[1])
    wl_load = loaded(wg_hbm.at[:, pl.ds(wides * WIDE, rest)], wl, 2)
    wbc_load = loaded(wbc_hbm, wa.at[0, :, pl.ds(0, 2 * STATE)], 3)
    wr_load = loaded(
        wi_hbm.at[:, pl.ds(wides * WIDE, rest)], wa.at[0, :, pl.ds(2 * STATE, rest)], 4
    )
    wi_load = [
        loaded(wi_hbm.at[:, pl.ds(c * WIDE, WIDE)], wa.at[1 + c], 5 + c) for c in range(wides)
    ]
    wg_load = [
        loaded(wg_hbm.at[:, pl.ds(c * WIDE, WIDE)], wg.at[c], 5 + wides + c) for c in range(wides)
    ]
    wo_load = [
        pltpu.make_async_copy(
            wo_hbm.at[:, pl.ds(c * CHUNK, CHUNK)], wo.at[c], load_sem.at[5 + 2 * wides]
        )
        for c in range(2 * chunks)
    ]
    small_load = [
        pltpu.make_async_copy(src, dst, small_sem.at[i])
        for i, (src, dst) in enumerate(
            (
                (bias_hbm, bias),
                (decay_log_hbm, decay_log),
                (conv_b_hbm, conv_b),
                (off_b_hbm, off_b),
                (conv_i_hbm, conv_i),
                (off_i_hbm, off_1),
                (skip_hbm, skip),
                (norm_hbm, norm_1),
            )
        )
    ]
    for copy in small_load:
        copy.start()
    tok_load.start()
    wst_load.start()
    wbc_load.start()
    wr_load.start()

    barrier = pltpu.get_barrier_semaphore()

    def greet_seq(i, carry):
        pl.semaphore_signal(
            barrier,
            inc=1,
            device_id={"seq": lax.rem(r + i, seqs), "head": g},
            device_id_type=MESH,
        )
        return carry

    lax.fori_loop(1, seqs, greet_seq, 0)
    for other in (right, left, across):
        pl.semaphore_signal(
            barrier, inc=1, device_id={"seq": r, "head": other}, device_id_type=MESH
        )

    def far_copy(src, dst, ss, rs, seq, head):
        return pltpu.make_async_remote_copy(
            src_ref=src,
            dst_ref=dst,
            send_sem=ss,
            recv_sem=rs,
            device_id={"seq": seq, "head": head},
            device_id_type=MESH,
        )

    lane = lax.broadcasted_iota(jnp.int32, (SPAN, SPAN), 1)
    sub = lax.broadcasted_iota(jnp.int32, (SPAN, SPAN), 0)
    low = lane < HEADDIM
    low_row = low[:1]
    head_of = lax.broadcasted_iota(jnp.int32, (SPAN, width), 1) // HEADDIM
    onto = jnp.where(head_of == lax.broadcasted_iota(jnp.int32, (SPAN, width), 0), 1.0, 0.0)
    spread[pl.ds(0, SPAN), :] = onto.astype(BF16)
    spread[pl.ds(SPAN, SPAN), :] = onto.astype(BF16)
    terms[...] = jnp.zeros_like(terms)
    dt_ref[...] = jnp.zeros_like(dt_ref)
    wst_load.wait()
    tok_load.wait()
    for copy in wi_load:
        copy.start()
    for side in range(2):
        at = pl.ds(side * (rows // 2), rows // 2)
        dt_ref[at, pl.ds(0, heads)] = lax.dot_general(
            tok[at, :], wst[...], (((1,), (1,)), ((), ())), preferred_element_type=F32
        )

    def raw_part(q, m):
        at = rows // 2 * m
        v = dot(tok[pl.ds(at, rows // 2), :], wa[q]).astype(BF16).astype(F32)
        for j in range(WIDE // SPAN):
            raw[q, j, pl.ds(HALO + at, rows // 2), :] = v[:, j * SPAN : (j + 1) * SPAN]

    wbc_load.wait()
    wr_load.wait()
    raw_part(0, 1)
    for copy in small_load:
        copy.wait()
    off_i = off_1[...].reshape(1, -1)
    norm_w = norm_1[...].reshape(1, -1)
    step = dt_ref[:, pl.ds(0, heads)] + bias[...]
    tail = jnp.exp(-jnp.abs(step))
    up = 1.0 + tail
    log1p = jnp.where(up == 1.0, tail, jnp.log(up) * (tail / jnp.where(up == 1.0, 1.0, up - 1.0)))
    dt = jnp.maximum(step, 0.0) + log1p
    log_a = dt * (-LOG2E * jnp.exp(decay_log[...]))
    dt_ref[:, pl.ds(0, heads)] = dt
    for t, term in enumerate(split(log_a, 3)):
        for k in range(spans):
            terms[pl.ds(t * SPAN, SPAN), pl.ds(k * SPAN, heads)] = term[k * SPAN : (k + 1) * SPAN]
    tri = jnp.where(lane <= sub, 1.0, 0.0).astype(BF16)
    wi_load[0].wait()
    raw_part(1, 1)
    cums = dot(jnp.concatenate([tri, tri, tri], axis=1), terms[...])
    ends = []
    for k in range(spans):
        at = pl.ds(k * SPAN, SPAN)
        cum = cums[:, k * SPAN : (k + 1) * SPAN]
        cum_ref[at, :] = cum
        end_w = jnp.exp2(jnp.minimum(cum[SPAN - 1 :, :] - cum, 0.0)) * dt_ref[at, :]
        ends.append(jnp.concatenate(split(end_w, 2), axis=1))
    w_end[...] = dot(jnp.concatenate(ends, axis=0), spread[...])

    for q in range(1, wides):
        wi_load[q].wait()
        raw_part(1 + q, 1)
    wl_load.start()
    for copy in wg_load:
        copy.start()
    for copy in wo_load:
        copy.start()

    pl.semaphore_wait(barrier, seqs + 2)

    edge = far_copy(
        raw.at[:, :, pl.ds(rows, HALO), :],
        raw.at[:, :, pl.ds(0, HALO), :],
        halo_sem.at[0],
        halo_sem.at[1],
        lax.rem(r + 1, seqs),
        g,
    )

    @pl.when(r < seqs - 1)
    def _():
        edge.start()

    def gate_store(v, cols):
        gate[:, cols] = silu(v.astype(BF16).astype(F32))

    order = [wides * WIDE + j * SPAN for j in range(rest // SPAN)]
    order += [j * SPAN for j in range(wides * WIDE // SPAN)]
    per_side = len(order) // 2
    place = {col: divmod(n, per_side) for n, col in enumerate(order)}
    my_tile = r // 2
    my_side = lax.rem(r, 2)
    chips = seqs // 2

    group = seqs // 4
    row = r // group

    def dec_copy(side, chip):
        return far_copy(
            dec_send.at[side], dec_recv.at[r], dec_ss.at[0], dec_rs.at[row], chip * 2 + side, g
        )

    def st_copy(side, chip):
        return far_copy(
            st_send.at[side, chip],
            st_recv.at[r],
            st_ss.at[0],
            st_rs.at[row],
            chip * 2 + side,
            g,
        )

    def pf_copy(dst):
        return far_copy(
            pf_send.at[dst], pf_recv.at[my_side, my_tile], pf_ss.at[0], pf_rs.at[0], dst, g
        )

    def bulk(ref, ss, rs):
        return far_copy(ref, ref, ss, rs, r, g)

    def each(first, last, act):
        def one(d, carry):
            act(d)
            return carry

        lax.fori_loop(first, jnp.minimum(r, last), one, 0)
        lax.fori_loop(jnp.maximum(r + 1, first), last, one, 0)

    def to_side(side, act):
        def one(i, carry):
            chip = my_tile + i
            act(side, jnp.where(chip >= chips, chip - chips, chip))
            return carry

        for i in range(1, chips):
            one(i, 0)

        @pl.when(my_side != side)
        def _():
            act(side, my_tile)

    total = jnp.zeros((1, SPAN), F32)
    for k in range(spans):
        total = total + cum_ref[pl.ds(k * SPAN + SPAN - 1, 1), :]
    total = jnp.exp2(total)
    for col, (side, n) in place.items():
        p = col // SPAN
        dec_send[side, :, pl.ds(n * SPAN, SPAN)] = jnp.where(
            low_row,
            jnp.broadcast_to(total[:, 2 * p : 2 * p + 1], (1, SPAN)),
            jnp.broadcast_to(total[:, 2 * p + 1 : 2 * p + 2], (1, SPAN)),
        )
    for side in range(2):
        to_side(side, lambda at, chip: dec_copy(at, chip).start())
    dec_recv[r] = dec_send[my_side]

    def conv(q, j, taps, offset, col, dst, blocks):
        cols = pl.ds(col, SPAN)
        for b in blocks:
            acc = offset[:, cols]
            for k in range(KERNEL):
                at = pl.ds(HALO - KERNEL + 1 + k + b * BLOCK, BLOCK)
                acc = acc + taps[pl.ds(k, 1), cols] * raw[q, j, at, :]
            dst[pl.ds(b * BLOCK, BLOCK), cols] = silu(acc).astype(BF16)

    tiles = STATE // 8

    def local_state(col):
        cols = pl.ds(col, SPAN)
        p = col // SPAN
        side, n = place[col]
        held = jnp.zeros((STATE, SPAN), F32)
        for k in range(spans):
            own = pl.ds(k * SPAN, SPAN)
            last = jnp.exp2(cum_ref[pl.ds(k * SPAN + SPAN - 1, 1), :])
            d = jnp.where(
                low_row,
                jnp.broadcast_to(last[:, 2 * p : 2 * p + 1], (1, SPAN)),
                jnp.broadcast_to(last[:, 2 * p + 1 : 2 * p + 2], (1, SPAN)),
            )
            prior[k, :, cols] = held.astype(BF16)
            scaled = (xs_ref[own, cols].astype(F32) * w_end[own, cols]).astype(BF16)
            held = d * held + dot(wt_ref[k], scaled)
        st_send[side, :, :, pl.ds(n * SPAN, SPAN)] = held.reshape(tiles, 8, SPAN).astype(LINK)
        if n == per_side - 1:
            to_side(side, lambda at, chip: st_copy(at, chip).start())

            @pl.when(my_side == side)
            def _():
                st_recv[r] = st_send[side, my_tile]

    def gate_wide(c):
        wg_load[c].wait()
        gate_store(dot(tok[...], wg[c]), pl.ds(c * WIDE, WIDE))

    convs = [(0, j, conv_b, off_b, j * SPAN, bc_ref) for j in range(2 * STATE // SPAN)]
    for n, col in enumerate(order):
        q, j = divmod(2 * STATE // SPAN + n, WIDE // SPAN)
        convs.append((q, j, conv_i, off_i, col, xs_ref))
    middle = rows // BLOCK // 2
    upper = range(middle + 1, rows // BLOCK)
    lower = range(1, middle + 1)
    per_part = WIDE // SPAN
    later = convs.pop(1)
    raw_part(0, 0)
    for args in convs:
        conv(*args, upper)
    for q in range(1, 1 + wides):
        raw_part(q, 0)
        for args in convs[max((q - 1) * per_part - 1, 0) : q * per_part - 1]:
            conv(*args, lower)
    for args in convs[wides * per_part - 1 :]:
        conv(*args, lower)

    @pl.when(r == 0)
    def _():
        raw[:, :, pl.ds(0, HALO), :] = jnp.zeros((1 + wides, WIDE // SPAN, HALO, SPAN), F32)

    @pl.when(r > 0)
    def _():
        edge.wait_recv()

    for args in convs:
        conv(*args, range(1))
    for k in range(spans):
        wt_ref[k] = bc_ref[pl.ds(k * SPAN, SPAN), pl.ds(0, STATE)].astype(F32).T.astype(BF16)
    for col in order:
        local_state(col)
    conv(*later, range(rows // BLOCK))

    def within(k, carry):
        at = pl.ds(pl.multiple_of(k * SPAN, SPAN), SPAN)
        cum = cum_ref[at, :]
        cum_t = cum.T
        dt_t = dt_ref[at, :].T
        read = bc_ref[at, pl.ds(STATE, STATE)]
        write_t = wt_ref[k]
        scores = jnp.where(lane <= sub, dot(read, write_t), 0.0)
        base = carry
        for p in range(pairs):
            cols = pl.ds(p * SPAN, SPAN)
            x = xs_ref[at, cols]
            shown = []
            weights = []
            for h in (2 * p, 2 * p + 1):
                spread = jnp.broadcast_to(cum[:, h : h + 1], (SPAN, SPAN))
                shown.append(spread)
                gap = jnp.minimum(spread - cum_t[h : h + 1, :], 0.0)
                weights.append((scores * jnp.exp2(gap) * dt_t[h : h + 1, :]).astype(BF16))
            zero = jnp.zeros_like(x)
            both = jnp.concatenate([jnp.where(low, x, zero), jnp.where(low, zero, x)], axis=0)
            intra = dot(jnp.concatenate(weights, axis=1), both)
            scale = jnp.exp2(jnp.where(low, shown[0], shown[1]))
            inter = scale * dot(read, prior[k, :, cols])
            ahead = jnp.exp2(
                jnp.where(
                    low_row,
                    jnp.broadcast_to(base[:, 2 * p : 2 * p + 1], (1, SPAN)),
                    jnp.broadcast_to(base[:, 2 * p + 1 : 2 * p + 2], (1, SPAN)),
                )
            )
            gain = jnp.where(
                low_row,
                jnp.broadcast_to(skip[:, 2 * p : 2 * p + 1], (1, SPAN)),
                jnp.broadcast_to(skip[:, 2 * p + 1 : 2 * p + 2], (1, SPAN)),
            )
            opened = gate[at, cols]
            part_a[at, cols] = (intra + inter + gain * x.astype(F32)) * opened
            part_b[at, cols] = scale * ahead * opened
        return base + cum[SPAN - 1 :, :]

    def own_scan(begin, end):
        def arrived(q, count):
            at = pl.ds(q * group, count)
            bulk(dec_recv.at[at], dec_ss.at[0], dec_rs.at[q]).wait_recv()
            bulk(st_recv.at[at], st_ss.at[0], st_rs.at[q]).wait_recv()

        def scan(d, carry):
            pf_send[d] = carry.astype(LINK)
            return dec_recv[d] * carry + st_recv[d].astype(F32)

        def one_group(q, carry):
            @pl.when(q == row)
            def _():
                arrived(q, group - 1)

            @pl.when(q != row)
            def _():
                arrived(q, group)

            first, last = q * group, (q + 1) * group
            held_scan[...] = lax.fori_loop(first, last, scan, held_scan[...])
            each(first, last, lambda d: pf_copy(d).start())

            @pl.when(q == row)
            def _():
                pf_recv[my_side, my_tile] = pf_send[r]

            return carry

        lax.fori_loop(begin, end, one_group, 0)

    def rounds(before, after):
        def of(done):
            return jnp.where(
                row == 0,
                done[0],
                jnp.where(row == 1, done[1], jnp.where(row == 2, done[2], done[3])),
            )

        own_scan(of(before), of(after))

    done = ((0, 0, 0, 0), (0, 0, 1, 1), (1, 2, 4, 4), (4, 4, 4, 4))

    held_scan[...] = jnp.zeros((8, half), F32)

    gate_wide(0)
    gate_wide(1)
    rounds(done[0], done[1])
    wl_load.wait()
    gate_store(dot(tok[...], wl[...]), pl.ds(wides * WIDE, rest))
    rounds(done[1], done[2])
    base = lax.fori_loop(0, spans // 2, within, jnp.zeros((1, SPAN), F32))
    rounds(done[2], done[3])
    lax.fori_loop(spans // 2, spans, within, base)
    pltpu.make_async_copy(wo, wo, load_sem.at[5 + 2 * wides]).wait()

    bulk(pf_send.at[pl.ds(0, seqs - 1)], pf_ss.at[0], pf_rs.at[0]).wait_recv()
    for side in range(2):
        got = pf_recv[side].astype(F32).reshape(STATE, half).astype(BF16)
        for col, (at, n) in place.items():
            if at == side:
                s_in[:, pl.ds(col, SPAN)] = got[:, n * SPAN : (n + 1) * SPAN]

    eye = jnp.where(lane == sub, 1.0, 0.0).astype(F32)

    def gated(slot, block):
        at = pl.ds(pl.multiple_of(block * SPAN, SPAN), SPAN)
        read = bc_ref[at, pl.ds(STATE, STATE)]
        squares = jnp.zeros((SPAN, CHUNK), F32)
        for c in range(chunks):
            cols = pl.ds(c * CHUNK, CHUNK)
            pre = part_a[at, cols] + part_b[at, cols] * dot(read, s_in[:, cols])
            squares = squares + pre * pre
            gw[slot, :, cols] = (pre * norm_w[:, cols]).astype(BF16)
        column = jnp.sum(squares, axis=1, keepdims=True)
        row = jnp.sum(eye * column, axis=0, keepdims=True)
        sq_send[slot] = jnp.broadcast_to(row, (8, SPAN))

    def sq_copy(slot, offset):
        return far_copy(
            sq_send.at[slot],
            sq_recv.at[offset - 1],
            sq_ss.at[0],
            sq_rs.at[0],
            r,
            lax.rem(g + offset, parts),
        )

    def stream(send, recv, ss, rs, c, way):
        at = way * chunks + c
        return far_copy(
            send.at[at],
            recv.at[at],
            ss.at[0],
            rs.at[0] if rs is not comb_rs else rs.at[c // (chunks - 1)],
            r,
            (right, left)[way],
        )

    def far_step(c, carry):
        for way in range(2):
            far_send[way * chunks + c] = dot(gw[0], wo[way * chunks + c]).astype(BF16)
            stream(far_send, far_recv, far_ss, far_rs, c, way).start()
        return carry

    def own_step(c, carry):
        for way in range(2):
            own_send[way * chunks + c] = dot(gw[1 + way], wo[(1 - way) * chunks + c]).astype(BF16)
            stream(own_send, own_recv, own_ss, own_rs, c, way).start()
        return carry

    def mine_step(c, carry):
        mine[c] = dot(gw[3], wo[c])
        return carry

    def comb_step(c, carry):
        for way in range(2):
            at = way * chunks + c
            value = dot(gw[1 + way], wo[at])
            comb_send[at] = (value + far_recv[at].astype(F32)).astype(BF16)
            stream(comb_send, comb_recv, comb_ss, comb_rs, c, way).start()
        return carry

    gated(0, across)
    sq_copy(0, 2).start()
    lax.fori_loop(0, chunks, far_step, 0)
    gated(1, right)
    sq_copy(1, 1).start()
    gated(2, left)
    sq_copy(2, 3).start()
    lax.fori_loop(0, chunks, own_step, 0)
    gated(3, g)
    lax.fori_loop(0, 2 * chunks, mine_step, 0)
    bulk(far_recv, far_ss.at[0], far_rs.at[0]).wait_recv()
    lax.fori_loop(0, chunks, comb_step, 0)

    others = pl.ds(0, seqs - 1)
    bulk(dec_recv.at[others], dec_ss.at[0], dec_rs.at[0]).wait_send()
    bulk(st_recv.at[others], st_ss.at[0], st_rs.at[0]).wait_send()
    bulk(pf_send.at[others], pf_ss.at[0], pf_rs.at[0]).wait_send()

    @pl.when(r < seqs - 1)
    def _():
        edge.wait_send()

    bulk(sq_recv, sq_ss.at[0], sq_rs.at[0]).wait_send()
    bulk(far_send, far_ss.at[0], far_rs.at[0]).wait_send()
    bulk(own_send, own_ss.at[0], own_rs.at[0]).wait_send()

    bulk(sq_recv, sq_ss.at[0], sq_rs.at[0]).wait_recv()
    squares = sq_send[3] + sq_recv[0] + sq_recv[1] + sq_recv[2]
    scale_row = 1.0 / jnp.sqrt(squares[:1] * (1.0 / inner_all) + EPS)
    scale = jnp.sum(eye * scale_row, axis=1, keepdims=True)

    bulk(own_recv, own_ss.at[0], own_rs.at[0]).wait_recv()
    for c in range(chunks):
        if c == 0:
            bulk(comb_recv.at[pl.ds(0, 2 * chunks - 2)], comb_ss.at[0], comb_rs.at[0]).wait_recv()
        if c == chunks - 1:
            bulk(comb_recv.at[pl.ds(0, 2)], comb_ss.at[0], comb_rs.at[1]).wait_recv()
        value = mine[c] + own_recv[chunks + c].astype(F32) + comb_recv[c].astype(F32)
        out[:, pl.ds(c * CHUNK, CHUNK)] = (value * scale).astype(BF16)
        value = mine[chunks + c] + own_recv[c].astype(F32) + comb_recv[chunks + c].astype(F32)
        out[:, pl.ds((chunks + c) * CHUNK, CHUNK)] = (value * scale).astype(BF16)

    bulk(comb_send, comb_ss.at[0], comb_rs.at[0]).wait_send()


def per_device(
    seqs,
    parts,
    tokens,
    proj_inner,
    proj_gate,
    proj_bc,
    proj_step,
    conv_inner,
    conv_bc,
    offset_inner,
    offset_bc,
    step_bias,
    decay_log,
    skip_gain,
    norm_weight,
    out_weight,
):
    rows, depth = tokens.shape
    width = proj_inner.shape[1]
    heads = step_bias.shape[0]
    chunks = width // CHUNK
    spans = rows // SPAN
    half = width // 2
    tiles = STATE // 8
    model = out_weight.shape[1]
    any_spec = pl.BlockSpec(memory_space=pl.ANY)
    vmem = pl.BlockSpec(memory_space=pltpu.VMEM)
    dma = pltpu.SemaphoreType.DMA
    streams = [pltpu.VMEM((2 * chunks, SPAN, CHUNK), BF16)] * 6
    scratch = [
        pltpu.VMEM((KERNEL, width), F32),
        pltpu.VMEM((KERNEL, 2 * STATE), F32),
        pltpu.VMEM((width,), F32),
        pltpu.VMEM((1, 2 * STATE), F32),
        pltpu.VMEM((1, heads), F32),
        pltpu.VMEM((1, heads), F32),
        pltpu.VMEM((1, heads), F32),
        pltpu.VMEM((width,), F32),
        pltpu.VMEM((rows, depth), BF16),
        pltpu.VMEM((1 + width // WIDE, depth, WIDE), BF16),
        pltpu.VMEM((width // WIDE, depth, WIDE), BF16),
        pltpu.VMEM((depth, width % WIDE), BF16),
        pltpu.VMEM((heads, depth), BF16),
        pltpu.VMEM((2 * chunks, width, CHUNK), BF16),
        pltpu.VMEM((1 + width // WIDE, WIDE // SPAN, rows + HALO, SPAN), F32),
        pltpu.VMEM((3 * SPAN, spans * SPAN), BF16),
        pltpu.VMEM((2 * SPAN, width), BF16),
        pltpu.VMEM((rows, width), F32),
        pltpu.VMEM((rows, width), BF16),
        pltpu.VMEM((rows, 2 * STATE), BF16),
        pltpu.VMEM((spans, STATE, SPAN), BF16),
        pltpu.VMEM((rows, SPAN), F32),
        pltpu.VMEM((rows, SPAN), F32),
        pltpu.VMEM((rows, width), F32),
        pltpu.VMEM((rows, width), F32),
        pltpu.VMEM((rows, width), F32),
        pltpu.VMEM((spans, STATE, width), BF16),
        pltpu.VMEM((2, tiles, 8, half), LINK),
        pltpu.VMEM((seqs, 8, half), LINK),
        pltpu.VMEM((2, 1, half), F32),
        pltpu.VMEM((seqs, 1, half), F32),
        pltpu.VMEM((seqs, 8, half), LINK),
        pltpu.VMEM((2, tiles, 8, half), LINK),
        pltpu.VMEM((STATE, width), BF16),
        pltpu.VMEM((8, half), F32),
        pltpu.VMEM((4, SPAN, width), BF16),
        *streams,
        pltpu.VMEM((2 * chunks, SPAN, CHUNK), F32),
        pltpu.VMEM((4, 8, SPAN), F32),
        pltpu.VMEM((3, 8, SPAN), F32),
        dma((6 + 2 * (width // WIDE),)),
        dma((8,)),
        dma((2,)),
        dma((1,)),
        dma((4,)),
        dma((1,)),
        dma((4,)),
        dma((1,)),
        dma((1,)),
        dma((1,)),
        dma((1,)),
        dma((1,)),
        dma((1,)),
        dma((1,)),
        dma((2,)),
        dma((1,)),
        dma((1,)),
    ]
    row = lambda v: v.reshape(1, -1)
    return pl.pallas_call(
        functools.partial(kernel, seqs, parts, float(parts * width)),
        out_shape=pltpu.VMEM((rows // parts, model), BF16),
        in_specs=[any_spec] * 14,
        out_specs=vmem,
        scratch_shapes=scratch,
        compiler_params=pltpu.CompilerParams(
            collective_id=0, has_side_effects=True, vmem_limit_bytes=62 * 1024 * 1024
        ),
    )(
        tokens,
        proj_inner,
        proj_gate,
        proj_bc,
        proj_step.T,
        conv_inner,
        conv_bc,
        offset_inner,
        row(offset_bc),
        row(step_bias),
        row(decay_log),
        row(skip_gain),
        norm_weight,
        out_weight,
    )


def solution(mesh):
    body = functools.partial(per_device, mesh.shape["seq"], mesh.shape["head"])
    return jax.shard_map(
        body,
        mesh=mesh,
        in_specs=(
            P("seq", None),
            P(None, "head"),
            P(None, "head"),
            P(),
            P(None, "head"),
            P(None, "head"),
            P(),
            P("head"),
            P(),
            P("head"),
            P("head"),
            P("head"),
            P("head"),
            P("head", None),
        ),
        out_specs=P(("seq", "head"), None),
        check_vma=False,
    )
```
